32 devices in a mesh: rows: 8 (over z, x), cols: 4 (over y, core).
Axes of the slice: x: 2, y: 2, z: 4, core: 2. Of those that a mesh axis runs over, the one named last changes fastest.
Arguments:
- tokens: bfloat16 [36864, 1280], P(('rows', 'cols')), may hold values from -6 to 6
- cotangent: bfloat16 [36864, 1280], P(('rows', 'cols')), may hold values from -6 to 6
- clip_lengths: int32 [24], P('rows'), may hold values from 384 to 1536, as said below
- clip_sets: int32 [24], P('rows'), may hold values from 0 to 7
- clip_scales: float32 [24], P('rows'), may hold values from 0.5 to 2
- norm1_gain: float32 [1280], replicated, may hold values from 0.5 to 1.5
- norm1_shift: float32 [1280], replicated, may hold values from -3 to 3
- w_query: bfloat16 [1280, 1280], P('rows', 'cols'), may hold values from -0.15625 to 0.15625
- query_bias: float32 [1280], P('cols'), may hold values from -3 to 3
- w_key: bfloat16 [1280, 1280], P('rows', 'cols'), may hold values from -0.15625 to 0.15625
- w_value: bfloat16 [1280, 1280], P('rows', 'cols'), may hold values from -0.15625 to 0.15625
- value_bias: float32 [1280], P('cols'), may hold values from -3 to 3
- w_out: bfloat16 [1280, 1280], P('cols', 'rows'), may hold values from -1.25 to 1.25
- out_bias: float32 [1280], replicated, may hold values from -3 to 3
- norm2_gain: float32 [1280], replicated, may hold values from 0.5 to 1.5
- norm2_shift: float32 [1280], replicated, may hold values from -3 to 3
- w_fc1: bfloat16 [1280, 5120], P('rows', 'cols'), may hold values from -0.15625 to 0.15625
- fc1_bias: float32 [5120], P('cols'), may hold values from -3 to 3
- w_fc2: bfloat16 [5120, 1280], P('cols', 'rows'), may hold values from -0.078125 to 0.078125
- fc2_bias: float32 [1280], replicated, may hold values from -3 to 3
- query_down: bfloat16 [8, 1280, 16], P(None, 'rows'), may hold values from -0.15625 to 0.15625
- query_up: bfloat16 [8, 16, 1280], P(None, 'rows', 'cols'), may hold values from -0.5 to 0.5
- key_down: bfloat16 [8, 1280, 16], P(None, 'rows'), may hold values from -0.15625 to 0.15625
- key_up: bfloat16 [8, 16, 1280], P(None, 'rows', 'cols'), may hold values from -0.5 to 0.5
- value_down: bfloat16 [8, 1280, 16], P(None, 'rows'), may hold values from -0.15625 to 0.15625
- value_up: bfloat16 [8, 16, 1280], P(None, 'rows', 'cols'), may hold values from -0.5 to 0.5
- out_down: bfloat16 [8, 1280, 16], P(None, 'cols', 'rows'), may hold values from -1.25 to 1.25
- out_up: bfloat16 [8, 16, 1280], P(None, None, 'rows'), may hold values from -0.5 to 0.5
- fc1_down: bfloat16 [8, 1280, 16], P(None, 'rows'), may hold values from -0.15625 to 0.15625
- fc1_up: bfloat16 [8, 16, 5120], P(None, 'rows', 'cols'), may hold values from -0.5 to 0.5
- fc2_down: bfloat16 [8, 5120, 16], P(None, 'cols', 'rows'), may hold values from -0.078125 to 0.078125
- fc2_up: bfloat16 [8, 16, 1280], P(None, None, 'rows'), may hold values from -0.5 to 0.5
Outputs:
- output: bfloat16 [36864, 1280], P(('rows', 'cols'))
- grad_tokens: bfloat16 [36864, 1280], P(('rows', 'cols'))
- grad_query_down: float32 [8, 1280, 16], P(None, 'rows')
- grad_query_up: float32 [8, 16, 1280], P(None, 'rows', 'cols')
- grad_key_down: float32 [8, 1280, 16], P(None, 'rows')
- grad_key_up: float32 [8, 16, 1280], P(None, 'rows', 'cols')
- grad_value_down: float32 [8, 1280, 16], P(None, 'rows')
- grad_value_up: float32 [8, 16, 1280], P(None, 'rows', 'cols')
- grad_out_down: float32 [8, 1280, 16], P(None, 'cols', 'rows')
- grad_out_up: float32 [8, 16, 1280], P(None, None, 'rows')
- grad_fc1_down: float32 [8, 1280, 16], P(None, 'rows')
- grad_fc1_up: float32 [8, 16, 5120], P(None, 'rows', 'cols')
- grad_fc2_down: float32 [8, 5120, 16], P(None, 'cols', 'rows')
- grad_fc2_up: float32 [8, 16, 1280], P(None, None, 'rows')
The draws below stay inside these ranges and needn't reach their ends.
Inputs may be any that keep to these rules, and one draw needn't show every extreme that they name: `clip_lengths`: every clip has at least 384 real tokens; clip 0 fills all 1536 slots and clip 1 has exactly 384.
All inputs are finite; a program needn't handle non-finite values.
Results may differ from the reference program's by a relative error of at most 0.02.
Values may be sent and summed in bfloat16 or wider, within the bound.
A program may use at most 448 MiB of HBM per device.

```python
import math
import jax
import jax.numpy as jnp
from jax import lax

D = 1280
HEADS = 16
FF = 5120
RANK = 16
SETS = 8
LEN = 1536
HEAD_DIM = 80
NCLIPS = 24
TOKENS = 36864


def draw_clip_lengths(key, part):
    drawn = jax.random.randint(key, (NCLIPS,), LEN // 4, LEN + 1, dtype=jnp.int32)
    drawn = drawn.at[0].set(LEN)
    return drawn.at[1].set(LEN // 4)


def place_ends(array, key, least, high):
    longest = array.shape.index(max(array.shape))
    spots = []
    for shift in (0, 1):
        where = [jax.random.randint(jax.random.fold_in(key, axis), (), 0, length) for axis, length in enumerate(array.shape)]
        where[longest] = (where[longest] + shift) % array.shape[longest]
        spots.append(tuple(where))
    return array.at[spots[0]].set(least).at[spots[1]].set(high)


def block_scale(stream_key, extent, pieces, low, high):
    loudness = 1.0
    for dim, shards_of in pieces:
        steps = jax.random.uniform(jax.random.fold_in(jax.random.fold_in(stream_key, 6), dim), (shards_of,), jnp.float32, low / len(pieces), high / len(pieces))
        loudness = loudness * jnp.repeat(jnp.exp(steps), extent[dim] // shards_of).reshape((-1,) + (1,) * (len(extent) - 1 - dim))
    return loudness


def gaussian(key, shape, scale, reach, split=(), kind=jnp.bfloat16):
    values = scale * jax.random.normal(key, shape, jnp.float32)
    if split:
        values = values * block_scale(key, shape, split, -0.22, 0.18)
    return jnp.clip(values, -reach, reach).astype(kind)


def setup_inputs(seed: int = 0) -> dict:
    seeds = jax.random.split(jax.random.key(seed), 33)
    tokens = gaussian(seeds[0], (TOKENS, D), 1.0, 6.0, ((0, 32),))
    cotangent = gaussian(seeds[1], (TOKENS, D), 1.0, 6.0, ((0, 32),))
    clip_lengths = draw_clip_lengths(jax.random.fold_in(seeds[32], 71), 0)
    clip_sets = place_ends(jax.random.randint(seeds[3], (NCLIPS,), 0, SETS), jax.random.fold_in(seeds[3], 1), 0, SETS - 1).astype(jnp.int32)
    clip_scales = jnp.clip(jnp.exp(math.log(2.0) - 1.3862944 * jax.random.uniform(seeds[4], (NCLIPS,), jnp.float32) ** block_scale(seeds[4], (NCLIPS,), ((0, 8),), -0.2, 0.2)), 0.5, 2.0)
    norm1_gain = jnp.clip(1.0 + 0.1 * jax.random.normal(seeds[5], (D,), jnp.float32), 0.5, 1.5)
    norm1_shift = gaussian(seeds[6], (D,), 0.5, 3.0, (), jnp.float32)
    w_query = gaussian(seeds[7], (D, D), D ** -0.5, 0.15625, ((0, 8), (1, 4)))
    query_bias = gaussian(seeds[8], (D,), 0.5, 3.0, ((0, 4),), jnp.float32)
    w_key = gaussian(seeds[9], (D, D), D ** -0.5, 0.15625, ((0, 8), (1, 4)))
    w_value = gaussian(seeds[10], (D, D), D ** -0.5, 0.15625, ((0, 8), (1, 4)))
    value_bias = gaussian(seeds[11], (D,), 0.5, 3.0, ((0, 4),), jnp.float32)
    w_out = gaussian(seeds[12], (D, D), (max(D // 64, 1)) ** -0.5, 1.25, ((0, 4), (1, 8)))
    out_bias = gaussian(seeds[13], (D,), 0.5, 3.0, (), jnp.float32)
    norm2_gain = jnp.clip(1.0 + 0.1 * jax.random.normal(seeds[14], (D,), jnp.float32), 0.5, 1.5)
    norm2_shift = gaussian(seeds[15], (D,), 0.5, 3.0, (), jnp.float32)
    w_fc1 = gaussian(seeds[16], (D, FF), D ** -0.5, 0.15625, ((0, 8), (1, 4)))
    fc1_bias = gaussian(seeds[17], (FF,), 0.5, 3.0, ((0, 4),), jnp.float32)
    w_fc2 = gaussian(seeds[18], (FF, D), FF ** -0.5, 0.078125, ((0, 4), (1, 8)))
    fc2_bias = gaussian(seeds[19], (D,), 0.5, 3.0, (), jnp.float32)
    query_down = gaussian(seeds[20], (SETS, D, RANK), D ** -0.5, 0.15625, ((1, 8),))
    query_up = gaussian(seeds[21], (SETS, RANK, D), 0.08, 0.5, ((1, 8), (2, 4)))
    key_down = gaussian(seeds[22], (SETS, D, RANK), D ** -0.5, 0.15625, ((1, 8),))
    key_up = gaussian(seeds[23], (SETS, RANK, D), 0.08, 0.5, ((1, 8), (2, 4)))
    value_down = gaussian(seeds[24], (SETS, D, RANK), D ** -0.5, 0.15625, ((1, 8),))
    value_up = gaussian(seeds[25], (SETS, RANK, D), 0.08, 0.5, ((1, 8), (2, 4)))
    out_down = gaussian(seeds[26], (SETS, D, RANK), (max(D // 64, 1)) ** -0.5, 1.25, ((1, 4), (2, 8)))
    out_up = gaussian(seeds[27], (SETS, RANK, D), 0.08, 0.5, ((2, 8),))
    fc1_down = gaussian(seeds[28], (SETS, D, RANK), D ** -0.5, 0.15625, ((1, 8),))
    fc1_up = gaussian(seeds[29], (SETS, RANK, FF), 0.08, 0.5, ((1, 8), (2, 4)))
    fc2_down = gaussian(seeds[30], (SETS, FF, RANK), FF ** -0.5, 0.078125, ((1, 4), (2, 8)))
    fc2_up = gaussian(seeds[31], (SETS, RANK, D), 0.08, 0.5, ((2, 8),))
    return {"tokens": tokens, "cotangent": cotangent, "clip_lengths": clip_lengths, "clip_sets": clip_sets, "clip_scales": clip_scales, "norm1_gain": norm1_gain, "norm1_shift": norm1_shift, "w_query": w_query, "query_bias": query_bias, "w_key": w_key, "w_value": w_value, "value_bias": value_bias, "w_out": w_out, "out_bias": out_bias, "norm2_gain": norm2_gain, "norm2_shift": norm2_shift, "w_fc1": w_fc1, "fc1_bias": fc1_bias, "w_fc2": w_fc2, "fc2_bias": fc2_bias, "query_down": query_down, "query_up": query_up, "key_down": key_down, "key_up": key_up, "value_down": value_down, "value_up": value_up, "out_down": out_down, "out_up": out_up, "fc1_down": fc1_down, "fc1_up": fc1_up, "fc2_down": fc2_down, "fc2_up": fc2_up}


HIGHEST = lax.Precision.HIGHEST
EPSILON = 1e-05
MASKED = -1000000000.0

@jax.custom_vjp
def low(v):
    return lax.optimization_barrier(v.astype(jnp.bfloat16)).astype(jnp.float32)

@jax.custom_vjp
def low_back(v):
    return v

def low_keep(v):
    return (low(v), None)

def low_pass(kept, grad):
    return (grad,)

def back_keep(v):
    return (v, None)

def back_low(kept, grad):
    return (low(grad),)
low.defvjp(low_keep, low_pass)
low_back.defvjp(back_keep, back_low)

def matmul(left_side, right_side):
    return jnp.dot(left_side, right_side, precision=HIGHEST)

def layer_norm(values, norm_gain, norm_shift):
    row_mean = lax.optimization_barrier(jnp.mean(values, axis=-1, keepdims=True))
    centred = values - row_mean
    row_var = lax.optimization_barrier(jnp.mean(centred * centred, axis=-1, keepdims=True))
    return centred * lax.rsqrt(row_var + EPSILON) * norm_gain + norm_shift

def adapter(hidden_state, down_table, up_table, selected_adapter, factor):
    return factor * matmul(matmul(hidden_state, down_table[selected_adapter]), up_table[selected_adapter])

def clip_forward(clip_tokens, adapters, frozen, length, factor, selected_adapter):
    query_down, query_up, key_down, key_up, value_down, value_up, out_down, out_up, fc1_down, fc1_up, fc2_down, fc2_up = adapters
    norm1_gain, norm1_shift, w_query, query_bias, w_key, w_value, value_bias, w_out, out_bias, norm2_gain, norm2_shift, w_fc1, fc1_bias, w_fc2, fc2_bias = frozen
    normed = low(layer_norm(clip_tokens, norm1_gain, norm1_shift))
    queries = low(low_back(matmul(normed, w_query) + query_bias + adapter(normed, query_down, query_up, selected_adapter, factor)))
    keys_all = low(low_back(matmul(normed, w_key) + adapter(normed, key_down, key_up, selected_adapter, factor)))
    values_all = low(low_back(matmul(normed, w_value) + value_bias + adapter(normed, value_down, value_up, selected_adapter, factor)))
    query_heads = queries.reshape(LEN, HEADS, HEAD_DIM)
    key_heads = keys_all.reshape(LEN, HEADS, HEAD_DIM)
    value_heads = values_all.reshape(LEN, HEADS, HEAD_DIM)
    scores = low_back(jnp.einsum('qhd,khd->hqk', query_heads, key_heads, precision=HIGHEST) * HEAD_DIM ** (-0.5))
    key_valid = jnp.arange(LEN, dtype=jnp.int32) < length
    scores = jnp.where(key_valid[None, None, :], scores, MASKED)
    row_top = lax.optimization_barrier(jnp.max(scores, axis=-1, keepdims=True))
    exp_terms = jnp.exp(scores - row_top)
    attn_probs = low(exp_terms / lax.optimization_barrier(jnp.sum(exp_terms, axis=-1, keepdims=True)))
    attended = jnp.einsum('hqk,khd->qhd', attn_probs, value_heads, precision=HIGHEST).reshape(LEN, D)
    attended = low(low_back(attended))
    branch = low_back(matmul(attended, w_out) + adapter(attended, out_down, out_up, selected_adapter, factor))
    middle = clip_tokens + branch + out_bias
    normed_mlp = low(layer_norm(middle, norm2_gain, norm2_shift))
    pre_act = low_back(matmul(normed_mlp, w_fc1) + fc1_bias + adapter(normed_mlp, fc1_down, fc1_up, selected_adapter, factor))
    activated = low(jax.nn.gelu(pre_act, approximate=False))
    branch_mlp = low_back(matmul(activated, w_fc2) + adapter(activated, fc2_down, fc2_up, selected_adapter, factor))
    return middle + branch_mlp + fc2_bias

def reference(tokens, cotangent, clip_lengths, clip_sets, clip_scales, norm1_gain, norm1_shift, w_query, query_bias, w_key, w_value, value_bias, w_out, out_bias, norm2_gain, norm2_shift, w_fc1, fc1_bias, w_fc2, fc2_bias, query_down, query_up, key_down, key_up, value_down, value_up, out_down, out_up, fc1_down, fc1_up, fc2_down, fc2_up):
    frozen = tuple((member.astype(jnp.float32) for member in (norm1_gain, norm1_shift, w_query, query_bias, w_key, w_value, value_bias, w_out, out_bias, norm2_gain, norm2_shift, w_fc1, fc1_bias, w_fc2, fc2_bias)))
    adapters = tuple((member.astype(jnp.float32) for member in (query_down, query_up, key_down, key_up, value_down, value_up, out_down, out_up, fc1_down, fc1_up, fc2_down, fc2_up)))
    token_clips = tokens.astype(jnp.float32).reshape(NCLIPS, LEN, D)
    cot_clips = cotangent.astype(jnp.float32).reshape(NCLIPS, LEN, D)
    zero_grads = tuple((jnp.zeros_like(member) for member in adapters))

    def scan_step(totals, inputs):
        clip_tokens, clip_cot, length, selected_adapter, factor = inputs

        def forward(values, tables):
            return clip_forward(values, tables, frozen, length, factor, selected_adapter)
        result, pullback = jax.vjp(forward, clip_tokens, adapters)
        token_grad, table_grads = pullback(clip_cot)
        totals = tuple((first_part + second_part for first_part, second_part in zip(totals, table_grads)))
        return (totals, (result, token_grad))
    totals, (results, token_grads) = lax.scan(scan_step, zero_grads, (token_clips, cot_clips, clip_lengths, clip_sets, clip_scales))
    return (results.reshape(TOKENS, D).astype(jnp.bfloat16), token_grads.reshape(TOKENS, D).astype(jnp.bfloat16), totals[0], totals[1], totals[2], totals[3], totals[4], totals[5], totals[6], totals[7], totals[8], totals[9], totals[10], totals[11])
```

```python
import functools
import math

import jax
import jax.numpy as jnp
from jax import lax
from jax.experimental import pallas as pl
from jax.experimental.pallas import tpu as pltpu
from jax.sharding import PartitionSpec as P

D = 1280
SETS = 8
RANK = 16
HEAD_DIM = 80
EPSILON = 1e-05
LOG2E = 1.4426950408889634
LOW = -1e30
F32 = jnp.float32
BF = jnp.bfloat16
BOTH = ("rows", "cols")


def dot(a, b):
    return lax.dot_general(a, b, (((1,), (0,)), ((), ())), preferred_element_type=F32)


def dot_t(a, b):
    return lax.dot_general(a, b, (((1,), (1,)), ((), ())), preferred_element_type=F32)


def token_sum(a, b):
    return dot(a.T.astype(BF), b)


def norm_parts(x):
    mean = jnp.mean(x, axis=-1, keepdims=True)
    centred = x - mean
    inverse = lax.rsqrt(jnp.mean(centred * centred, axis=-1, keepdims=True) + EPSILON)
    return centred * inverse, inverse


def params(n, limit=60 << 20):
    return pltpu.CompilerParams(
        dimension_semantics=("arbitrary",) * n, vmem_limit_bytes=limit
    )


def cost(flops, nbytes, trans=0):
    return pl.CostEstimate(flops=int(flops), bytes_accessed=int(nbytes), transcendentals=int(trans))


def attend_kernel(hh, length, qb, kb, lens, x_ref, o_ref, lse_ref, k_scr, vt_scr, acc, m_scr, l_scr):
    p = pl.program_id(0)
    qi = pl.program_id(1)
    w = hh * HEAD_DIM
    c = HEAD_DIM**-0.5 * LOG2E

    @pl.when(qi == 0)
    def _():
        vt_scr[...] = x_ref[0, :, 2 * w : 3 * w].T
        for h in range(hh):
            k_scr[h] = x_ref[0, :, w + h * HEAD_DIM : w + (h + 1) * HEAD_DIM]

    size = lens[p]
    block = x_ref[0, pl.ds(pl.multiple_of(qi * qb, qb), qb), 0:w]
    qs = [block[:, h * HEAD_DIM : (h + 1) * HEAD_DIM] for h in range(hh)]
    m_scr[...] = jnp.full_like(m_scr, LOW)
    l_scr[...] = jnp.zeros_like(l_scr)
    acc[...] = jnp.zeros_like(acc)

    def chunk(i, masked):
        r0 = pl.multiple_of(i * kb, kb)
        for h in range(hh):
            s = dot_t(k_scr[h, pl.ds(r0, kb), :], qs[h])
            if masked:
                keys = lax.broadcasted_iota(jnp.int32, (kb, qb), 0) + i * kb
                s = jnp.where(keys < size, s, LOW)
            old = m_scr[h : h + 1]
            top = jnp.maximum(old, jnp.max(s, axis=0, keepdims=True))
            probs = jnp.exp2((s - top) * c)
            shrink = jnp.exp2((old - top) * c)
            l_scr[h : h + 1] = l_scr[h : h + 1] * shrink + jnp.sum(probs, axis=0, keepdims=True)
            m_scr[h : h + 1] = top
            acc[h] = acc[h] * shrink + dot(
                vt_scr[h * HEAD_DIM : (h + 1) * HEAD_DIM, pl.ds(r0, kb)], probs.astype(BF)
            )

    full = size // kb

    def step(i, carry):
        chunk(i, False)
        return carry

    lax.fori_loop(0, full, step, 0)

    @pl.when(full * kb < size)
    def _():
        chunk(full, True)

    outs = [acc[h] * (1.0 / l_scr[h : h + 1]) for h in range(hh)]
    o_ref[0] = jnp.concatenate(outs, axis=0).T.astype(BF)
    lse_ref[0] = m_scr[0:hh] * c + jnp.log2(l_scr[0:hh])


def attend(x, lens, hh):
    problems, length, w3 = x.shape
    w = hh * HEAD_DIM
    qb = math.gcd(length, 512)
    kb = math.gcd(length, 768)
    return pl.pallas_call(
        functools.partial(attend_kernel, hh, length, qb, kb),
        out_shape=(
            jax.ShapeDtypeStruct((problems, length, w), BF),
            jax.ShapeDtypeStruct((problems, hh, length), F32),
        ),
        grid_spec=pltpu.PrefetchScalarGridSpec(
            num_scalar_prefetch=1,
            grid=(problems, length // qb),
            in_specs=[pl.BlockSpec((1, length, w3), lambda p, q, l: (p, 0, 0))],
            out_specs=[
                pl.BlockSpec((1, qb, w), lambda p, q, l: (p, q, 0)),
                pl.BlockSpec((1, hh, qb), lambda p, q, l: (p, 0, q)),
            ],
            scratch_shapes=[
                pltpu.VMEM((hh, length, HEAD_DIM), BF),
                pltpu.VMEM((w, length), BF),
                pltpu.VMEM((hh, HEAD_DIM, qb), F32),
                pltpu.VMEM((max(8, hh), qb), F32),
                pltpu.VMEM((max(8, hh), qb), F32),
            ],
        ),
        compiler_params=params(2),
        cost_estimate=cost(
            problems * hh * 4 * length * length * 256, x.size * 3, problems * hh * length * length
        ),
        name="attend",
    )(lens, x)


def attend_back_kernel(
    hh, length, qb, kb, lens, x_ref, o_ref, do_ref, lse_ref, dx_ref, k_scr, v_scr, kt_scr, dk, dv, dqt
):
    p = pl.program_id(0)
    qi = pl.program_id(1)
    w = hh * HEAD_DIM
    scale = HEAD_DIM**-0.5
    c = scale * LOG2E

    @pl.when(qi == 0)
    def _():
        kt_scr[...] = x_ref[0, :, w : 2 * w].T
        for h in range(hh):
            k_scr[h] = x_ref[0, :, w + h * HEAD_DIM : w + (h + 1) * HEAD_DIM]
            v_scr[h] = x_ref[0, :, 2 * w + h * HEAD_DIM : 2 * w + (h + 1) * HEAD_DIM]
        dk[...] = jnp.zeros_like(dk)
        dv[...] = jnp.zeros_like(dv)

    size = lens[p]
    rows = pl.ds(pl.multiple_of(qi * qb, qb), qb)
    block = x_ref[0, rows, 0:w]
    qs = [block[:, h * HEAD_DIM : (h + 1) * HEAD_DIM] for h in range(hh)]
    do = do_ref[0]
    dos = [do[:, h * HEAD_DIM : (h + 1) * HEAD_DIM] for h in range(hh)]
    prod = (do.astype(F32) * o_ref[0].astype(F32)).T
    inner = [
        jnp.sum(prod[h * HEAD_DIM : (h + 1) * HEAD_DIM], axis=0, keepdims=True) for h in range(hh)
    ]
    dqt[...] = jnp.zeros_like(dqt)

    def chunk(i, masked):
        keys_at = pl.ds(pl.multiple_of(i * kb, kb), kb)
        for h in range(hh):
            s = dot_t(k_scr[h, keys_at, :], qs[h])
            probs = jnp.exp2(s * c - lse_ref[0, h : h + 1])
            if masked:
                keys = lax.broadcasted_iota(jnp.int32, (kb, qb), 0) + i * kb
                probs = jnp.where(keys < size, probs, 0.0)
            dp = dot_t(v_scr[h, keys_at, :], dos[h])
            ds = (probs * (dp - inner[h])).astype(BF)
            dv[h, keys_at, :] += dot(probs.astype(BF), dos[h])
            dk[h, keys_at, :] += dot(ds, qs[h])
            dqt[h] += dot(kt_scr[h * HEAD_DIM : (h + 1) * HEAD_DIM, keys_at], ds)

    full = size // kb

    def step(i, carry):
        chunk(i, False)
        return carry

    lax.fori_loop(0, full, step, 0)

    @pl.when(full * kb < size)
    def _():
        chunk(full, True)

    dq = jnp.concatenate([dqt[h] for h in range(hh)], axis=0).T * scale
    dx_ref[0, rows, 0:w] = dq.astype(BF)

    @pl.when(qi == pl.num_programs(1) - 1)
    def _():
        for h in range(hh):
            dx_ref[0, :, w + h * HEAD_DIM : w + (h + 1) * HEAD_DIM] = (dk[h] * scale).astype(BF)
            dx_ref[0, :, 2 * w + h * HEAD_DIM : 2 * w + (h + 1) * HEAD_DIM] = dv[h].astype(BF)


def attend_back(x, o, do, lse, lens, hh):
    problems, length, w3 = x.shape
    w = hh * HEAD_DIM
    qb = math.gcd(length, 512)
    kb = math.gcd(length, 512)
    return pl.pallas_call(
        functools.partial(attend_back_kernel, hh, length, qb, kb),
        out_shape=jax.ShapeDtypeStruct((problems, length, w3), BF),
        grid_spec=pltpu.PrefetchScalarGridSpec(
            num_scalar_prefetch=1,
            grid=(problems, length // qb),
            in_specs=[
                pl.BlockSpec((1, length, w3), lambda p, q, l: (p, 0, 0)),
                pl.BlockSpec((1, qb, w), lambda p, q, l: (p, q, 0)),
                pl.BlockSpec((1, qb, w), lambda p, q, l: (p, q, 0)),
                pl.BlockSpec((1, hh, qb), lambda p, q, l: (p, 0, q)),
            ],
            out_specs=pl.BlockSpec((1, length, w3), lambda p, q, l: (p, 0, 0)),
            scratch_shapes=[
                pltpu.VMEM((hh, length, HEAD_DIM), BF),
                pltpu.VMEM((hh, length, HEAD_DIM), BF),
                pltpu.VMEM((w, length), BF),
                pltpu.VMEM((hh, length, HEAD_DIM), F32),
                pltpu.VMEM((hh, length, HEAD_DIM), F32),
                pltpu.VMEM((hh, HEAD_DIM, qb), F32),
            ],
        ),
        compiler_params=params(2),
        cost_estimate=cost(
            problems * hh * 10 * length * length * 256, x.size * 6, problems * hh * length * length
        ),
        name="attend_back",
    )(lens, x, o, do, lse)


def spread(up3, width):
    piece = lax.broadcasted_iota(jnp.int32, up3.shape, 0) // RANK
    return jnp.concatenate([jnp.where(piece == j, up3, jnp.zeros_like(up3)) for j in range(3)], axis=1)


def project_kernel(
    tm, width, sets, scales, x_ref, gain, shift, w_ref, bias, down, up, normed_ref, ranks_ref, y_ref, n_scr, r_scr
):
    c = pl.program_id(0)
    m = pl.program_id(1)
    rows = pl.ds(pl.multiple_of(m * tm, tm), tm)

    @pl.when(c == 0)
    def _():
        unit, _ = norm_parts(x_ref[...].astype(F32))
        normed = (unit * gain[...] + shift[...]).astype(BF)
        n_scr[rows, :] = normed
        normed_ref[...] = normed
        rank = (dot_t(normed, down[0]) * scales[m]).astype(BF)
        r_scr[rows, :] = rank
        ranks_ref[...] = rank

    y = dot(n_scr[rows, :], w_ref[:, 0].reshape(D, 3 * width))
    y += dot(r_scr[rows, :], spread(up[0, 0], width))
    y_ref[0] = (y + bias[0]).astype(BF)


def project(tokens, gain, shift, gathered, bias, down, up, sets, scales, tm):
    own = tokens.shape[0]
    rr, nc, _, w3 = gathered.shape
    width = w3 // 3
    first = lambda c, m, s, a: (jnp.where(c == 0, m, own // tm - 1), 0)
    return pl.pallas_call(
        functools.partial(project_kernel, tm, width),
        out_shape=(
            jax.ShapeDtypeStruct((own, D), BF),
            jax.ShapeDtypeStruct((own, 3 * RANK), BF),
            jax.ShapeDtypeStruct((nc, own, w3), BF),
        ),
        grid_spec=pltpu.PrefetchScalarGridSpec(
            num_scalar_prefetch=2,
            grid=(nc, own // tm),
            in_specs=[
                pl.BlockSpec((tm, D), first),
                pl.BlockSpec((1, D), lambda c, m, s, a: (0, 0)),
                pl.BlockSpec((1, D), lambda c, m, s, a: (0, 0)),
                pl.BlockSpec((rr, 1, D // rr, w3), lambda c, m, s, a: (0, c, 0, 0)),
                pl.BlockSpec((1, 1, w3), lambda c, m, s, a: (c, 0, 0)),
                pl.BlockSpec((1, 3 * RANK, D), lambda c, m, s, a: (s[m], 0, 0)),
                pl.BlockSpec((1, 1, 3 * RANK, width), lambda c, m, s, a: (s[m], c, 0, 0)),
            ],
            out_specs=[
                pl.BlockSpec((tm, D), first),
                pl.BlockSpec((tm, 3 * RANK), first),
                pl.BlockSpec((1, tm, w3), lambda c, m, s, a: (c, m, 0)),
            ],
            scratch_shapes=[pltpu.VMEM((own, D), BF), pltpu.VMEM((own, 3 * RANK), BF)],
        ),
        compiler_params=params(2),
        cost_estimate=cost(2 * own * D * nc * w3 * 1.3, D * nc * w3 * 2 + own * (2 * D + nc * w3) * 2),
        name="project",
    )(sets, scales, tokens, gain, shift, gathered, bias, down, up)


def project_back_kernel(
    tm,
    width,
    sets,
    scales,
    dy_ref,
    w_ref,
    up,
    down,
    x_ref,
    normed_ref,
    ranks_ref,
    gm_ref,
    gain,
    gt_ref,
    gup_ref,
    gdown_ref,
    acc,
    racc,
):
    c = pl.program_id(0)
    m = pl.program_id(1)
    last = c == pl.num_programs(0) - 1
    rows = pl.ds(pl.multiple_of(m * tm, tm), tm)
    which = sets[m]
    dy = dy_ref[0]
    part = dot_t(dy, w_ref[:, 0].reshape(D, 3 * width))
    rpart = dot_t(dy, spread(up[0, 0], width))

    @pl.when(c == 0)
    def _():
        acc[rows, :] = part
        racc[rows, :] = rpart

    @pl.when(c > 0)
    def _():
        acc[rows, :] += part
        racc[rows, :] += rpart

    @pl.when(m == 0)
    def _():
        gup_ref[...] = jnp.zeros_like(gup_ref)

    @pl.when((m == 0) & (c == 0))
    def _():
        gdown_ref[...] = jnp.zeros_like(gdown_ref)

    wide = token_sum(ranks_ref[...].astype(F32), dy)
    gup_ref[which, 0] += jnp.concatenate(
        [wide[j * RANK : (j + 1) * RANK, j * width : (j + 1) * width] for j in range(3)], axis=0
    )

    @pl.when(last)
    def _():
        grank = racc[rows, :] * scales[m]
        grad = acc[rows, :] + dot(grank.astype(BF), down[0])
        gdown_ref[which] += token_sum(grank, normed_ref[...])
        unit, inverse = norm_parts(x_ref[...].astype(F32))
        e = grad * gain[...]
        mean = jnp.mean(e, axis=-1, keepdims=True)
        second = jnp.mean(e * unit, axis=-1, keepdims=True)
        gt_ref[...] = (gm_ref[...] + (e - mean - unit * second) * inverse).astype(BF)


def project_back(dy, gathered, up, down, tokens, normed, ranks, grad_middle, gain, sets, scales, tm):
    own = tokens.shape[0]
    rr, nc, _, w3 = gathered.shape
    width = w3 // 3
    final = lambda c, m, s, a: (jnp.where(c == nc - 1, m, 0), 0)
    return pl.pallas_call(
        functools.partial(project_back_kernel, tm, width),
        out_shape=(
            jax.ShapeDtypeStruct((own, D), BF),
            jax.ShapeDtypeStruct((SETS, nc, 3 * RANK, width), F32),
            jax.ShapeDtypeStruct((SETS, 3 * RANK, D), F32),
        ),
        grid_spec=pltpu.PrefetchScalarGridSpec(
            num_scalar_prefetch=2,
            grid=(nc, own // tm),
            in_specs=[
                pl.BlockSpec((1, tm, w3), lambda c, m, s, a: (c, m, 0)),
                pl.BlockSpec((rr, 1, D // rr, w3), lambda c, m, s, a: (0, c, 0, 0)),
                pl.BlockSpec((1, 1, 3 * RANK, width), lambda c, m, s, a: (s[m], c, 0, 0)),
                pl.BlockSpec((1, 3 * RANK, D), lambda c, m, s, a: (s[m], 0, 0)),
                pl.BlockSpec((tm, D), final),
                pl.BlockSpec((tm, D), final),
                pl.BlockSpec((tm, 3 * RANK), lambda c, m, s, a: (m, 0)),
                pl.BlockSpec((tm, D), final),
                pl.BlockSpec((1, D), lambda c, m, s, a: (0, 0)),
            ],
            out_specs=[
                pl.BlockSpec((tm, D), final),
                pl.BlockSpec((SETS, 1, 3 * RANK, width), lambda c, m, s, a: (0, c, 0, 0)),
                pl.BlockSpec((SETS, 3 * RANK, D), lambda c, m, s, a: (0, 0, 0)),
            ],
            scratch_shapes=[pltpu.VMEM((own, D), F32), pltpu.VMEM((own, 3 * RANK), F32)],
        ),
        compiler_params=params(2),
        cost_estimate=cost(2 * own * D * nc * w3 * 1.5, D * nc * w3 * 2 + own * (4 * D + nc * w3) * 2),
        name="project_back",
    )(sets, scales, dy, gathered, up, down, tokens, normed, ranks, grad_middle, gain)


def out_kernel(
    nc,
    sets,
    scales,
    att_ref,
    x_ref,
    w_ref,
    bias,
    odown,
    oup,
    gain,
    shift,
    fdown,
    att_out,
    middle_ref,
    normed_ref,
    ro_ref,
    r1_ref,
):
    m = pl.program_id(0)
    a = scales[m]
    att = jnp.concatenate([att_ref[i] for i in range(nc)], axis=1)
    att_out[...] = att
    ro = (dot_t(att, odown[0]) * a).astype(BF)
    ro_ref[...] = ro
    middle = x_ref[...].astype(F32) + dot_t(att, w_ref[...]) + dot(ro, oup[0]) + bias[...]
    middle_ref[...] = middle
    unit, _ = norm_parts(middle)
    normed = (unit * gain[...] + shift[...]).astype(BF)
    normed_ref[...] = normed
    r1_ref[...] = (dot_t(normed, fdown[0]) * a).astype(BF)


def out_project(att, tokens, wo_t, bias, odown, oup, gain, shift, fdown, sets, scales, tm):
    nc, own, width = att.shape
    row = lambda m, s, a: (m, 0)
    flat = lambda m, s, a: (0, 0)
    table = lambda m, s, a: (s[m], 0, 0)
    return pl.pallas_call(
        functools.partial(out_kernel, nc),
        out_shape=(
            jax.ShapeDtypeStruct((own, D), BF),
            jax.ShapeDtypeStruct((own, D), F32),
            jax.ShapeDtypeStruct((own, D), BF),
            jax.ShapeDtypeStruct((own, RANK), BF),
            jax.ShapeDtypeStruct((own, RANK), BF),
        ),
        grid_spec=pltpu.PrefetchScalarGridSpec(
            num_scalar_prefetch=2,
            grid=(own // tm,),
            in_specs=[
                pl.BlockSpec((nc, tm, width), lambda m, s, a: (0, m, 0)),
                pl.BlockSpec((tm, D), row),
                pl.BlockSpec((D, D), flat),
                pl.BlockSpec((1, D), flat),
                pl.BlockSpec((1, RANK, D), table),
                pl.BlockSpec((1, RANK, D), table),
                pl.BlockSpec((1, D), flat),
                pl.BlockSpec((1, D), flat),
                pl.BlockSpec((1, RANK, D), table),
            ],
            out_specs=[
                pl.BlockSpec((tm, D), row),
                pl.BlockSpec((tm, D), row),
                pl.BlockSpec((tm, D), row),
                pl.BlockSpec((tm, RANK), row),
                pl.BlockSpec((tm, RANK), row),
            ],
        ),
        compiler_params=params(1),
        cost_estimate=cost(2 * own * D * D * 1.5, D * D * 2 + own * D * 12),
        name="out_project",
    )(sets, scales, att, tokens, wo_t, bias, odown, oup, gain, shift, fdown)


def out_back_kernel(nc, width, sets, scales, gb_ref, w_ref, oup, odown, att_ref, ro_ref, ga_ref, gup_ref, gdown_ref):
    m = pl.program_id(0)
    which = sets[m]

    @pl.when(m == 0)
    def _():
        gup_ref[...] = jnp.zeros_like(gup_ref)
        gdown_ref[...] = jnp.zeros_like(gdown_ref)

    gb = gb_ref[...]
    gro = dot_t(gb, oup[0]) * scales[m]
    ga = (dot(gb, w_ref[...]) + dot(gro.astype(BF), odown[0])).astype(BF)
    for i in range(nc):
        ga_ref[i] = ga[:, i * width : (i + 1) * width]
    gup_ref[which] += token_sum(ro_ref[...].astype(F32), gb)
    gdown_ref[which] += token_sum(gro, att_ref[...])


def out_back(gb, wo_t, oup, odown, att, ro, sets, scales, tm, nc):
    own = gb.shape[0]
    width = D // nc
    row = lambda m, s, a: (m, 0)
    table = lambda m, s, a: (s[m], 0, 0)
    whole = lambda m, s, a: (0, 0, 0)
    return pl.pallas_call(
        functools.partial(out_back_kernel, nc, width),
        out_shape=(
            jax.ShapeDtypeStruct((nc, own, width), BF),
            jax.ShapeDtypeStruct((SETS, RANK, D), F32),
            jax.ShapeDtypeStruct((SETS, RANK, D), F32),
        ),
        grid_spec=pltpu.PrefetchScalarGridSpec(
            num_scalar_prefetch=2,
            grid=(own // tm,),
            in_specs=[
                pl.BlockSpec((tm, D), row),
                pl.BlockSpec((D, D), lambda m, s, a: (0, 0)),
                pl.BlockSpec((1, RANK, D), table),
                pl.BlockSpec((1, RANK, D), table),
                pl.BlockSpec((tm, D), row),
                pl.BlockSpec((tm, RANK), row),
            ],
            out_specs=[
                pl.BlockSpec((nc, tm, width), lambda m, s, a: (0, m, 0)),
                pl.BlockSpec((SETS, RANK, D), whole),
                pl.BlockSpec((SETS, RANK, D), whole),
            ],
        ),
        compiler_params=params(1),
        cost_estimate=cost(2 * own * D * D * 1.5, D * D * 2 + own * D * 6),
        name="out_back",
    )(sets, scales, gb, wo_t, oup, odown, att, ro)


def mlp_kernel(
    tm,
    sets,
    scales,
    n_ref,
    g_ref,
    mid_ref,
    w1_ref,
    w2_ref,
    b1,
    f1up,
    f2down,
    f2up,
    f1down,
    r1_ref,
    bias2,
    gain,
    out_ref,
    gm_ref,
    gb_ref,
    gf1up,
    gf2down,
    gf2up,
    gf1down,
    acc,
    gacc,
    r2acc,
    gr1acc,
    gr2,
):
    c = pl.program_id(0)
    m = pl.program_id(1)
    rows = pl.ds(pl.multiple_of(m * tm, tm), tm)
    which = sets[m]
    a = scales[m]
    g = g_ref[...]
    normed = n_ref[...]
    hidden = w1_ref.shape[-1]

    @pl.when(c == 0)
    def _():
        gr2[rows, :] = dot_t(g, f2up[0]) * a
        acc[rows, :] = jnp.zeros((tm, D), F32)
        gacc[rows, :] = jnp.zeros((tm, D), F32)
        r2acc[rows, :] = jnp.zeros((tm, RANK), F32)
        gr1acc[rows, :] = jnp.zeros((tm, RANK), F32)

    @pl.when(m == 0)
    def _():
        gf1up[...] = jnp.zeros_like(gf1up)
        gf2down[...] = jnp.zeros_like(gf2down)

    @pl.when((m == 0) & (c == 0))
    def _():
        gf2up[...] = jnp.zeros_like(gf2up)
        gf1down[...] = jnp.zeros_like(gf1down)

    w1 = w1_ref[:, 0].reshape(D, hidden)
    w2 = w2_ref[:, 0].reshape(D, hidden)
    r1 = r1_ref[...]
    grank2 = gr2[rows, :]
    pre = dot(normed, w1) + dot(r1, f1up[0, 0]) + b1[0]
    phi_up = 0.5 + 0.5 * lax.erf(pre * (0.5**0.5))
    density = jnp.exp(pre * pre * -0.5) * ((2.0 * math.pi) ** -0.5)
    act = (pre * phi_up).astype(BF)
    slope = phi_up + pre * density
    gact = dot(g, w2) + dot(grank2.astype(BF), f2down[0, 0])
    gpre = (gact * slope).astype(BF)
    acc[rows, :] += dot_t(act, w2)
    r2acc[rows, :] += dot_t(act, f2down[0, 0])
    gacc[rows, :] += dot_t(gpre, w1)
    gr1acc[rows, :] += dot_t(gpre, f1up[0, 0])
    gf2down[which, 0] += token_sum(grank2, act)
    gf1up[which, 0] += token_sum(r1.astype(F32), gpre)

    @pl.when(c == pl.num_programs(0) - 1)
    def _():
        r2 = r2acc[rows, :] * a
        middle = mid_ref[...]
        out_ref[...] = (middle + acc[rows, :] + dot(r2.astype(BF), f2up[0]) + bias2[...]).astype(BF)
        gf2up[which] += token_sum(r2, g)
        gr1 = gr1acc[rows, :] * a
        e = (gacc[rows, :] + dot(gr1.astype(BF), f1down[0])) * gain[...]
        gf1down[which] += token_sum(gr1, normed)
        unit, inverse = norm_parts(middle)
        mean = jnp.mean(e, axis=-1, keepdims=True)
        second = jnp.mean(e * unit, axis=-1, keepdims=True)
        gm = g.astype(F32) + (e - mean - unit * second) * inverse
        gm_ref[...] = gm
        gb_ref[...] = gm.astype(BF)


def mlp(normed, g, middle, gathered, b1, f1up, f2down, f2up, f1down, r1, bias2, gain, sets, scales, tm):
    own = g.shape[0]
    rr, nc, _, hidden = gathered.shape
    row = lambda c, m, s, a: (m, 0)
    final = lambda c, m, s, a: (jnp.where(c == nc - 1, m, 0), 0)
    flat = lambda c, m, s, a: (0, 0)
    table = lambda c, m, s, a: (s[m], 0, 0)
    ctable = lambda c, m, s, a: (s[m], c, 0, 0)
    whole = lambda c, m, s, a: (0, 0, 0)
    cwhole = lambda c, m, s, a: (0, c, 0, 0)
    wblock = (rr, 1, D // rr, hidden)
    return pl.pallas_call(
        functools.partial(mlp_kernel, tm),
        out_shape=(
            jax.ShapeDtypeStruct((own, D), BF),
            jax.ShapeDtypeStruct((own, D), F32),
            jax.ShapeDtypeStruct((own, D), BF),
            jax.ShapeDtypeStruct((SETS, nc, RANK, hidden), F32),
            jax.ShapeDtypeStruct((SETS, nc, RANK, hidden), F32),
            jax.ShapeDtypeStruct((SETS, RANK, D), F32),
            jax.ShapeDtypeStruct((SETS, RANK, D), F32),
        ),
        grid_spec=pltpu.PrefetchScalarGridSpec(
            num_scalar_prefetch=2,
            grid=(nc, own // tm),
            in_specs=[
                pl.BlockSpec((tm, D), row),
                pl.BlockSpec((tm, D), row),
                pl.BlockSpec((tm, D), final),
                pl.BlockSpec(wblock, lambda c, m, s, a: (0, c, 0, 0)),
                pl.BlockSpec(wblock, lambda c, m, s, a: (0, c, 1, 0)),
                pl.BlockSpec((1, 1, hidden), lambda c, m, s, a: (c, 0, 0)),
                pl.BlockSpec((1, 1, RANK, hidden), ctable),
                pl.BlockSpec((1, 1, RANK, hidden), ctable),
                pl.BlockSpec((1, RANK, D), table),
                pl.BlockSpec((1, RANK, D), table),
                pl.BlockSpec((tm, RANK), row),
                pl.BlockSpec((1, D), flat),
                pl.BlockSpec((1, D), flat),
            ],
            out_specs=[
                pl.BlockSpec((tm, D), final),
                pl.BlockSpec((tm, D), final),
                pl.BlockSpec((tm, D), final),
                pl.BlockSpec((SETS, 1, RANK, hidden), cwhole),
                pl.BlockSpec((SETS, 1, RANK, hidden), cwhole),
                pl.BlockSpec((SETS, RANK, D), whole),
                pl.BlockSpec((SETS, RANK, D), whole),
            ],
            scratch_shapes=[
                pltpu.VMEM((own, D), F32),
                pltpu.VMEM((own, D), F32),
                pltpu.VMEM((own, RANK), F32),
                pltpu.VMEM((own, RANK), F32),
                pltpu.VMEM((own, RANK), F32),
            ],
        ),
        compiler_params=params(2, 67043328),
        cost_estimate=cost(8 * own * D * nc * hidden * 1.2, D * nc * hidden * 4 + own * D * 30, own * nc * hidden * 2),
        name="mlp",
    )(sets, scales, normed, g, middle, gathered, gathered, b1, f1up, f2down, f2up, f1down, r1, bias2, gain)


def pick(flag, first, second):
    return jnp.where(flag, first, second)


class Exchange:
    def __init__(self, nc, own, clips, clip_len):
        self.nc, self.own, self.clips, self.clip_len = nc, own, clips, clip_len
        self.local = nc == 4 and clips == 3 and 2 * own * 2 == clips * clip_len
        col = lax.axis_index("cols")
        self.y, self.k = col // 2, col % 2
        self.holder = self.y != self.k

    def lens(self, lengths):
        if not self.local:
            return (lengths,)
        mine = pick(self.y == 0, lengths[0], lengths[2])
        return (jnp.stack([mine, mine]), lengths[1:2])

    def to_heads(self, v):
        if not self.local:
            moved = lax.all_to_all(v, "cols", 0, 0, tiled=True)
            return (moved.reshape(self.clips, self.clip_len, v.shape[-1]),)
        y, k, own, half = self.y, self.k, self.own, self.clip_len // 2
        f = v.shape[-1]
        start = pick(k == 1, own - half, 0)
        one = lax.dynamic_slice(v, (2 * k + 1 - y, start, 0), (1, half, f))
        two = lax.dynamic_slice(v, (2 * (1 - k) + 1 - y, start, 0), (1, half, f))
        got_one = lax.ppermute(one, "cols", [(1, 3), (2, 0)])
        got_two = lax.ppermute(two, "cols", [(1, 2), (2, 1)])
        away = lax.dynamic_slice(v, (2 * (1 - k), 0, 0), (2, own, f))
        mine = lax.dynamic_slice(v, (2 * k, 0, 0), (2, own, f))
        got = lax.ppermute(away, "cols", [(i, i ^ 1) for i in range(4)])
        chip = jnp.concatenate([pick(k == 0, mine, got), pick(k == 0, got, mine)], axis=1)
        clip = lax.dynamic_slice(chip, (0, y * half, 0), (2, self.clip_len, f))
        near = lax.dynamic_slice(chip, (y, (1 - y) * self.clip_len, 0), (1, half, f))
        far = pick(self.holder, got_two, got_one)
        shared = jnp.concatenate([pick(y == 0, near, far), pick(y == 0, far, near)], axis=1)
        return (clip, shared)

    def from_heads(self, parts):
        if not self.local:
            (v,) = parts
            return lax.all_to_all(v.reshape(self.nc, self.own, v.shape[-1]), "cols", 0, 0, tiled=True)
        clip, shared = parts
        y, k, own, half = self.y, self.k, self.own, self.clip_len // 2
        f = clip.shape[-1]
        far = lax.dynamic_slice(shared, (0, (1 - y) * half, 0), (1, half, f))
        near = lax.dynamic_slice(shared, (0, y * half, 0), (1, half, f))
        got_one = lax.ppermute(far, "cols", [(3, 1), (0, 2)])
        got_two = lax.ppermute(far, "cols", [(2, 1), (1, 2)])
        both = jnp.concatenate([near, near], axis=0)
        chip = jnp.concatenate(
            [
                pick(y == 0, clip[:, :half], both),
                clip[:, half:] * 0 + pick(y == 0, clip[:, half:], clip[:, :half]),
                pick(y == 0, both, clip[:, half:]),
            ],
            axis=1,
        )
        mine = lax.dynamic_slice(chip, (0, k * own, 0), (2, own, f))
        away = lax.dynamic_slice(chip, (0, (1 - k) * own, 0), (2, own, f))
        got = lax.ppermute(away, "cols", [(i, i ^ 1) for i in range(4)])
        low, high = pick(k == 0, mine, got), pick(k == 0, got, mine)
        out = jnp.concatenate([low, high], axis=0)
        row = lax.broadcasted_iota(jnp.int32, (own, 1), 0)
        inside = self.holder & pick(k == 1, row >= own - half, row < half)
        pad = ((0, 0), (own - half, 0), (0, 0))
        end = ((0, 0), (0, own - half), (0, 0))
        place = lambda v: pick(k == 1, jnp.pad(v, pad), jnp.pad(v, end))[0]
        one, two = place(got_one), place(got_two)
        pieces = []
        for c in range(4):
            from_one = inside & (2 * k + 1 - y == c)
            from_two = inside & (2 * (1 - k) + 1 - y == c)
            pieces.append(pick(from_one, one, pick(from_two, two, out[c])))
        return jnp.stack(pieces)


def pack(pieces, lanes):
    flat = jnp.concatenate([v.astype(BF).reshape(-1, lanes) for v in pieces], axis=0)
    extra = -flat.shape[0] % 16
    return jnp.pad(flat, ((0, extra), (0, 0)))


def scatter_sum(pieces, lanes):
    whole = jnp.concatenate([v.astype(BF) for v in pieces], axis=1).reshape(-1, lanes)
    return lax.psum_scatter(whole, BOTH, scatter_dimension=0, tiled=True).astype(F32).reshape(-1)


def halves(v):
    high = v.astype(BF)
    return high, (v - high.astype(F32)).astype(BF)


def body(
    tokens,
    cotangent,
    clip_lengths,
    clip_sets,
    clip_scales,
    norm1_gain,
    norm1_shift,
    w_query,
    query_bias,
    w_key,
    w_value,
    value_bias,
    w_out,
    out_bias,
    norm2_gain,
    norm2_shift,
    w_fc1,
    fc1_bias,
    w_fc2,
    fc2_bias,
    query_down,
    query_up,
    key_down,
    key_up,
    value_down,
    value_up,
    out_down,
    out_up,
    fc1_down,
    fc1_up,
    fc2_down,
    fc2_up,
):
    nr = lax.axis_size("rows")
    nc = lax.axis_size("cols")
    col = lax.axis_index("cols")
    clips = clip_lengths.shape[0]
    own = tokens.shape[0]
    clip_len = own * nc // clips
    tm = math.gcd(own, clip_len)
    width = query_bias.shape[0]
    hidden = fc1_bias.shape[0]
    hh = width // HEAD_DIM
    dr = w_query.shape[0]
    rk = RANK // nr
    part = SETS * RANK // nc
    exchange = Exchange(nc, own, clips, clip_len)

    block_clip = (col * own + jnp.arange(own // tm, dtype=jnp.int32) * tm) // clip_len
    sets = jnp.take(clip_sets, block_clip)
    scales = jnp.take(clip_scales, block_clip)

    def shared_rows(v):
        return lax.dynamic_slice(v.reshape(SETS * RANK, dr), (col * part, 0), (part, dr))

    def flip(v):
        return jnp.swapaxes(v, 1, 2)

    qh, ql = halves(query_bias)
    vh, vl = halves(value_bias)
    none = jnp.zeros_like(qh)
    pieces = [
        jnp.concatenate([w_query, w_key, w_value], axis=1),
        jnp.stack([shared_rows(flip(v)) for v in (query_down, key_down, value_down)]),
        jnp.stack([query_up, key_up, value_up]),
        jnp.stack([qh, none, vh, ql, none, vl]),
    ]
    g1 = lax.all_gather(pack(pieces, 3 * width), BOTH, axis=0).reshape(nr, nc, -1, 3 * width)
    at = dr
    rows = 3 * part * dr // (3 * width)
    down_qkv = (
        g1[:, :, at : at + rows]
        .reshape(nr, nc, 3, part, dr)
        .transpose(2, 1, 3, 0, 4)
        .reshape(3, SETS, RANK, D)
        .transpose(1, 0, 2, 3)
        .reshape(SETS, 3 * RANK, D)
    )
    at += rows
    rows = SETS * rk
    up_qkv = (
        g1[:, :, at : at + rows]
        .reshape(nr, nc, 3, SETS, rk, width)
        .transpose(3, 1, 2, 0, 4, 5)
        .reshape(SETS, nc, 3 * RANK, width)
    )
    at += rows
    bias_qkv = jnp.sum(g1[0, :, at : at + 2].astype(F32), axis=1, keepdims=True)

    pieces = [
        w_fc1,
        w_fc2.T,
        w_out.T,
        jnp.stack([shared_rows(flip(fc1_down)), shared_rows(out_up), shared_rows(fc2_up)]),
        fc1_up,
        flip(fc2_down),
        flip(out_down),
        jnp.stack(halves(fc1_bias)),
    ]
    packed, _ = lax.optimization_barrier((pack(pieces, hidden), g1))
    g2 = lax.all_gather(packed, BOTH, axis=0).reshape(nr, nc, -1, hidden)
    at = 2 * dr

    def take(rows):
        nonlocal at
        got = g2[:, :, at : at + rows]
        at += rows
        return got

    wo_t = take(dr * width // hidden).reshape(nr, nc, dr, width).transpose(0, 2, 1, 3).reshape(D, D)
    tables = (
        take(3 * part * dr // hidden)
        .reshape(nr, nc, 3, part, dr)
        .transpose(2, 1, 3, 0, 4)
        .reshape(3, SETS, RANK, D)
    )
    f1down, oup, f2up = tables[0], tables[1], tables[2]
    by_hidden = lambda v: v.reshape(nr, nc, SETS, rk, hidden).transpose(2, 1, 0, 3, 4).reshape(SETS, nc, RANK, hidden)
    f1up = by_hidden(take(SETS * rk))
    f2down = by_hidden(take(SETS * rk))
    odown = (
        take(SETS * rk * width // hidden)
        .reshape(nr, nc, SETS, rk, width)
        .transpose(2, 0, 3, 1, 4)
        .reshape(SETS, RANK, D)
    )
    b1 = jnp.sum(take(2)[0].astype(F32), axis=1, keepdims=True)

    gain1, shift1 = norm1_gain[None], norm1_shift[None]
    gain2, shift2 = norm2_gain[None], norm2_shift[None]

    normed, ranks, y = project(tokens, gain1, shift1, g1, bias_qkv, down_qkv, up_qkv, sets, scales, tm)
    heads = exchange.to_heads(y)
    lens = exchange.lens(clip_lengths)
    results = [attend(v, n, hh) for v, n in zip(heads, lens)]
    att = exchange.from_heads([r[0] for r in results])
    att, middle, normed_mlp, ro, r1 = out_project(
        att, tokens, wo_t, out_bias[None], odown, oup, gain2, shift2, f1down, sets, scales, tm
    )
    output, grad_middle, grad_branch, gf1up, gf2down, gf2up, gf1down = mlp(
        normed_mlp, cotangent, middle, g2, b1, f1up, f2down, f2up, f1down, r1, fc2_bias[None], gain2, sets, scales, tm
    )
    ga, goup, godown = out_back(grad_branch, wo_t, oup, odown, att, ro, sets, scales, tm, nc)

    def split_model(v):
        k = v.shape[0]
        return v.reshape(k, nc, part, nr, dr).transpose(3, 1, 0, 2, 4).reshape(nr * nc, -1)

    def join_model(v, k):
        every = lax.all_gather(v.reshape(k, part, dr), "cols", axis=1, tiled=True)
        return every.reshape(k, SETS, RANK, dr)

    by_rank = lambda v: v.reshape(SETS, nc, nr, rk, hidden).transpose(2, 1, 0, 3, 4).reshape(nr * nc, -1)
    late = [
        split_model(jnp.stack([gf1down, goup, gf2up])),
        by_rank(gf1up),
        by_rank(gf2down),
        godown.reshape(SETS, nr, rk, nc, width).transpose(1, 3, 0, 2, 4).reshape(nr * nc, -1),
    ]
    summed = scatter_sum(late, hidden)
    sizes = [3 * part * dr, SETS * rk * hidden, SETS * rk * hidden, SETS * rk * width]
    edges = [sum(sizes[:i]) for i in range(5)]
    cut = [summed[edges[i] : edges[i + 1]] for i in range(4)]
    model = join_model(cut[0], 3)
    grad_fc1_down, grad_out_up, grad_fc2_up = flip(model[0]), model[1], model[2]
    grad_fc1_up = cut[1].reshape(SETS, rk, hidden)
    grad_fc2_down = flip(cut[2].reshape(SETS, rk, hidden))
    grad_out_down = flip(cut[3].reshape(SETS, rk, width))

    grads = exchange.to_heads(ga)
    backs = [
        attend_back(v, r[0], d, r[1], n, hh) for v, r, d, n in zip(heads, results, grads, lens)
    ]
    dy = exchange.from_heads(backs)
    grad_tokens, gup, gdown = project_back(
        dy, g1, up_qkv, down_qkv, tokens, normed, ranks, grad_middle, gain1, sets, scales, tm
    )
    last = [
        split_model(gdown.reshape(SETS, 3, RANK, D).swapaxes(0, 1)),
        gup.reshape(SETS, nc, 3, nr, rk, width).transpose(3, 1, 2, 0, 4, 5).reshape(nr * nc, -1),
    ]
    summed = scatter_sum(last, 3 * width)
    model = join_model(summed[: 3 * part * dr], 3)
    ups = summed[3 * part * dr :].reshape(3, SETS, rk, width)
    return (
        output,
        grad_tokens,
        flip(model[0]),
        ups[0],
        flip(model[1]),
        ups[1],
        flip(model[2]),
        ups[2],
        grad_out_down,
        grad_out_up,
        grad_fc1_down,
        grad_fc1_up,
        grad_fc2_down,
        grad_fc2_up,
    )


def solution(mesh):
    both = P(("rows", "cols"), None)
    grid = P("rows", "cols")
    turned = P("cols", "rows")
    down = P(None, "rows", None)
    up = P(None, "rows", "cols")
    far_down = P(None, "cols", "rows")
    far_up = P(None, None, "rows")
    return jax.shard_map(
        body,
        mesh=mesh,
        in_specs=(
            both,
            both,
            P("rows"),
            P("rows"),
            P("rows"),
            P(),
            P(),
            grid,
            P("cols"),
            grid,
            grid,
            P("cols"),
            turned,
            P(),
            P(),
            P(),
            grid,
            P("cols"),
            turned,
            P(),
            down,
            up,
            down,
            up,
            down,
            up,
            far_down,
            far_up,
            down,
            up,
            far_down,
            far_up,
        ),
        out_specs=(
            both,
            both,
            down,
            up,
            down,
            up,
            down,
            up,
            far_down,
            far_up,
            down,
            up,
            far_down,
            far_up,
        ),
        check_vma=False,
    )
```

```python
import functools
import math

import jax
import jax.numpy as jnp
from jax import lax
from jax.experimental import pallas as pl
from jax.experimental.pallas import tpu as pltpu
from jax.sharding import PartitionSpec as P


D = 1280
SETS = 8
RANK = 16
HEAD_DIM = 80
EPSILON = 1e-05
LOG2E = 1.4426950408889634
LOW = -1e30
F32 = jnp.float32
BF = jnp.bfloat16
BOTH = ("rows", "cols")


def dot(a, b):
    return lax.dot_general(a, b, (((1,), (0,)), ((), ())), preferred_element_type=F32)


def dot_t(a, b):
    return lax.dot_general(a, b, (((1,), (1,)), ((), ())), preferred_element_type=F32)


def token_sum(a, b):
    return dot(a.T.astype(BF), b)


def norm_parts(x):
    mean = jnp.mean(x, axis=-1, keepdims=True)
    centred = x - mean
    inverse = lax.rsqrt(jnp.mean(centred * centred, axis=-1, keepdims=True) + EPSILON)
    return centred * inverse, inverse


def params(n, limit=60 << 20):
    return pltpu.CompilerParams(
        dimension_semantics=("arbitrary",) * n, vmem_limit_bytes=limit
    )


def cost(flops, nbytes, trans=0):
    return pl.CostEstimate(flops=int(flops), bytes_accessed=int(nbytes), transcendentals=int(trans))


def set_mask(shape, which, group, per):
    column = lax.broadcasted_iota(jnp.int32, shape, len(shape) - 1)
    return (column % group) // per == which


def choose(code, refs, dst, at):
    for j, ref in enumerate(refs):

        @pl.when(code == j)
        def _(ref=ref):
            dst[at] = ref[0, :, 0 : dst.shape[-1]]


def gather_clip(refs, plan, dst, bs):
    blocks = plan.shape[0] // 2
    for b in range(blocks):
        rows = slice(b * bs, (b + 1) * bs)
        for j, ref in enumerate(refs):

            @pl.when(plan[b] == j)
            def _(ref=ref, b=b, rows=rows):
                off = pl.multiple_of(plan[blocks + b] * bs, bs)
                dst[0, rows, :] = ref[0, pl.ds(off, bs), 0 : dst.shape[2]]


def attend_kernel(hh, length, qb, kb, ns, lens, plan, index, *refs):
    sources, (o_ref, lse_ref, x_ref, k_scr, vt_scr, acc, m_scr, l_scr) = refs[:ns], refs[ns:]
    p = pl.program_id(0)
    qi = pl.program_id(1)
    w = hh * HEAD_DIM
    c = HEAD_DIM**-0.5 * LOG2E

    @pl.when(qi == 0)
    def _():
        gather_clip(sources, plan, x_ref, 2 * length // plan.shape[0])
        vt_scr[...] = x_ref[0, :, 2 * w : 3 * w].T
        for h in range(hh):
            k_scr[h] = x_ref[0, :, w + h * HEAD_DIM : w + (h + 1) * HEAD_DIM]

    size = lens[p]
    block = x_ref[0, pl.ds(pl.multiple_of(qi * qb, qb), qb), 0:w]
    qs = [block[:, h * HEAD_DIM : (h + 1) * HEAD_DIM] for h in range(hh)]
    m_scr[...] = jnp.full_like(m_scr, LOW)
    l_scr[...] = jnp.zeros_like(l_scr)
    acc[...] = jnp.zeros_like(acc)

    def chunk(i, masked):
        r0 = pl.multiple_of(i * kb, kb)
        for h in range(hh):
            s = dot_t(k_scr[h, pl.ds(r0, kb), :], qs[h])
            if masked:
                keys = lax.broadcasted_iota(jnp.int32, (kb, qb), 0) + i * kb
                s = jnp.where(keys < size, s, LOW)
            old = m_scr[h : h + 1]
            top = jnp.maximum(old, jnp.max(s, axis=0, keepdims=True))
            probs = jnp.exp2((s - top) * c)
            shrink = jnp.exp2((old - top) * c)
            l_scr[h : h + 1] = l_scr[h : h + 1] * shrink + jnp.sum(probs, axis=0, keepdims=True)
            m_scr[h : h + 1] = top
            acc[h] = acc[h] * shrink + dot(
                vt_scr[h * HEAD_DIM : (h + 1) * HEAD_DIM, pl.ds(r0, kb)], probs.astype(BF)
            )

    full = size // kb

    def step(i, carry):
        chunk(i, False)
        return carry

    lax.fori_loop(0, full, step, 0)

    @pl.when(full * kb < size)
    def _():
        chunk(full, True)

    outs = [acc[h] * (1.0 / l_scr[h : h + 1]) for h in range(hh)]
    o_ref[0, :, 0:w] = jnp.concatenate(outs, axis=0).T.astype(BF)
    lse_ref[0] = m_scr[0:hh] * c + jnp.log2(l_scr[0:hh])


def lanes_of(n):
    return -(-n // 128) * 128


def source_specs(sources, problems):
    def spec(j, v):
        return pl.BlockSpec(
            (1,) + v.shape[1:], lambda p, q, l, plan, index: (index[j * problems + p], 0, 0)
        )

    return [spec(j, v) for j, v in enumerate(sources)]


def attend(sources, plan, index, lens, length, hh):
    problems = lens.shape[0]
    w3 = 3 * hh * HEAD_DIM
    w = hh * HEAD_DIM
    qb = math.gcd(length, 512)
    kb = math.gcd(length, 768)
    return pl.pallas_call(
        functools.partial(attend_kernel, hh, length, qb, kb, len(sources)),
        out_shape=(
            jax.ShapeDtypeStruct((problems, length, lanes_of(w)), BF),
            jax.ShapeDtypeStruct((problems, hh, length), F32),
            jax.ShapeDtypeStruct((problems, length, w3), BF),
        ),
        grid_spec=pltpu.PrefetchScalarGridSpec(
            num_scalar_prefetch=3,
            grid=(problems, length // qb),
            in_specs=source_specs(sources, problems),
            out_specs=[
                pl.BlockSpec((1, qb, lanes_of(w)), lambda p, q, *_: (p, q, 0)),
                pl.BlockSpec((1, hh, qb), lambda p, q, *_: (p, 0, q)),
                pl.BlockSpec((1, length, w3), lambda p, q, *_: (p, 0, 0)),
            ],
            scratch_shapes=[
                pltpu.VMEM((hh, length, HEAD_DIM), BF),
                pltpu.VMEM((w, length), BF),
                pltpu.VMEM((hh, HEAD_DIM, qb), F32),
                pltpu.VMEM((max(8, hh), qb), F32),
                pltpu.VMEM((max(8, hh), qb), F32),
            ],
        ),
        compiler_params=params(2),
        cost_estimate=cost(
            problems * hh * 4 * length * length * 256,
            problems * length * w3 * 6,
            problems * hh * length * length,
        ),
        name="attend",
    )(lens, plan, index, *sources)


def attend_back_kernel(hh, length, qb, kb, ns, lens, plan, index, *refs):
    sources = refs[:ns]
    x_ref, o_ref, lse_ref, dx_ref, do_scr, k_scr, v_scr, kt_scr, dk, dv, dqt = refs[ns:]
    p = pl.program_id(0)
    qi = pl.program_id(1)
    w = hh * HEAD_DIM
    scale = HEAD_DIM**-0.5
    c = scale * LOG2E

    @pl.when(qi == 0)
    def _():
        gather_clip(sources, plan, do_scr, 2 * length // plan.shape[0])
        kt_scr[...] = x_ref[0, :, w : 2 * w].T
        for h in range(hh):
            k_scr[h] = x_ref[0, :, w + h * HEAD_DIM : w + (h + 1) * HEAD_DIM]
            v_scr[h] = x_ref[0, :, 2 * w + h * HEAD_DIM : 2 * w + (h + 1) * HEAD_DIM]
        dk[...] = jnp.zeros_like(dk)
        dv[...] = jnp.zeros_like(dv)

    size = lens[p]
    rows = pl.ds(pl.multiple_of(qi * qb, qb), qb)
    block = x_ref[0, rows, 0:w]
    qs = [block[:, h * HEAD_DIM : (h + 1) * HEAD_DIM] for h in range(hh)]
    do = do_scr[0, rows, :]
    dos = [do[:, h * HEAD_DIM : (h + 1) * HEAD_DIM] for h in range(hh)]
    prod = (do.astype(F32) * o_ref[0, :, 0:w].astype(F32)).T
    inner = [
        jnp.sum(prod[h * HEAD_DIM : (h + 1) * HEAD_DIM], axis=0, keepdims=True) for h in range(hh)
    ]
    dqt[...] = jnp.zeros_like(dqt)

    def chunk(i, masked):
        keys_at = pl.ds(pl.multiple_of(i * kb, kb), kb)
        for h in range(hh):
            s = dot_t(k_scr[h, keys_at, :], qs[h])
            probs = jnp.exp2(s * c - lse_ref[0, h : h + 1])
            if masked:
                keys = lax.broadcasted_iota(jnp.int32, (kb, qb), 0) + i * kb
                probs = jnp.where(keys < size, probs, 0.0)
            dp = dot_t(v_scr[h, keys_at, :], dos[h])
            ds = (probs * (dp - inner[h])).astype(BF)
            dv[h, keys_at, :] += dot(probs.astype(BF), dos[h])
            dk[h, keys_at, :] += dot(ds, qs[h])
            dqt[h] += dot(kt_scr[h * HEAD_DIM : (h + 1) * HEAD_DIM, keys_at], ds)

    full = size // kb

    def step(i, carry):
        chunk(i, False)
        return carry

    lax.fori_loop(0, full, step, 0)

    @pl.when(full * kb < size)
    def _():
        chunk(full, True)

    dq = jnp.concatenate([dqt[h] for h in range(hh)], axis=0).T * scale
    dx_ref[0, rows, 0:w] = dq.astype(BF)

    @pl.when(qi == pl.num_programs(1) - 1)
    def _():
        for h in range(hh):
            dx_ref[0, :, w + h * HEAD_DIM : w + (h + 1) * HEAD_DIM] = (dk[h] * scale).astype(BF)
            dx_ref[0, :, 2 * w + h * HEAD_DIM : 2 * w + (h + 1) * HEAD_DIM] = dv[h].astype(BF)


def attend_back(sources, plan, index, x, o, lse, lens, hh):
    problems, length, w3 = x.shape
    w = hh * HEAD_DIM
    qb = math.gcd(length, 512)
    kb = math.gcd(length, 512)
    return pl.pallas_call(
        functools.partial(attend_back_kernel, hh, length, qb, kb, len(sources)),
        out_shape=jax.ShapeDtypeStruct((problems, length, lanes_of(w3)), BF),
        grid_spec=pltpu.PrefetchScalarGridSpec(
            num_scalar_prefetch=3,
            grid=(problems, length // qb),
            in_specs=source_specs(sources, problems)
            + [
                pl.BlockSpec((1, length, w3), lambda p, q, *_: (p, 0, 0)),
                pl.BlockSpec((1, qb, lanes_of(w)), lambda p, q, *_: (p, q, 0)),
                pl.BlockSpec((1, hh, qb), lambda p, q, *_: (p, 0, q)),
            ],
            out_specs=pl.BlockSpec((1, length, lanes_of(w3)), lambda p, q, *_: (p, 0, 0)),
            scratch_shapes=[
                pltpu.VMEM((1, length, w), BF),
                pltpu.VMEM((hh, length, HEAD_DIM), BF),
                pltpu.VMEM((hh, length, HEAD_DIM), BF),
                pltpu.VMEM((w, length), BF),
                pltpu.VMEM((hh, length, HEAD_DIM), F32),
                pltpu.VMEM((hh, length, HEAD_DIM), F32),
                pltpu.VMEM((hh, HEAD_DIM, qb), F32),
            ],
        ),
        compiler_params=params(2),
        cost_estimate=cost(
            problems * hh * 10 * length * length * 256, x.size * 6, problems * hh * length * length
        ),
        name="attend_back",
    )(lens, plan, index, *sources, x, o, lse)


def project_kernel(
    tm, width, group, per, sets, scales, order, x_ref, gain, shift, w_ref, bias, down, up, *outs
):
    normed_ref, ranks_ref, away_ref, mine_ref, n_scr, r_scr = outs
    c = pl.program_id(0)
    m = pl.program_id(1)
    rows = pl.ds(pl.multiple_of(m * tm, tm), tm)
    wide = group * w_ref.shape[0]

    @pl.when(c == 0)
    def _():
        unit, _ = norm_parts(x_ref[...].astype(F32))
        normed = (unit * gain[...] + shift[...]).astype(BF)
        n_scr[rows, :] = normed
        normed_ref[...] = normed
        rank = dot(normed, down[...]) * scales[m]
        keep = set_mask(rank.shape, sets[m], group, per)
        rank = jnp.where(keep, rank, 0.0).astype(BF)
        r_scr[rows, :] = rank
        ranks_ref[...] = rank

    y = dot(n_scr[rows, :], w_ref[:, 0].reshape(D, 3 * width)) + bias[0]
    table = up[:, 0].reshape(wide, 3 * width)
    rank = r_scr[rows, :]
    extra = [
        dot(rank[:, j * wide : (j + 1) * wide], table[:, j * width : (j + 1) * width]) for j in range(3)
    ]
    y = (y + jnp.concatenate(extra, axis=1)).astype(BF)
    half = pl.num_programs(0) // 2

    @pl.when(c < half)
    def _():
        away_ref[0, :, 0 : 3 * width] = y

    @pl.when(c >= half)
    def _():
        mine_ref[0, :, 0 : 3 * width] = y


def project(tokens, gain, shift, gathered, bias, tables, sets, scales, order, tm, per):
    own = tokens.shape[0]
    rr, nc, _, w3 = gathered.shape
    width = w3 // 3
    group = SETS * per
    wide = group * rr
    nm = own // tm
    half = nc // 2
    first = lambda c, m, *_: (jnp.where(c == 0, m, nm - 1), 0)
    flat = lambda c, m, *_: (0, 0)
    return pl.pallas_call(
        functools.partial(project_kernel, tm, width, group, per),
        out_shape=(
            jax.ShapeDtypeStruct((own, D), BF),
            jax.ShapeDtypeStruct((own, 3 * wide), BF),
            jax.ShapeDtypeStruct((half, own, lanes_of(w3)), BF),
            jax.ShapeDtypeStruct((half, own, lanes_of(w3)), BF),
        ),
        grid_spec=pltpu.PrefetchScalarGridSpec(
            num_scalar_prefetch=3,
            grid=(nc, nm),
            in_specs=[
                pl.BlockSpec((tm, D), first),
                pl.BlockSpec((1, D), flat),
                pl.BlockSpec((1, D), flat),
                pl.BlockSpec((rr, 1, D // rr, w3), lambda c, m, s, a, o: (0, o[c], 0, 0)),
                pl.BlockSpec((1, 1, w3), lambda c, m, s, a, o: (o[c], 0, 0)),
                pl.BlockSpec((D, 3 * wide), flat),
                pl.BlockSpec(
                    (rr, 1, group, w3), lambda c, m, s, a, o: (0, o[c], D // rr // group, 0)
                ),
            ],
            out_specs=[
                pl.BlockSpec((tm, D), first),
                pl.BlockSpec((tm, 3 * wide), first),
                pl.BlockSpec(
                    (1, tm, lanes_of(w3)),
                    lambda c, m, *_: (jnp.minimum(c, half - 1), jnp.where(c < half, m, nm - 1), 0),
                ),
                pl.BlockSpec(
                    (1, tm, lanes_of(w3)),
                    lambda c, m, *_: (jnp.maximum(c - half, 0), jnp.where(c < half, 0, m), 0),
                ),
            ],
            scratch_shapes=[pltpu.VMEM((own, D), BF), pltpu.VMEM((own, 3 * wide), BF)],
        ),
        compiler_params=params(2),
        cost_estimate=cost(2 * own * D * nc * w3 * 1.3, D * nc * w3 * 2 + own * (2 * D + nc * w3) * 2),
        name="project",
    )(sets, scales, order, tokens, gain, shift, gathered, bias, tables, gathered)


def piece_specs(sources, tm, at):
    def spec(j, v):
        def where_from(*ids):
            code = ids[-1]
            i = at(*ids[:-1])
            hit = code[3 * i] == j
            return (jnp.where(hit, code[3 * i + 1], 0), jnp.where(hit, code[3 * i + 2], 0), 0)

        return pl.BlockSpec((1, tm, v.shape[-1]), where_from)

    return [spec(j, v) for j, v in enumerate(sources)]


def lane_tiles(v, group):
    n = v.shape[1]
    pad = -n % 128
    if pad:
        v = jnp.concatenate([v, jnp.zeros((v.shape[0], pad), v.dtype)], axis=1)
    return [
        v[:, t * 128 : (t + 1) * 128].reshape(-1, group, 128) for t in range((n + pad) // 128)
    ]


def put_tiles(ref, first, v, group):
    for t, tile in enumerate(lane_tiles(v, group)):
        at = (first + t) * group
        ref[:, 0, at : at + group, :] = tile.astype(BF)


def adapt_back_kernel(tm, width, group, per, ns, nm, sets, scales, code, *refs):
    sources = refs[:ns]
    up, normed_ref, ranks_ref, dy_ref, grank_ref, gup_ref, gdown_ref, racc, gup, gdown = refs[ns:]
    c = pl.program_id(0)
    m = pl.program_id(1)
    last = c == pl.num_programs(0) - 1
    rows = pl.ds(pl.multiple_of(m * tm, tm), tm)
    wide = group * up.shape[0]
    choose(code[3 * (c * nm + m)], sources, dy_ref, 0)
    dy = dy_ref[0]
    table = up[:, 0].reshape(wide, 3 * width)
    pieces = [dy[:, j * width : (j + 1) * width] for j in range(3)]
    rpart = jnp.concatenate(
        [dot_t(pieces[j], table[:, j * width : (j + 1) * width]) for j in range(3)], axis=1
    )

    @pl.when(c == 0)
    def _():
        racc[rows, :] = rpart

    @pl.when(c > 0)
    def _():
        racc[rows, :] += rpart

    turned = ranks_ref[...].T
    for j in range(3):
        part = dot(turned[j * wide : (j + 1) * wide], pieces[j])

        @pl.when(m == 0)
        def _(j=j, part=part):
            gup[j] = part

        @pl.when(m > 0)
        def _(j=j, part=part):
            gup[j] += part

    @pl.when(m == nm - 1)
    def _():
        tiles = -(-width // 128)
        for j in range(3):
            put_tiles(gup_ref, j * tiles, gup[j], group)

    @pl.when(last)
    def _():
        grank = racc[rows, :] * scales[m]
        grank = jnp.where(set_mask(grank.shape, sets[m], group, per), grank, 0.0)
        grank_ref[...] = grank.astype(BF)
        part = token_sum(grank, normed_ref[...])

        @pl.when(m == 0)
        def _():
            gdown[...] = part

        @pl.when(m > 0)
        def _():
            gdown[...] += part

        @pl.when(m == nm - 1)
        def _():
            for j in range(3):
                gdown_ref[j] = gdown[j * wide : (j + 1) * wide, :].T.astype(BF)


def adapt_back(sources, code, gathered, normed, ranks, sets, scales, tm, per):
    own = normed.shape[0]
    rr, nc, _, w3 = gathered.shape
    width = w3 // 3
    group = SETS * per
    wide = group * rr
    nm = own // tm
    tiles = 3 * -(-width // 128)
    final = lambda c, m, *_: (jnp.where(c == nc - 1, m, 0), 0)
    return pl.pallas_call(
        functools.partial(adapt_back_kernel, tm, width, group, per, len(sources), nm),
        out_shape=(
            jax.ShapeDtypeStruct((nc, own, w3), BF),
            jax.ShapeDtypeStruct((own, 3 * wide), BF),
            jax.ShapeDtypeStruct((rr, nc, tiles * group, 128), BF),
            jax.ShapeDtypeStruct((3, D, wide), BF),
        ),
        grid_spec=pltpu.PrefetchScalarGridSpec(
            num_scalar_prefetch=3,
            grid=(nc, nm),
            in_specs=piece_specs(sources, tm, lambda c, m, s, a: c * nm + m)
            + [
                pl.BlockSpec((rr, 1, group, w3), lambda c, m, *_: (0, c, D // rr // group, 0)),
                pl.BlockSpec((tm, D), final),
                pl.BlockSpec((tm, 3 * wide), lambda c, m, *_: (m, 0)),
            ],
            out_specs=[
                pl.BlockSpec((1, tm, w3), lambda c, m, *_: (c, m, 0)),
                pl.BlockSpec((tm, 3 * wide), final),
                pl.BlockSpec((rr, 1, tiles * group, 128), lambda c, m, *_: (0, c, 0, 0)),
                pl.BlockSpec((3, D, wide), lambda c, m, *_: (0, 0, 0)),
            ],
            scratch_shapes=[
                pltpu.VMEM((own, 3 * wide), F32),
                pltpu.VMEM((3, wide, width), F32),
                pltpu.VMEM((3 * wide, D), F32),
            ],
        ),
        compiler_params=params(2),
        cost_estimate=cost(own * D * nc * w3 * 0.6, own * nc * w3 * 4),
        name="adapt_back",
    )(sets, scales, code, *sources, gathered, normed, ranks)


def project_back_kernel(tm, width, dy_ref, w_ref, grank_ref, down, x_ref, gm_ref, gain, gt_ref, acc):
    c = pl.program_id(0)
    m = pl.program_id(1)
    rows = pl.ds(pl.multiple_of(m * tm, tm), tm)
    part = dot_t(dy_ref[0], w_ref[:, 0].reshape(D, 3 * width))

    @pl.when(c == 0)
    def _():
        acc[rows, :] = part + dot_t(grank_ref[...], down[...])

    @pl.when(c > 0)
    def _():
        acc[rows, :] += part

    @pl.when(c == pl.num_programs(0) - 1)
    def _():
        unit, inverse = norm_parts(x_ref[...].astype(F32))
        e = acc[rows, :] * gain[...]
        mean = jnp.mean(e, axis=-1, keepdims=True)
        second = jnp.mean(e * unit, axis=-1, keepdims=True)
        gt_ref[...] = (gm_ref[...] + (e - mean - unit * second) * inverse).astype(BF)


def project_back(dy, gathered, grank, tables, tokens, grad_middle, gain, tm):
    own = tokens.shape[0]
    rr, nc, _, w3 = gathered.shape
    width = w3 // 3
    wide3 = grank.shape[1]
    nm = own // tm
    final = lambda c, m: (jnp.where(c == nc - 1, m, 0), 0)
    return pl.pallas_call(
        functools.partial(project_back_kernel, tm, width),
        out_shape=jax.ShapeDtypeStruct((own, D), BF),
        grid=(nc, nm),
        in_specs=[
            pl.BlockSpec((1, tm, w3), lambda c, m: (c, m, 0)),
            pl.BlockSpec((rr, 1, D // rr, w3), lambda c, m: (0, c, 0, 0)),
            pl.BlockSpec((tm, wide3), lambda c, m: (jnp.where(c == 0, m, nm - 1), 0)),
            pl.BlockSpec((D, wide3), lambda c, m: (0, 0)),
            pl.BlockSpec((tm, D), final),
            pl.BlockSpec((tm, D), final),
            pl.BlockSpec((1, D), lambda c, m: (0, 0)),
        ],
        out_specs=pl.BlockSpec((tm, D), final),
        scratch_shapes=[pltpu.VMEM((own, D), F32)],
        compiler_params=params(2),
        cost_estimate=cost(2 * own * D * nc * w3 * 1.1, D * nc * w3 * 2 + own * (4 * D + nc * w3) * 2),
        name="project_back",
    )(dy, gathered, grank, tables, tokens, grad_middle, gain)


def out_kernel(nc, nm, group, per, ns, sets, scales, code, *refs):
    sources = refs[:ns]
    x_ref, w_ref, bias, odown, oup, gain, shift, fdown = refs[ns : ns + 8]
    att_out, middle_ref, normed_ref, ro_ref, r1_ref, a_scr = refs[ns + 8 :]
    m = pl.program_id(0)
    c = pl.program_id(1)
    choose(code[3 * (c * nm + m)], sources, a_scr, c)

    @pl.when(c == nc - 1)
    def _():
        att = jnp.concatenate([a_scr[i] for i in range(nc)], axis=1)
        att_out[...] = att
        ro = dot_t(att, odown[...]) * scales[m]
        keep = set_mask(ro.shape, sets[m], group, per)
        ro = jnp.where(keep, ro, 0.0).astype(BF)
        ro_ref[...] = ro
        middle = x_ref[...].astype(F32) + dot_t(att, w_ref[...]) + dot_t(ro, oup[...]) + bias[...]
        middle_ref[...] = middle
        unit, _ = norm_parts(middle)
        normed = (unit * gain[...] + shift[...]).astype(BF)
        normed_ref[...] = normed
        r1_ref[...] = jnp.where(keep, dot(normed, fdown[...]) * scales[m], 0.0).astype(BF)


def out_project(sources, code, tokens, wo_t, bias, odown, tables, gain, shift, sets, scales, tm, nc, per, rr):
    own = tokens.shape[0]
    width = D // nc
    group = SETS * per
    wide = group * rr
    nm = own // tm
    row = lambda m, c, *_: (m, 0)
    flat = lambda m, c, *_: (0, 0)
    return pl.pallas_call(
        functools.partial(out_kernel, nc, nm, group, per, len(sources)),
        out_shape=(
            jax.ShapeDtypeStruct((own, D), BF),
            jax.ShapeDtypeStruct((own, D), F32),
            jax.ShapeDtypeStruct((own, D), BF),
            jax.ShapeDtypeStruct((own, wide), BF),
            jax.ShapeDtypeStruct((own, wide), BF),
        ),
        grid_spec=pltpu.PrefetchScalarGridSpec(
            num_scalar_prefetch=3,
            grid=(nm, nc),
            in_specs=piece_specs(sources, tm, lambda m, c, s, a: c * nm + m)
            + [
                pl.BlockSpec((tm, D), row),
                pl.BlockSpec((D, D), flat),
                pl.BlockSpec((1, D), flat),
                pl.BlockSpec((wide, D), flat),
                pl.BlockSpec((D, wide), lambda m, c, *_: (0, 4)),
                pl.BlockSpec((1, D), flat),
                pl.BlockSpec((1, D), flat),
                pl.BlockSpec((D, wide), lambda m, c, *_: (0, 3)),
            ],
            out_specs=[
                pl.BlockSpec((tm, D), row),
                pl.BlockSpec((tm, D), row),
                pl.BlockSpec((tm, D), row),
                pl.BlockSpec((tm, wide), row),
                pl.BlockSpec((tm, wide), row),
            ],
            scratch_shapes=[pltpu.VMEM((nc, tm, width), BF)],
        ),
        compiler_params=params(2),
        cost_estimate=cost(2 * own * D * D * 1.5, D * D * 2 + own * D * 12),
        name="out_project",
    )(sets, scales, code, *sources, tokens, wo_t, bias, odown, tables, gain, shift, tables)


def out_back_kernel(nc, width, group, per, sets, scales, side, gb_ref, w_ref, oup, odown, att_ref, ro_ref, *outs):
    away_ref, mine_ref, gup_ref, gdown_ref, gup, gdown = outs
    m = pl.program_id(0)

    @pl.when(m == 0)
    def _():
        gup[...] = jnp.zeros_like(gup)
        gdown[...] = jnp.zeros_like(gdown)

    gb = gb_ref[...]
    gro = dot(gb, oup[...]) * scales[m]
    gro = jnp.where(set_mask(gro.shape, sets[m], group, per), gro, 0.0)
    ga = (dot(gb, w_ref[...]) + dot(gro.astype(BF), odown[...])).astype(BF)
    half = nc // 2
    for i in range(nc):
        piece = ga[:, i * width : (i + 1) * width]

        @pl.when(side[0] == i // half)
        def _(i=i, piece=piece):
            mine_ref[i % half, :, 0:width] = piece

        @pl.when(side[0] != i // half)
        def _(i=i, piece=piece):
            away_ref[i % half, :, 0:width] = piece

    gup[...] += dot(ro_ref[...].T, gb)
    gdown[...] += token_sum(gro, att_ref[...])

    @pl.when(m == pl.num_programs(0) - 1)
    def _():
        gup_ref[...] = gup[...].T.astype(BF)
        whole = gdown[...]
        for i in range(nc):
            for t, tile in enumerate(lane_tiles(whole[:, i * width : (i + 1) * width], group)):
                gdown_ref[:, i, t * group : (t + 1) * group, :] = tile.astype(BF)


def out_back(gb, wo_t, tables, odown, att, ro, sets, scales, side, tm, nc, per, rr):
    own = gb.shape[0]
    width = D // nc
    group = SETS * per
    wide = group * rr
    half = nc // 2
    tiles = -(-width // 128)
    row = lambda m, *_: (m, 0)
    flat = lambda m, *_: (0, 0)
    return pl.pallas_call(
        functools.partial(out_back_kernel, nc, width, group, per),
        out_shape=(
            jax.ShapeDtypeStruct((half, own, lanes_of(width)), BF),
            jax.ShapeDtypeStruct((half, own, lanes_of(width)), BF),
            jax.ShapeDtypeStruct((D, wide), BF),
            jax.ShapeDtypeStruct((rr, nc, tiles * group, 128), BF),
        ),
        grid_spec=pltpu.PrefetchScalarGridSpec(
            num_scalar_prefetch=3,
            grid=(own // tm,),
            in_specs=[
                pl.BlockSpec((tm, D), row),
                pl.BlockSpec((D, D), flat),
                pl.BlockSpec((D, wide), lambda m, *_: (0, 4)),
                pl.BlockSpec((wide, D), flat),
                pl.BlockSpec((tm, D), row),
                pl.BlockSpec((tm, wide), row),
            ],
            out_specs=[
                pl.BlockSpec((half, tm, lanes_of(width)), lambda m, *_: (0, m, 0)),
                pl.BlockSpec((half, tm, lanes_of(width)), lambda m, *_: (0, m, 0)),
                pl.BlockSpec((D, wide), flat),
                pl.BlockSpec((rr, nc, tiles * group, 128), lambda m, *_: (0, 0, 0, 0)),
            ],
            scratch_shapes=[pltpu.VMEM((wide, D), F32), pltpu.VMEM((wide, D), F32)],
        ),
        compiler_params=params(1),
        cost_estimate=cost(2 * own * D * D * 1.5, D * D * 2 + own * D * 6),
        name="out_back",
    )(sets, scales, side, gb, wo_t, tables, odown, att, ro)


def mlp_kernel(tm, nm, group, per, sets, scales, *refs):
    n_ref, g_ref, mid_ref, w1_ref, w2_ref, b1, up1_ref, down2_ref, up2, down1, r1_ref, bias2, gain = refs[:13]
    out_ref, gm_ref, gb_ref, gup1_ref, gdown2_ref, gup2_ref, gdown1_ref = refs[13:20]
    acc, gacc, r2acc, gr1acc, gr2, gup1, gdown2, gup2, gdown1 = refs[20:]
    c = pl.program_id(0)
    m = pl.program_id(1)
    rows = pl.ds(pl.multiple_of(m * tm, tm), tm)
    a = scales[m]
    g = g_ref[...]
    normed = n_ref[...]
    hidden = w1_ref.shape[-1]
    wide = r1_ref.shape[1]
    keep = set_mask((tm, wide), sets[m], group, per)

    @pl.when(c == 0)
    def _():
        gr2[rows, :] = jnp.where(keep, dot(g, up2[...]) * a, 0.0).astype(BF)
        acc[rows, :] = jnp.zeros((tm, D), F32)
        gacc[rows, :] = jnp.zeros((tm, D), F32)
        r2acc[rows, :] = jnp.zeros((tm, wide), F32)
        gr1acc[rows, :] = jnp.zeros((tm, wide), F32)

    @pl.when(m == 0)
    def _():
        gup1[...] = jnp.zeros_like(gup1)
        gdown2[...] = jnp.zeros_like(gdown2)

    @pl.when((m == 0) & (c == 0))
    def _():
        gup2[...] = jnp.zeros_like(gup2)
        gdown1[...] = jnp.zeros_like(gdown1)

    w1 = w1_ref[:, 0].reshape(D, hidden)
    w2 = w2_ref[:, 0].reshape(D, hidden)
    up1 = up1_ref[:, 0].reshape(wide, hidden)
    down2 = down2_ref[:, 0].reshape(wide, hidden)
    r1 = r1_ref[...]
    grank2 = gr2[rows, :]
    pre = dot(normed, w1) + dot(r1, up1) + b1[0]
    upper = 0.5 + 0.5 * lax.erf(pre * (0.5**0.5))
    density = jnp.exp(pre * pre * -0.5) * ((2.0 * math.pi) ** -0.5)
    act = (pre * upper).astype(BF)
    slope = upper + pre * density
    gact = dot(g, w2) + dot(grank2, down2)
    gpre = (gact * slope).astype(BF)
    acc[rows, :] += dot_t(act, w2)
    r2acc[rows, :] += dot_t(act, down2)
    gacc[rows, :] += dot_t(gpre, w1)
    gr1acc[rows, :] += dot_t(gpre, up1)
    gdown2[...] += dot(grank2.T, act)
    gup1[...] += dot(r1.T, gpre)

    @pl.when(m == nm - 1)
    def _():
        put_tiles(gup1_ref, 0, gup1[...], group)
        put_tiles(gdown2_ref, 0, gdown2[...], group)

    @pl.when(c == pl.num_programs(0) - 1)
    def _():
        r2 = jnp.where(keep, r2acc[rows, :] * a, 0.0).astype(BF)
        middle = mid_ref[...]
        out_ref[...] = (middle + acc[rows, :] + dot_t(r2, up2[...]) + bias2[...]).astype(BF)
        gup2[...] += dot(r2.T, g)
        gr1 = jnp.where(keep, gr1acc[rows, :] * a, 0.0).astype(BF)
        e = (gacc[rows, :] + dot_t(gr1, down1[...])) * gain[...]
        gdown1[...] += dot(gr1.T, normed)
        unit, inverse = norm_parts(middle)
        mean = jnp.mean(e, axis=-1, keepdims=True)
        second = jnp.mean(e * unit, axis=-1, keepdims=True)
        gm = g.astype(F32) + (e - mean - unit * second) * inverse
        gm_ref[...] = gm
        gb_ref[...] = gm.astype(BF)

        @pl.when(m == nm - 1)
        def _():
            gup2_ref[...] = gup2[...].T.astype(BF)
            gdown1_ref[...] = gdown1[...].T.astype(BF)


def mlp(normed, g, middle, gathered, b1, tables, r1, bias2, gain, sets, scales, tm, per, at):
    own = g.shape[0]
    rr, nc, _, hidden = gathered.shape
    group = SETS * per
    wide = group * rr
    nm = own // tm
    tiles = -(-hidden // 128)
    row = lambda c, m, *_: (m, 0)
    final = lambda c, m, *_: (jnp.where(c == nc - 1, m, 0), 0)
    flat = lambda c, m, *_: (0, 0)
    wblock = (rr, 1, D // rr, hidden)
    return pl.pallas_call(
        functools.partial(mlp_kernel, tm, nm, group, per),
        out_shape=(
            jax.ShapeDtypeStruct((own, D), BF),
            jax.ShapeDtypeStruct((own, D), F32),
            jax.ShapeDtypeStruct((own, D), BF),
            jax.ShapeDtypeStruct((rr, nc, tiles * group, 128), BF),
            jax.ShapeDtypeStruct((rr, nc, tiles * group, 128), BF),
            jax.ShapeDtypeStruct((D, wide), BF),
            jax.ShapeDtypeStruct((D, wide), BF),
        ),
        grid_spec=pltpu.PrefetchScalarGridSpec(
            num_scalar_prefetch=2,
            grid=(nc, nm),
            in_specs=[
                pl.BlockSpec((tm, D), row),
                pl.BlockSpec((tm, D), row),
                pl.BlockSpec((tm, D), final, pipeline_mode=pl.Buffered(1)),
                pl.BlockSpec(wblock, lambda c, m, *_: (0, c, 0, 0)),
                pl.BlockSpec(wblock, lambda c, m, *_: (0, c, 1, 0)),
                pl.BlockSpec((1, 1, hidden), lambda c, m, *_: (c, 0, 0)),
                pl.BlockSpec((rr, 1, group, hidden), lambda c, m, *_: (0, c, at // group, 0)),
                pl.BlockSpec((rr, 1, group, hidden), lambda c, m, *_: (0, c, at // group + 1, 0)),
                pl.BlockSpec((D, wide), lambda c, m, *_: (0, 5), pipeline_mode=pl.Buffered(1)),
                pl.BlockSpec((D, wide), lambda c, m, *_: (0, 3), pipeline_mode=pl.Buffered(1)),
                pl.BlockSpec((tm, wide), row),
                pl.BlockSpec((1, D), flat),
                pl.BlockSpec((1, D), flat),
            ],
            out_specs=[
                pl.BlockSpec((tm, D), final),
                pl.BlockSpec((tm, D), final),
                pl.BlockSpec((tm, D), final),
                pl.BlockSpec((rr, 1, tiles * group, 128), lambda c, m, *_: (0, c, 0, 0)),
                pl.BlockSpec((rr, 1, tiles * group, 128), lambda c, m, *_: (0, c, 0, 0)),
                pl.BlockSpec((D, wide), flat),
                pl.BlockSpec((D, wide), flat),
            ],
            scratch_shapes=[
                pltpu.VMEM((own, D), F32),
                pltpu.VMEM((own, D), F32),
                pltpu.VMEM((own, wide), F32),
                pltpu.VMEM((own, wide), F32),
                pltpu.VMEM((own, wide), BF),
                pltpu.VMEM((wide, hidden), F32),
                pltpu.VMEM((wide, hidden), F32),
                pltpu.VMEM((wide, D), F32),
                pltpu.VMEM((wide, D), F32),
            ],
        ),
        compiler_params=params(2, 67043328),
        cost_estimate=cost(8 * own * D * nc * hidden * 1.2, D * nc * hidden * 4 + own * D * 30, own * nc * hidden * 2),
        name="mlp",
    )(
        sets, scales, normed, g, middle, gathered, gathered, b1, gathered, gathered, tables, tables, r1, bias2, gain
    )


def assemble_kernel(width, parts, w_ref, o_ref, w_out, o_out):
    _, nc = w_ref.shape[:2]
    columns, downs = [], []
    for c in range(nc):
        block = w_ref[:, c]
        rows = [block[:, :, j * width : (j + 1) * width] for j in range(parts)]
        columns.append(jnp.concatenate(rows, axis=1).reshape(D, width))
        downs.append(o_ref[:, c, :, 0:width].reshape(-1, width))
    w_out[...] = jnp.concatenate(columns, axis=1)
    o_out[...] = jnp.concatenate(downs, axis=1)


def assemble(gathered, at_w, rows_w, at_o, group, width):
    nr, nc, _, hidden = gathered.shape
    parts = hidden // width
    if rows_w % 8 == 0 and at_w % rows_w == 0:
        return pl.pallas_call(
            functools.partial(assemble_kernel, width, parts),
            out_shape=(
                jax.ShapeDtypeStruct((D, D), BF),
                jax.ShapeDtypeStruct((nr * group, D), BF),
            ),
            grid=(1,),
            in_specs=[
                pl.BlockSpec((nr, nc, rows_w, hidden), lambda i: (0, 0, at_w // rows_w, 0)),
                pl.BlockSpec((nr, nc, group, hidden), lambda i: (0, 0, at_o // group, 0)),
            ],
            out_specs=[
                pl.BlockSpec((D, D), lambda i: (0, 0)),
                pl.BlockSpec((nr * group, D), lambda i: (0, 0)),
            ],
            compiler_params=params(1),
            name="assemble",
        )(gathered, gathered)
    w = gathered[:, :, at_w : at_w + rows_w].reshape(nr, nc, rows_w, parts, width)
    o = gathered[:, :, at_o : at_o + group, :width]
    return (
        w.transpose(0, 3, 2, 1, 4).reshape(D, D),
        o.transpose(0, 2, 1, 3).reshape(nr * group, D),
    )


def pick(flag, first, second):
    return jnp.where(flag, first, second)


def table_of(values):
    return jnp.stack([jnp.asarray(v, jnp.int32) for v in values])


class Exchange:
    def __init__(self, nc, own, clips, clip_len, tm):
        self.nc, self.own, self.clips, self.clip_len, self.tm = nc, own, clips, clip_len, tm
        self.local = nc == 4 and clips == 3 and own == 3 * tm and clip_len == 4 * tm
        col = lax.axis_index("cols")
        self.nm = nm = own // tm
        if not self.local:
            self.order = jnp.arange(nc, dtype=jnp.int32)
            self.side = jnp.ones((1,), jnp.int32)
            self.plans = [jnp.zeros((2,), jnp.int32)]
            self.indices = [jnp.arange(clips, dtype=jnp.int32)]
            entry = jnp.arange(nc * nm, dtype=jnp.int32)
            self.code = jnp.stack([entry * 0, entry // nm, entry % nm], axis=1).reshape(-1)
            return
        y, k = col // 2, col % 2
        self.y, self.k = y, k
        self.holder = y != k
        self.order = (jnp.arange(4, dtype=jnp.int32) + 2 * (1 - k)) % 4
        self.side = k[None]
        b = jnp.arange(4, dtype=jnp.int32)
        g = b + 2 * y
        clip_plan = jnp.concatenate([pick(g // 3 == k, 0, 1), g % 3])
        g = pick(y == 0, 4 + b, b - 2)
        near = b // 2 == y
        source = pick(near, pick(g // 3 == k, 0, 1), pick(self.holder, 3, 2))
        shared_plan = jnp.concatenate([source, pick(near, g % 3, b % 2)])
        self.plans = [clip_plan.astype(jnp.int32), shared_plan.astype(jnp.int32)]
        self.indices = [jnp.array([0, 1, 0, 1], jnp.int32), table_of([y, y, 0, 0])]
        entry = jnp.arange(12, dtype=jnp.int32)
        c, m = entry // 3, entry % 3
        g = 3 * k + m
        inside = (g >= 2 * y) & (g < 2 * y + 4)
        same, idx = c // 2 == k, c % 2
        source = pick(
            inside,
            pick(same, 0, 2),
            pick(idx == y, pick(same, 1, 3), pick(same, 4, 5)),
        )
        block = pick(
            inside,
            g - 2 * y,
            pick(y == 0, g - 4, pick(idx == y, g + 2, g)),
        )
        self.code = (
            jnp.stack([source, pick(inside, idx, 0), block], axis=1).astype(jnp.int32).reshape(-1)
        )

    def lens(self, lengths):
        if not self.local:
            return (lengths,)
        mine = pick(self.y == 0, lengths[0], lengths[2])
        return (jnp.stack([mine, mine]), lengths[1:2])

    def to_heads(self, away, mine):
        f = mine.shape[-1]
        if not self.local:
            moved = lax.all_to_all(jnp.concatenate([away, mine]), "cols", 0, 0, tiled=True)
            return [[moved.reshape(self.clips, self.clip_len, f)]]
        y, k, half = self.y, self.k, self.clip_len // 2
        start = pick(k == 1, self.own - half, 0)
        got = lax.ppermute(away, "cols", [(i, i ^ 1) for i in range(4)])
        one = lax.dynamic_slice(mine, (1 - y, start, 0), (1, half, f))
        two = lax.dynamic_slice(away, (1 - y, start, 0), (1, half, f))
        got_one = lax.ppermute(one, "cols", [(1, 3), (2, 0)])
        got_two = lax.ppermute(two, "cols", [(1, 2), (2, 1)])
        return [[mine, got], [mine, got, got_one, got_two]]

    def from_heads(self, parts):
        if not self.local:
            (v,) = parts
            v = v.reshape(self.nc, self.own, v.shape[-1])
            return [lax.all_to_all(v, "cols", 0, 0, tiled=True)]
        clip, shared = parts
        half = self.clip_len // 2
        far = lax.dynamic_slice(shared, (0, (1 - self.y) * half, 0), (1, half, clip.shape[-1]))
        swap = [(i, i ^ 1) for i in range(4)]
        got_one = lax.ppermute(far, "cols", [(3, 1), (0, 2)])
        got_two = lax.ppermute(far, "cols", [(2, 1), (1, 2)])
        got_shared = lax.ppermute(shared, "cols", swap)
        return [clip, shared, lax.ppermute(clip, "cols", swap), got_shared, got_one, got_two]


def up_to(n, k):
    return -(-n // k) * k


def rows_padded(v, rows, lanes):
    return jnp.pad(v.astype(BF), ((0, rows - v.shape[0]), (0, lanes - v.shape[1])))


def halves(v):
    high = v.astype(BF)
    return high, (v - high.astype(F32)).astype(BF)


def scatter_sum(pieces):
    whole = jnp.concatenate(pieces, axis=2)
    n = whole.shape[2]
    whole = jnp.pad(whole, ((0, 0), (0, 0), (0, up_to(n, 8) - n), (0, 0)))
    return whole.reshape(-1, 128)


def join(v, nc):
    col = lax.axis_index("cols")
    zeros = (0,) * v.ndim
    held = lax.dynamic_update_slice(jnp.zeros((nc,) + v.shape, v.dtype), v[None], (col,) + zeros)
    step = 1
    while step < nc:
        base = col // step * step
        sent = lax.dynamic_slice(held, (base,) + zeros, (step,) + v.shape)
        got = lax.ppermute(sent, "cols", [(i, i ^ step) for i in range(nc)])
        held = lax.dynamic_update_slice(held, got, (base ^ step,) + zeros)
        step *= 2
    return held


def body(
    tokens,
    cotangent,
    clip_lengths,
    clip_sets,
    clip_scales,
    norm1_gain,
    norm1_shift,
    w_query,
    query_bias,
    w_key,
    w_value,
    value_bias,
    w_out,
    out_bias,
    norm2_gain,
    norm2_shift,
    w_fc1,
    fc1_bias,
    w_fc2,
    fc2_bias,
    query_down,
    query_up,
    key_down,
    key_up,
    value_down,
    value_up,
    out_down,
    out_up,
    fc1_down,
    fc1_up,
    fc2_down,
    fc2_up,
):
    nr = lax.axis_size("rows")
    nc = lax.axis_size("cols")
    col = lax.axis_index("cols")
    clips = clip_lengths.shape[0]
    own = tokens.shape[0]
    clip_len = own * nc // clips
    tm = math.gcd(own, clip_len)
    width = query_bias.shape[0]
    hidden = fc1_bias.shape[0]
    hh = width // HEAD_DIM
    dr = w_query.shape[0]
    per = RANK // nr
    group = SETS * per
    wide = group * nr
    dc = dr // nc
    exchange = Exchange(nc, own, clips, clip_len, tm)

    block_clip = (col * own + jnp.arange(own // tm, dtype=jnp.int32) * tm) // clip_len
    sets = jnp.take(clip_sets, block_clip)
    scales = jnp.take(clip_scales, block_clip)

    downs = jnp.stack([query_down, key_down, value_down, fc1_down])
    downs = lax.dynamic_slice(downs, (0, 0, col * dc, 0), (4, SETS, dc, RANK))
    downs = downs.reshape(4, SETS, dc, nr, per).transpose(2, 0, 3, 1, 4).reshape(dc, 4 * wide)
    ups = jnp.stack([out_up, fc2_up])
    ups = lax.dynamic_slice(ups, (0, 0, 0, col * dc), (2, SETS, RANK, dc))
    ups = ups.reshape(2, SETS, nr, per, dc).transpose(4, 0, 2, 1, 3).reshape(dc, 2 * wide)
    tables = jnp.concatenate([downs, ups], axis=1)

    lanes = 3 * width
    qh, ql = halves(query_bias)
    vh, vl = halves(value_bias)
    none = jnp.zeros_like(qh)
    natural = lanes >= 6 * wide
    small = rows_padded(tables, dc, lanes) if natural else tables.reshape(-1, lanes)
    small_rows = small.shape[0]
    at_bias = dr + group
    at_table = up_to(at_bias + 2, 16)
    packed = jnp.concatenate(
        [
            jnp.concatenate([w_query, w_key, w_value], axis=1),
            jnp.concatenate([v.reshape(group, width) for v in (query_up, key_up, value_up)], axis=1),
            rows_padded(jnp.stack([jnp.concatenate([qh, none, vh]), jnp.concatenate([ql, none, vl])]), at_table - at_bias, lanes),
            rows_padded(small, up_to(small_rows, 16), lanes),
        ],
        axis=0,
    )
    g1 = lax.all_gather(packed, BOTH, axis=0).reshape(nr, nc, -1, lanes)
    tables = g1[:, :, at_table : at_table + small_rows]
    if natural:
        tables = tables[..., : 6 * wide]
    tables = tables.reshape(D, 6 * wide)
    bias_qkv = jnp.sum(g1[0, :, at_bias : at_bias + 2].astype(F32), axis=1, keepdims=True)

    parts = hidden // width
    rows_w = dr // parts
    at_w = 2 * dr
    at_f = up_to(at_w + rows_w, 16)
    at_o = at_f + 2 * group
    at_b = at_o + group
    wo = w_out.T.reshape(parts, rows_w, width).transpose(1, 0, 2).reshape(rows_w, hidden)
    turn = lambda v: jnp.swapaxes(v, 1, 2).reshape(group, -1)
    packed = jnp.concatenate(
        [
            w_fc1,
            w_fc2.T,
            rows_padded(wo, at_f - at_w, hidden),
            fc1_up.reshape(group, hidden),
            turn(fc2_down),
            rows_padded(turn(out_down), group, hidden),
            rows_padded(jnp.stack(halves(fc1_bias)), 16, hidden),
        ],
        axis=0,
    )
    packed, g1 = lax.optimization_barrier((packed, g1))
    g2 = lax.all_gather(packed, BOTH, axis=0).reshape(nr, nc, -1, hidden)
    wo_t, odown = assemble(g2, at_w, rows_w, at_o, group, width)
    b1 = jnp.sum(g2[0, :, at_b : at_b + 2].astype(F32), axis=1, keepdims=True)

    gain1, shift1 = norm1_gain[None], norm1_shift[None]
    gain2, shift2 = norm2_gain[None], norm2_shift[None]

    normed, ranks, away, mine = project(
        tokens, gain1, shift1, g1, bias_qkv, tables, sets, scales, exchange.order, tm, per
    )
    lens = exchange.lens(clip_lengths)
    results = []
    for sources, plan, index, n in zip(
        exchange.to_heads(away, mine), exchange.plans, exchange.indices, lens
    ):
        if results:
            n, _ = lax.optimization_barrier((n, results[-1][1]))
        results.append(attend(sources, plan, index, n, clip_len, hh))
    pieces = exchange.from_heads([r[0] for r in results])
    att, middle, normed_mlp, ro, r1 = out_project(
        pieces, exchange.code, tokens, wo_t, out_bias[None], odown, tables, gain2, shift2, sets, scales, tm, nc, per, nr
    )
    output, grad_middle, grad_branch, gup1, gdown2, gup2, gdown1 = mlp(
        normed_mlp, cotangent, middle, g2, b1, tables, r1, fc2_bias[None], gain2, sets, scales, tm, per, at_f
    )
    away, mine, goup, godown = out_back(
        grad_branch, wo_t, tables, odown, att, ro, sets, scales, exchange.side, tm, nc, per, nr
    )

    by_model = lambda v: v.reshape(nr, nc, dc, wide)
    late = scatter_sum([gup1, gdown2, godown, by_model(gdown1), by_model(goup), by_model(gup2)])
    late, away, mine = lax.optimization_barrier((late, away, mine))
    summed = lax.psum_scatter(late, BOTH, scatter_dimension=0, tiled=True).astype(F32)

    def untile(v, n):
        t = v.shape[0] // group
        return v.reshape(t, group, 128).transpose(1, 0, 2).reshape(group, t * 128)[:, :n].reshape(SETS, per, n)

    def model_tables(v):
        k = v.shape[0] // dc
        every = join(v, nc).reshape(nc, k, dc, wide).swapaxes(0, 1)
        return every.reshape(k, dr, nr, SETS, per)

    as_down = lambda v: v.transpose(2, 0, 1, 3).reshape(SETS, dr, RANK)
    as_up = lambda v: v.transpose(2, 1, 3, 0).reshape(SETS, RANK, dr)
    flip = lambda v: jnp.swapaxes(v, 1, 2)
    a = gup1.shape[2]
    b = godown.shape[2]
    grad_fc1_up = untile(summed[:a], hidden)
    grad_fc2_down = flip(untile(summed[a : 2 * a], hidden))
    grad_out_down = flip(untile(summed[2 * a : 2 * a + b], width))
    model = model_tables(summed[2 * a + b : 2 * a + b + 3 * dc])
    grad_fc1_down, grad_out_up, grad_fc2_up = as_down(model[0]), as_up(model[1]), as_up(model[2])

    calls = list(
        zip(exchange.to_heads(away, mine), exchange.plans, exchange.indices, results, lens)
    )
    backs = []
    for sources, plan, index, (o, lse, x), n in reversed(calls):
        if backs:
            n, _ = lax.optimization_barrier((n, backs[-1]))
        backs.append(attend_back(sources, plan, index, x, o, lse, n, hh))
    pieces = exchange.from_heads(backs[::-1])
    dy, grank, gup, gdown = adapt_back(
        pieces, exchange.code, g1, normed, ranks, sets, scales, tm, per
    )
    last = scatter_sum([gup] + [by_model(gdown[j]) for j in range(3)])
    last, dy = lax.optimization_barrier((last, dy))
    summed = lax.psum_scatter(last, BOTH, scatter_dimension=0, tiled=True).astype(F32)
    grad_tokens = project_back(dy, g1, grank, tables, tokens, grad_middle, gain1, tm)
    a = gup.shape[2] // 3
    up = [untile(summed[j * a : (j + 1) * a], width) for j in range(3)]
    model = model_tables(summed[3 * a : 3 * a + 3 * dc])
    down = [as_down(model[j]) for j in range(3)]
    return (
        output,
        grad_tokens,
        down[0],
        up[0],
        down[1],
        up[1],
        down[2],
        up[2],
        grad_out_down,
        grad_out_up,
        grad_fc1_down,
        grad_fc1_up,
        grad_fc2_down,
        grad_fc2_up,
    )


def solution(mesh):
    both = P(("rows", "cols"), None)
    grid = P("rows", "cols")
    turned = P("cols", "rows")
    down = P(None, "rows", None)
    up = P(None, "rows", "cols")
    far_down = P(None, "cols", "rows")
    far_up = P(None, None, "rows")
    return jax.shard_map(
        body,
        mesh=mesh,
        in_specs=(
            both,
            both,
            P("rows"),
            P("rows"),
            P("rows"),
            P(),
            P(),
            grid,
            P("cols"),
            grid,
            grid,
            P("cols"),
            turned,
            P(),
            P(),
            P(),
            grid,
            P("cols"),
            turned,
            P(),
            down,
            up,
            down,
            up,
            down,
            up,
            far_down,
            far_up,
            down,
            up,
            far_down,
            far_up,
        ),
        out_specs=(
            both,
            both,
            down,
            up,
            down,
            up,
            down,
            up,
            far_down,
            far_up,
            down,
            up,
            far_down,
            far_up,
        ),
        check_vma=False,
    )
```

```python
import functools
import math

import jax
import jax.numpy as jnp
from jax import lax
from jax.experimental import pallas as pl
from jax.experimental.pallas import tpu as pltpu
from jax.sharding import PartitionSpec as P


D = 1280
SETS = 8
RANK = 16
HEAD_DIM = 80
EPSILON = 1e-05
LOG2E = 1.4426950408889634
LOW = -1e30
F32 = jnp.float32
BF = jnp.bfloat16
BOTH = ("rows", "cols")


def dot(a, b):
    return lax.dot_general(a, b, (((1,), (0,)), ((), ())), preferred_element_type=F32)


def dot_t(a, b):
    return lax.dot_general(a, b, (((1,), (1,)), ((), ())), preferred_element_type=F32)


def token_sum(a, b):
    return dot(a.T.astype(BF), b)


def norm_parts(x):
    mean = jnp.mean(x, axis=-1, keepdims=True)
    centred = x - mean
    inverse = lax.rsqrt(jnp.mean(centred * centred, axis=-1, keepdims=True) + EPSILON)
    return centred * inverse, inverse


def params(n, limit=60 << 20):
    return pltpu.CompilerParams(
        dimension_semantics=("arbitrary",) * n, vmem_limit_bytes=limit
    )


def cost(flops, nbytes, trans=0):
    return pl.CostEstimate(flops=int(flops), bytes_accessed=int(nbytes), transcendentals=int(trans))


def set_mask(shape, which, group, per):
    column = lax.broadcasted_iota(jnp.int32, shape, len(shape) - 1)
    return (column % group) // per == which


def choose(code, refs, dst, at):
    for j, ref in enumerate(refs):

        @pl.when(code == j)
        def _(ref=ref):
            dst[at] = ref[0, :, 0 : dst.shape[-1]]


def gather_clip(refs, plan, dst, bs):
    blocks = plan.shape[0] // 2
    for b in range(blocks):
        rows = slice(b * bs, (b + 1) * bs)
        for j, ref in enumerate(refs):

            @pl.when(plan[b] == j)
            def _(ref=ref, b=b, rows=rows):
                off = pl.multiple_of(plan[blocks + b] * bs, bs)
                dst[0, rows, :] = ref[0, pl.ds(off, bs), 0 : dst.shape[2]]


def attend_kernel(hh, length, qb, kb, ns, lens, plan, index, *refs):
    sources, (o_ref, lse_ref, x_ref, k_scr, vt_scr, acc, m_scr, l_scr) = refs[:ns], refs[ns:]
    p = pl.program_id(0)
    qi = pl.program_id(1)
    w = hh * HEAD_DIM
    c = HEAD_DIM**-0.5 * LOG2E

    @pl.when(qi == 0)
    def _():
        gather_clip(sources, plan, x_ref, 2 * length // plan.shape[0])
        vt_scr[...] = x_ref[0, :, 2 * w : 3 * w].T
        for h in range(hh):
            k_scr[h] = x_ref[0, :, w + h * HEAD_DIM : w + (h + 1) * HEAD_DIM]

    size = lens[p]
    block = x_ref[0, pl.ds(pl.multiple_of(qi * qb, qb), qb), 0:w]
    qs = [block[:, h * HEAD_DIM : (h + 1) * HEAD_DIM] for h in range(hh)]
    m_scr[...] = jnp.full_like(m_scr, LOW)
    l_scr[...] = jnp.zeros_like(l_scr)
    acc[...] = jnp.zeros_like(acc)

    def chunk(i, masked):
        r0 = pl.multiple_of(i * kb, kb)
        for h in range(hh):
            s = dot_t(k_scr[h, pl.ds(r0, kb), :], qs[h])
            if masked:
                keys = lax.broadcasted_iota(jnp.int32, (kb, qb), 0) + i * kb
                s = jnp.where(keys < size, s, LOW)
            old = m_scr[h : h + 1]
            top = jnp.maximum(old, jnp.max(s, axis=0, keepdims=True))
            probs = jnp.exp2((s - top) * c)
            shrink = jnp.exp2((old - top) * c)
            l_scr[h : h + 1] = l_scr[h : h + 1] * shrink + jnp.sum(probs, axis=0, keepdims=True)
            m_scr[h : h + 1] = top
            acc[h] = acc[h] * shrink + dot(
                vt_scr[h * HEAD_DIM : (h + 1) * HEAD_DIM, pl.ds(r0, kb)], probs.astype(BF)
            )

    full = size // kb

    def step(i, carry):
        chunk(i, False)
        return carry

    lax.fori_loop(0, full, step, 0)

    @pl.when(full * kb < size)
    def _():
        chunk(full, True)

    outs = [acc[h] * (1.0 / l_scr[h : h + 1]) for h in range(hh)]
    o_ref[0, :, 0:w] = jnp.concatenate(outs, axis=0).T.astype(BF)
    lse_ref[0] = m_scr[0:hh] * c + jnp.log2(l_scr[0:hh])


def lanes_of(n):
    return -(-n // 128) * 128


def source_specs(sources, problems):
    def spec(j, v):
        return pl.BlockSpec(
            (1,) + v.shape[1:], lambda p, q, l, plan, index: (index[j * problems + p], 0, 0)
        )

    return [spec(j, v) for j, v in enumerate(sources)]


def attend(sources, plan, index, lens, length, hh):
    problems = lens.shape[0]
    w3 = 3 * hh * HEAD_DIM
    w = hh * HEAD_DIM
    qb = math.gcd(length, 512)
    kb = math.gcd(length, 768)
    return pl.pallas_call(
        functools.partial(attend_kernel, hh, length, qb, kb, len(sources)),
        out_shape=(
            jax.ShapeDtypeStruct((problems, length, lanes_of(w)), BF),
            jax.ShapeDtypeStruct((problems, hh, length), F32),
            jax.ShapeDtypeStruct((problems, length, w3), BF),
        ),
        grid_spec=pltpu.PrefetchScalarGridSpec(
            num_scalar_prefetch=3,
            grid=(problems, length // qb),
            in_specs=source_specs(sources, problems),
            out_specs=[
                pl.BlockSpec((1, qb, lanes_of(w)), lambda p, q, *_: (p, q, 0)),
                pl.BlockSpec((1, hh, qb), lambda p, q, *_: (p, 0, q)),
                pl.BlockSpec((1, length, w3), lambda p, q, *_: (p, 0, 0)),
            ],
            scratch_shapes=[
                pltpu.VMEM((hh, length, HEAD_DIM), BF),
                pltpu.VMEM((w, length), BF),
                pltpu.VMEM((hh, HEAD_DIM, qb), F32),
                pltpu.VMEM((max(8, hh), qb), F32),
                pltpu.VMEM((max(8, hh), qb), F32),
            ],
        ),
        compiler_params=params(2),
        cost_estimate=cost(
            problems * hh * 4 * length * length * 256,
            problems * length * w3 * 6,
            problems * hh * length * length,
        ),
        name="attend",
    )(lens, plan, index, *sources)


def attend_back_kernel(hh, length, qb, kb, ns, lens, plan, index, *refs):
    sources = refs[:ns]
    x_ref, o_ref, lse_ref, dx_ref, do_scr, k_scr, v_scr, kt_scr, dk, dv, dqt = refs[ns:]
    p = pl.program_id(0)
    qi = pl.program_id(1)
    w = hh * HEAD_DIM
    scale = HEAD_DIM**-0.5
    c = scale * LOG2E

    @pl.when(qi == 0)
    def _():
        gather_clip(sources, plan, do_scr, 2 * length // plan.shape[0])
        kt_scr[...] = x_ref[0, :, w : 2 * w].T
        for h in range(hh):
            k_scr[h] = x_ref[0, :, w + h * HEAD_DIM : w + (h + 1) * HEAD_DIM]
            v_scr[h] = x_ref[0, :, 2 * w + h * HEAD_DIM : 2 * w + (h + 1) * HEAD_DIM]
        dk[...] = jnp.zeros_like(dk)
        dv[...] = jnp.zeros_like(dv)

    size = lens[p]
    rows = pl.ds(pl.multiple_of(qi * qb, qb), qb)
    block = x_ref[0, rows, 0:w]
    qs = [block[:, h * HEAD_DIM : (h + 1) * HEAD_DIM] for h in range(hh)]
    do = do_scr[0, rows, :]
    dos = [do[:, h * HEAD_DIM : (h + 1) * HEAD_DIM] for h in range(hh)]
    prod = (do.astype(F32) * o_ref[0, :, 0:w].astype(F32)).T
    inner = [
        jnp.sum(prod[h * HEAD_DIM : (h + 1) * HEAD_DIM], axis=0, keepdims=True) for h in range(hh)
    ]
    dqt[...] = jnp.zeros_like(dqt)

    def chunk(i, masked):
        keys_at = pl.ds(pl.multiple_of(i * kb, kb), kb)
        for h in range(hh):
            s = dot_t(k_scr[h, keys_at, :], qs[h])
            probs = jnp.exp2(s * c - lse_ref[0, h : h + 1])
            if masked:
                keys = lax.broadcasted_iota(jnp.int32, (kb, qb), 0) + i * kb
                probs = jnp.where(keys < size, probs, 0.0)
            dp = dot_t(v_scr[h, keys_at, :], dos[h])
            ds = (probs * (dp - inner[h])).astype(BF)
            dv[h, keys_at, :] += dot(probs.astype(BF), dos[h])
            dk[h, keys_at, :] += dot(ds, qs[h])
            dqt[h] += dot(kt_scr[h * HEAD_DIM : (h + 1) * HEAD_DIM, keys_at], ds)

    full = size // kb

    def step(i, carry):
        chunk(i, False)
        return carry

    lax.fori_loop(0, full, step, 0)

    @pl.when(full * kb < size)
    def _():
        chunk(full, True)

    dq = jnp.concatenate([dqt[h] for h in range(hh)], axis=0).T * scale
    dx_ref[0, rows, 0:w] = dq.astype(BF)

    @pl.when(qi == pl.num_programs(1) - 1)
    def _():
        for h in range(hh):
            dx_ref[0, :, w + h * HEAD_DIM : w + (h + 1) * HEAD_DIM] = (dk[h] * scale).astype(BF)
            dx_ref[0, :, 2 * w + h * HEAD_DIM : 2 * w + (h + 1) * HEAD_DIM] = dv[h].astype(BF)


def attend_back(sources, plan, index, x, o, lse, lens, hh):
    problems, length, w3 = x.shape
    w = hh * HEAD_DIM
    qb = math.gcd(length, 512)
    kb = math.gcd(length, 512)
    return pl.pallas_call(
        functools.partial(attend_back_kernel, hh, length, qb, kb, len(sources)),
        out_shape=jax.ShapeDtypeStruct((problems, length, lanes_of(w3)), BF),
        grid_spec=pltpu.PrefetchScalarGridSpec(
            num_scalar_prefetch=3,
            grid=(problems, length // qb),
            in_specs=source_specs(sources, problems)
            + [
                pl.BlockSpec((1, length, w3), lambda p, q, *_: (p, 0, 0)),
                pl.BlockSpec((1, qb, lanes_of(w)), lambda p, q, *_: (p, q, 0)),
                pl.BlockSpec((1, hh, qb), lambda p, q, *_: (p, 0, q)),
            ],
            out_specs=pl.BlockSpec((1, length, lanes_of(w3)), lambda p, q, *_: (p, 0, 0)),
            scratch_shapes=[
                pltpu.VMEM((1, length, w), BF),
                pltpu.VMEM((hh, length, HEAD_DIM), BF),
                pltpu.VMEM((hh, length, HEAD_DIM), BF),
                pltpu.VMEM((w, length), BF),
                pltpu.VMEM((hh, length, HEAD_DIM), F32),
                pltpu.VMEM((hh, length, HEAD_DIM), F32),
                pltpu.VMEM((hh, HEAD_DIM, qb), F32),
            ],
        ),
        compiler_params=params(2),
        cost_estimate=cost(
            problems * hh * 10 * length * length * 256, x.size * 6, problems * hh * length * length
        ),
        name="attend_back",
    )(lens, plan, index, *sources, x, o, lse)


def project_kernel(
    tm, width, group, per, sets, scales, order, x_ref, gain, shift, w_ref, bias, down, up, *outs
):
    normed_ref, ranks_ref, away_ref, mine_ref, n_scr, r_scr = outs
    c = pl.program_id(0)
    m = pl.program_id(1)
    rows = pl.ds(pl.multiple_of(m * tm, tm), tm)
    wide = group * w_ref.shape[0]

    @pl.when(c == 0)
    def _():
        unit, _ = norm_parts(x_ref[...].astype(F32))
        normed = (unit * gain[...] + shift[...]).astype(BF)
        n_scr[rows, :] = normed
        normed_ref[...] = normed
        rank = dot(normed, down[...]) * scales[m]
        keep = set_mask(rank.shape, sets[m], group, per)
        rank = jnp.where(keep, rank, 0.0).astype(BF)
        r_scr[rows, :] = rank
        ranks_ref[...] = rank

    y = dot(n_scr[rows, :], w_ref[:, 0].reshape(D, 3 * width)) + bias[0]
    table = up[:, 0].reshape(wide, 3 * width)
    rank = r_scr[rows, :]
    extra = [
        dot(rank[:, j * wide : (j + 1) * wide], table[:, j * width : (j + 1) * width]) for j in range(3)
    ]
    y = (y + jnp.concatenate(extra, axis=1)).astype(BF)
    half = pl.num_programs(0) // 2

    @pl.when(c < half)
    def _():
        away_ref[0, :, 0 : 3 * width] = y

    @pl.when(c >= half)
    def _():
        mine_ref[0, :, 0 : 3 * width] = y


def project(tokens, gain, shift, gathered, bias, tables, sets, scales, order, tm, per):
    own = tokens.shape[0]
    rr, nc, _, w3 = gathered.shape
    width = w3 // 3
    group = SETS * per
    wide = group * rr
    nm = own // tm
    half = nc // 2
    first = lambda c, m, *_: (jnp.where(c == 0, m, nm - 1), 0)
    flat = lambda c, m, *_: (0, 0)
    return pl.pallas_call(
        functools.partial(project_kernel, tm, width, group, per),
        out_shape=(
            jax.ShapeDtypeStruct((own, D), BF),
            jax.ShapeDtypeStruct((own, 3 * wide), BF),
            jax.ShapeDtypeStruct((half, own, lanes_of(w3)), BF),
            jax.ShapeDtypeStruct((half, own, lanes_of(w3)), BF),
        ),
        grid_spec=pltpu.PrefetchScalarGridSpec(
            num_scalar_prefetch=3,
            grid=(nc, nm),
            in_specs=[
                pl.BlockSpec((tm, D), first),
                pl.BlockSpec((1, D), flat),
                pl.BlockSpec((1, D), flat),
                pl.BlockSpec((rr, 1, D // rr, w3), lambda c, m, s, a, o: (0, o[c], 0, 0)),
                pl.BlockSpec((1, 1, w3), lambda c, m, s, a, o: (o[c], 0, 0)),
                pl.BlockSpec((D, 3 * wide), flat),
                pl.BlockSpec(
                    (rr, 1, group, w3), lambda c, m, s, a, o: (0, o[c], D // rr // group, 0)
                ),
            ],
            out_specs=[
                pl.BlockSpec((tm, D), first),
                pl.BlockSpec((tm, 3 * wide), first),
                pl.BlockSpec(
                    (1, tm, lanes_of(w3)),
                    lambda c, m, *_: (jnp.minimum(c, half - 1), jnp.where(c < half, m, nm - 1), 0),
                ),
                pl.BlockSpec(
                    (1, tm, lanes_of(w3)),
                    lambda c, m, *_: (jnp.maximum(c - half, 0), jnp.where(c < half, 0, m), 0),
                ),
            ],
            scratch_shapes=[pltpu.VMEM((own, D), BF), pltpu.VMEM((own, 3 * wide), BF)],
        ),
        compiler_params=params(2),
        cost_estimate=cost(2 * own * D * nc * w3 * 1.3, D * nc * w3 * 2 + own * (2 * D + nc * w3) * 2),
        name="project",
    )(sets, scales, order, tokens, gain, shift, gathered, bias, tables, gathered)


def piece_specs(sources, tm, at):
    def spec(j, v):
        def where_from(*ids):
            code = ids[-1]
            i = at(*ids[:-1])
            hit = code[3 * i] == j
            return (jnp.where(hit, code[3 * i + 1], 0), jnp.where(hit, code[3 * i + 2], 0), 0)

        return pl.BlockSpec((1, tm, v.shape[-1]), where_from)

    return [spec(j, v) for j, v in enumerate(sources)]


def lane_tiles(v, group):
    n = v.shape[1]
    pad = -n % 128
    if pad:
        v = jnp.concatenate([v, jnp.zeros((v.shape[0], pad), v.dtype)], axis=1)
    return [
        v[:, t * 128 : (t + 1) * 128].reshape(-1, group, 128) for t in range((n + pad) // 128)
    ]


def put_tiles(ref, first, v, group):
    for t, tile in enumerate(lane_tiles(v, group)):
        at = (first + t) * group
        ref[:, 0, at : at + group, :] = tile.astype(BF)


def fold_sets(turned, group, per):
    wide = turned.shape[0]
    row = lax.broadcasted_iota(jnp.int32, (RANK, wide), 0)
    column = lax.broadcasted_iota(jnp.int32, (RANK, wide), 1)
    match = (column // group == row // per) & (column % per == row % per)
    return dot(jnp.where(match, 1.0, 0.0).astype(BF), turned).astype(BF)


def adapt_back_kernel(tm, width, group, per, ns, nm, sets, scales, slots, code, *refs):
    sources = refs[:ns]
    up, normed_ref, ranks_ref, dy_ref, grank_ref, gup_ref, gdown_ref, racc, gup, gdown = refs[ns:]
    slot = slots[pl.program_id(1)]
    c = pl.program_id(0)
    m = pl.program_id(1)
    last = c == pl.num_programs(0) - 1
    rows = pl.ds(pl.multiple_of(m * tm, tm), tm)
    wide = group * up.shape[0]
    choose(code[3 * (c * nm + m)], sources, dy_ref, 0)
    dy = dy_ref[0]
    table = up[:, 0].reshape(wide, 3 * width)
    pieces = [dy[:, j * width : (j + 1) * width] for j in range(3)]
    rpart = jnp.concatenate(
        [dot_t(pieces[j], table[:, j * width : (j + 1) * width]) for j in range(3)], axis=1
    )

    @pl.when(c == 0)
    def _():
        racc[rows, :] = rpart

    @pl.when(c > 0)
    def _():
        racc[rows, :] += rpart

    turned = ranks_ref[...].T

    @pl.when(m == 0)
    def _():
        gup[...] = jnp.zeros_like(gup)

    for j in range(3):
        gup[slot, j] += dot(fold_sets(turned[j * wide : (j + 1) * wide], group, per), pieces[j])

    @pl.when(m == nm - 1)
    def _():
        tiles = -(-width // 128)
        clips = gup.shape[0]
        for i in range(clips):
            for j in range(3):
                for t, tile in enumerate(lane_tiles(gup[i, j], RANK)):
                    gup_ref[0, (i * 3 + j) * tiles + t] = tile[0].astype(BF)

    @pl.when(last)
    def _():
        grank = racc[rows, :] * scales[m]
        grank = jnp.where(set_mask(grank.shape, sets[m], group, per), grank, 0.0)
        grank_ref[...] = grank.astype(BF)
        turned = grank.T.astype(BF)

        @pl.when(m == 0)
        def _():
            gdown[...] = jnp.zeros_like(gdown)

        for j in range(3):
            part = dot(fold_sets(turned[j * wide : (j + 1) * wide], group, per), normed_ref[...])
            gdown[slot, j * RANK : (j + 1) * RANK] += part

        @pl.when(m == nm - 1)
        def _():
            whole = gdown[...].reshape(-1, D)
            pad = gdown_ref.shape[0] * 128 - whole.shape[0]
            whole = jnp.concatenate([whole, jnp.zeros((pad, D), F32)], axis=0)
            for i in range(gdown_ref.shape[0]):
                gdown_ref[i] = whole[i * 128 : (i + 1) * 128].T.astype(BF)


def adapt_back(sources, code, gathered, normed, ranks, sets, scales, slots, clips, tm, per):
    own = normed.shape[0]
    rr, nc, _, w3 = gathered.shape
    width = w3 // 3
    group = SETS * per
    wide = group * rr
    nm = own // tm
    tiles = 3 * -(-width // 128)
    folded = -(-clips * 3 * RANK // 128)
    final = lambda c, m, *_: (jnp.where(c == nc - 1, m, 0), 0)
    return pl.pallas_call(
        functools.partial(adapt_back_kernel, tm, width, group, per, len(sources), nm),
        out_shape=(
            jax.ShapeDtypeStruct((nc, own, w3), BF),
            jax.ShapeDtypeStruct((own, 3 * wide), BF),
            jax.ShapeDtypeStruct((nc, clips * tiles, RANK, 128), BF),
            jax.ShapeDtypeStruct((folded, D, 128), BF),
        ),
        grid_spec=pltpu.PrefetchScalarGridSpec(
            num_scalar_prefetch=4,
            grid=(nc, nm),
            in_specs=piece_specs(sources, tm, lambda c, m, s, a, i: c * nm + m)
            + [
                pl.BlockSpec((rr, 1, group, w3), lambda c, m, *_: (0, c, D // rr // group, 0)),
                pl.BlockSpec((tm, D), final),
                pl.BlockSpec((tm, 3 * wide), lambda c, m, *_: (m, 0)),
            ],
            out_specs=[
                pl.BlockSpec((1, tm, w3), lambda c, m, *_: (c, m, 0)),
                pl.BlockSpec((tm, 3 * wide), final),
                pl.BlockSpec((1, clips * tiles, RANK, 128), lambda c, m, *_: (c, 0, 0, 0)),
                pl.BlockSpec((folded, D, 128), lambda c, m, *_: (0, 0, 0)),
            ],
            scratch_shapes=[
                pltpu.VMEM((own, 3 * wide), F32),
                pltpu.VMEM((clips, 3, RANK, width), F32),
                pltpu.VMEM((clips, 3 * RANK, D), F32),
            ],
        ),
        compiler_params=params(2),
        cost_estimate=cost(own * D * nc * w3 * 0.6, own * nc * w3 * 4),
        name="adapt_back",
    )(sets, scales, slots, code, *sources, gathered, normed, ranks)


def project_back_kernel(tm, width, dy_ref, w_ref, grank_ref, down, x_ref, gm_ref, gain, gt_ref, acc):
    c = pl.program_id(0)
    m = pl.program_id(1)
    rows = pl.ds(pl.multiple_of(m * tm, tm), tm)
    part = dot_t(dy_ref[0], w_ref[:, 0].reshape(D, 3 * width))

    @pl.when(c == 0)
    def _():
        acc[rows, :] = part + dot_t(grank_ref[...], down[...])

    @pl.when(c > 0)
    def _():
        acc[rows, :] += part

    @pl.when(c == pl.num_programs(0) - 1)
    def _():
        unit, inverse = norm_parts(x_ref[...].astype(F32))
        e = acc[rows, :] * gain[...]
        mean = jnp.mean(e, axis=-1, keepdims=True)
        second = jnp.mean(e * unit, axis=-1, keepdims=True)
        gt_ref[...] = (gm_ref[...] + (e - mean - unit * second) * inverse).astype(BF)


def project_back(dy, gathered, grank, tables, tokens, grad_middle, gain, tm):
    own = tokens.shape[0]
    rr, nc, _, w3 = gathered.shape
    width = w3 // 3
    wide3 = grank.shape[1]
    nm = own // tm
    final = lambda c, m: (jnp.where(c == nc - 1, m, 0), 0)
    return pl.pallas_call(
        functools.partial(project_back_kernel, tm, width),
        out_shape=jax.ShapeDtypeStruct((own, D), BF),
        grid=(nc, nm),
        in_specs=[
            pl.BlockSpec((1, tm, w3), lambda c, m: (c, m, 0)),
            pl.BlockSpec((rr, 1, D // rr, w3), lambda c, m: (0, c, 0, 0)),
            pl.BlockSpec((tm, wide3), lambda c, m: (jnp.where(c == 0, m, nm - 1), 0)),
            pl.BlockSpec((D, wide3), lambda c, m: (0, 0)),
            pl.BlockSpec((tm, D), final),
            pl.BlockSpec((tm, D), final),
            pl.BlockSpec((1, D), lambda c, m: (0, 0)),
        ],
        out_specs=pl.BlockSpec((tm, D), final),
        scratch_shapes=[pltpu.VMEM((own, D), F32)],
        compiler_params=params(2),
        cost_estimate=cost(2 * own * D * nc * w3 * 1.1, D * nc * w3 * 2 + own * (4 * D + nc * w3) * 2),
        name="project_back",
    )(dy, gathered, grank, tables, tokens, grad_middle, gain)


def out_kernel(nc, nm, group, per, ns, sets, scales, code, *refs):
    sources = refs[:ns]
    x_ref, w_ref, bias, odown, oup, gain, shift, fdown = refs[ns : ns + 8]
    att_out, middle_ref, normed_ref, ro_ref, r1_ref, a_scr = refs[ns + 8 :]
    m = pl.program_id(0)
    c = pl.program_id(1)
    choose(code[3 * (c * nm + m)], sources, a_scr, c)

    @pl.when(c == nc - 1)
    def _():
        att = jnp.concatenate([a_scr[i] for i in range(nc)], axis=1)
        att_out[...] = att
        ro = dot_t(att, odown[...]) * scales[m]
        keep = set_mask(ro.shape, sets[m], group, per)
        ro = jnp.where(keep, ro, 0.0).astype(BF)
        ro_ref[...] = ro
        middle = x_ref[...].astype(F32) + dot_t(att, w_ref[...]) + dot_t(ro, oup[...]) + bias[...]
        middle_ref[...] = middle
        unit, _ = norm_parts(middle)
        normed = (unit * gain[...] + shift[...]).astype(BF)
        normed_ref[...] = normed
        r1_ref[...] = jnp.where(keep, dot(normed, fdown[...]) * scales[m], 0.0).astype(BF)


def out_project(sources, code, tokens, wo_t, bias, odown, tables, gain, shift, sets, scales, tm, nc, per, rr):
    own = tokens.shape[0]
    width = D // nc
    group = SETS * per
    wide = group * rr
    nm = own // tm
    row = lambda m, c, *_: (m, 0)
    flat = lambda m, c, *_: (0, 0)
    return pl.pallas_call(
        functools.partial(out_kernel, nc, nm, group, per, len(sources)),
        out_shape=(
            jax.ShapeDtypeStruct((own, D), BF),
            jax.ShapeDtypeStruct((own, D), F32),
            jax.ShapeDtypeStruct((own, D), BF),
            jax.ShapeDtypeStruct((own, wide), BF),
            jax.ShapeDtypeStruct((own, wide), BF),
        ),
        grid_spec=pltpu.PrefetchScalarGridSpec(
            num_scalar_prefetch=3,
            grid=(nm, nc),
            in_specs=piece_specs(sources, tm, lambda m, c, s, a: c * nm + m)
            + [
                pl.BlockSpec((tm, D), row),
                pl.BlockSpec((D, D), flat),
                pl.BlockSpec((1, D), flat),
                pl.BlockSpec((wide, D), flat),
                pl.BlockSpec((D, wide), lambda m, c, *_: (0, 4)),
                pl.BlockSpec((1, D), flat),
                pl.BlockSpec((1, D), flat),
                pl.BlockSpec((D, wide), lambda m, c, *_: (0, 3)),
            ],
            out_specs=[
                pl.BlockSpec((tm, D), row),
                pl.BlockSpec((tm, D), row),
                pl.BlockSpec((tm, D), row),
                pl.BlockSpec((tm, wide), row),
                pl.BlockSpec((tm, wide), row),
            ],
            scratch_shapes=[pltpu.VMEM((nc, tm, width), BF)],
        ),
        compiler_params=params(2),
        cost_estimate=cost(2 * own * D * D * 1.5, D * D * 2 + own * D * 12),
        name="out_project",
    )(sets, scales, code, *sources, tokens, wo_t, bias, odown, tables, gain, shift, tables)


def out_back_kernel(nc, width, group, per, sets, scales, side, gb_ref, w_ref, oup, odown, att_ref, ro_ref, *outs):
    away_ref, mine_ref, gup_ref, gdown_ref, gup, gdown = outs
    m = pl.program_id(0)

    @pl.when(m == 0)
    def _():
        gup[...] = jnp.zeros_like(gup)
        gdown[...] = jnp.zeros_like(gdown)

    gb = gb_ref[...]
    gro = dot(gb, oup[...]) * scales[m]
    gro = jnp.where(set_mask(gro.shape, sets[m], group, per), gro, 0.0)
    ga = (dot(gb, w_ref[...]) + dot(gro.astype(BF), odown[...])).astype(BF)
    half = nc // 2
    for i in range(nc):
        piece = ga[:, i * width : (i + 1) * width]

        @pl.when(side[0] == i // half)
        def _(i=i, piece=piece):
            mine_ref[i % half, :, 0:width] = piece

        @pl.when(side[0] != i // half)
        def _(i=i, piece=piece):
            away_ref[i % half, :, 0:width] = piece

    gup[...] += dot(ro_ref[...].T, gb)
    gdown[...] += token_sum(gro, att_ref[...])

    @pl.when(m == pl.num_programs(0) - 1)
    def _():
        gup_ref[...] = gup[...].T.astype(BF)
        whole = gdown[...]
        for i in range(nc):
            for t, tile in enumerate(lane_tiles(whole[:, i * width : (i + 1) * width], group)):
                gdown_ref[:, i, t * group : (t + 1) * group, :] = tile.astype(BF)


def out_back(gb, wo_t, tables, odown, att, ro, sets, scales, side, tm, nc, per, rr):
    own = gb.shape[0]
    width = D // nc
    group = SETS * per
    wide = group * rr
    half = nc // 2
    tiles = -(-width // 128)
    row = lambda m, *_: (m, 0)
    flat = lambda m, *_: (0, 0)
    return pl.pallas_call(
        functools.partial(out_back_kernel, nc, width, group, per),
        out_shape=(
            jax.ShapeDtypeStruct((half, own, lanes_of(width)), BF),
            jax.ShapeDtypeStruct((half, own, lanes_of(width)), BF),
            jax.ShapeDtypeStruct((D, wide), BF),
            jax.ShapeDtypeStruct((rr, nc, tiles * group, 128), BF),
        ),
        grid_spec=pltpu.PrefetchScalarGridSpec(
            num_scalar_prefetch=3,
            grid=(own // tm,),
            in_specs=[
                pl.BlockSpec((tm, D), row),
                pl.BlockSpec((D, D), flat),
                pl.BlockSpec((D, wide), lambda m, *_: (0, 4)),
                pl.BlockSpec((wide, D), flat),
                pl.BlockSpec((tm, D), row),
                pl.BlockSpec((tm, wide), row),
            ],
            out_specs=[
                pl.BlockSpec((half, tm, lanes_of(width)), lambda m, *_: (0, m, 0)),
                pl.BlockSpec((half, tm, lanes_of(width)), lambda m, *_: (0, m, 0)),
                pl.BlockSpec((D, wide), flat),
                pl.BlockSpec((rr, nc, tiles * group, 128), lambda m, *_: (0, 0, 0, 0)),
            ],
            scratch_shapes=[pltpu.VMEM((wide, D), F32), pltpu.VMEM((wide, D), F32)],
        ),
        compiler_params=params(1),
        cost_estimate=cost(2 * own * D * D * 1.5, D * D * 2 + own * D * 6),
        name="out_back",
    )(sets, scales, side, gb, wo_t, tables, odown, att, ro)


def mlp_kernel(tm, nm, group, per, sets, scales, *refs):
    n_ref, g_ref, mid_ref, w1_ref, w2_ref, b1, up1_ref, down2_ref, up2, down1, r1_ref, bias2, gain = refs[:13]
    out_ref, gm_ref, gb_ref, gup1_ref, gdown2_ref, gup2_ref, gdown1_ref = refs[13:20]
    acc, gacc, r2acc, gr1acc, gr2, gup1, gdown2, gup2, gdown1 = refs[20:]
    c = pl.program_id(0)
    m = pl.program_id(1)
    rows = pl.ds(pl.multiple_of(m * tm, tm), tm)
    a = scales[m]
    g = g_ref[...]
    normed = n_ref[...]
    hidden = w1_ref.shape[-1]
    wide = r1_ref.shape[1]
    keep = set_mask((tm, wide), sets[m], group, per)

    @pl.when(c == 0)
    def _():
        gr2[rows, :] = jnp.where(keep, dot(g, up2[...]) * a, 0.0).astype(BF)
        acc[rows, :] = jnp.zeros((tm, D), F32)
        gacc[rows, :] = jnp.zeros((tm, D), F32)
        r2acc[rows, :] = jnp.zeros((tm, wide), F32)
        gr1acc[rows, :] = jnp.zeros((tm, wide), F32)

    @pl.when(m == 0)
    def _():
        gup1[...] = jnp.zeros_like(gup1)
        gdown2[...] = jnp.zeros_like(gdown2)

    @pl.when((m == 0) & (c == 0))
    def _():
        gup2[...] = jnp.zeros_like(gup2)
        gdown1[...] = jnp.zeros_like(gdown1)

    w1 = w1_ref[:, 0].reshape(D, hidden)
    w2 = w2_ref[:, 0].reshape(D, hidden)
    up1 = up1_ref[:, 0].reshape(wide, hidden)
    down2 = down2_ref[:, 0].reshape(wide, hidden)
    r1 = r1_ref[...]
    grank2 = gr2[rows, :]
    pre = dot(normed, w1) + dot(r1, up1) + b1[0]
    upper = 0.5 + 0.5 * lax.erf(pre * (0.5**0.5))
    density = jnp.exp(pre * pre * -0.5) * ((2.0 * math.pi) ** -0.5)
    act = (pre * upper).astype(BF)
    slope = upper + pre * density
    gact = dot(g, w2) + dot(grank2, down2)
    gpre = (gact * slope).astype(BF)
    acc[rows, :] += dot_t(act, w2)
    r2acc[rows, :] += dot_t(act, down2)
    gacc[rows, :] += dot_t(gpre, w1)
    gr1acc[rows, :] += dot_t(gpre, up1)
    gdown2[...] += dot(grank2.T, act)
    gup1[...] += dot(r1.T, gpre)

    @pl.when(m == nm - 1)
    def _():
        put_tiles(gup1_ref, 0, gup1[...], group)
        put_tiles(gdown2_ref, 0, gdown2[...], group)

    @pl.when(c == pl.num_programs(0) - 1)
    def _():
        r2 = jnp.where(keep, r2acc[rows, :] * a, 0.0).astype(BF)
        middle = mid_ref[...]
        out_ref[...] = (middle + acc[rows, :] + dot_t(r2, up2[...]) + bias2[...]).astype(BF)
        gup2[...] += dot(r2.T, g)
        gr1 = jnp.where(keep, gr1acc[rows, :] * a, 0.0).astype(BF)
        e = (gacc[rows, :] + dot_t(gr1, down1[...])) * gain[...]
        gdown1[...] += dot(gr1.T, normed)
        unit, inverse = norm_parts(middle)
        mean = jnp.mean(e, axis=-1, keepdims=True)
        second = jnp.mean(e * unit, axis=-1, keepdims=True)
        gm = g.astype(F32) + (e - mean - unit * second) * inverse
        gm_ref[...] = gm
        gb_ref[...] = gm.astype(BF)

        @pl.when(m == nm - 1)
        def _():
            gup2_ref[...] = gup2[...].T.astype(BF)
            gdown1_ref[...] = gdown1[...].T.astype(BF)


def mlp(normed, g, middle, gathered, b1, tables, r1, bias2, gain, sets, scales, tm, per, at):
    own = g.shape[0]
    rr, nc, _, hidden = gathered.shape
    group = SETS * per
    wide = group * rr
    nm = own // tm
    tiles = -(-hidden // 128)
    row = lambda c, m, *_: (m, 0)
    final = lambda c, m, *_: (jnp.where(c == nc - 1, m, 0), 0)
    flat = lambda c, m, *_: (0, 0)
    wblock = (rr, 1, D // rr, hidden)
    return pl.pallas_call(
        functools.partial(mlp_kernel, tm, nm, group, per),
        out_shape=(
            jax.ShapeDtypeStruct((own, D), BF),
            jax.ShapeDtypeStruct((own, D), F32),
            jax.ShapeDtypeStruct((own, D), BF),
            jax.ShapeDtypeStruct((rr, nc, tiles * group, 128), BF),
            jax.ShapeDtypeStruct((rr, nc, tiles * group, 128), BF),
            jax.ShapeDtypeStruct((D, wide), BF),
            jax.ShapeDtypeStruct((D, wide), BF),
        ),
        grid_spec=pltpu.PrefetchScalarGridSpec(
            num_scalar_prefetch=2,
            grid=(nc, nm),
            in_specs=[
                pl.BlockSpec((tm, D), row),
                pl.BlockSpec((tm, D), row),
                pl.BlockSpec((tm, D), final, pipeline_mode=pl.Buffered(1)),
                pl.BlockSpec(wblock, lambda c, m, *_: (0, c, 0, 0)),
                pl.BlockSpec(wblock, lambda c, m, *_: (0, c, 1, 0)),
                pl.BlockSpec((1, 1, hidden), lambda c, m, *_: (c, 0, 0)),
                pl.BlockSpec((rr, 1, group, hidden), lambda c, m, *_: (0, c, at // group, 0)),
                pl.BlockSpec((rr, 1, group, hidden), lambda c, m, *_: (0, c, at // group + 1, 0)),
                pl.BlockSpec((D, wide), lambda c, m, *_: (0, 5), pipeline_mode=pl.Buffered(1)),
                pl.BlockSpec((D, wide), lambda c, m, *_: (0, 3), pipeline_mode=pl.Buffered(1)),
                pl.BlockSpec((tm, wide), row),
                pl.BlockSpec((1, D), flat),
                pl.BlockSpec((1, D), flat),
            ],
            out_specs=[
                pl.BlockSpec((tm, D), final),
                pl.BlockSpec((tm, D), final),
                pl.BlockSpec((tm, D), final),
                pl.BlockSpec((rr, 1, tiles * group, 128), lambda c, m, *_: (0, c, 0, 0)),
                pl.BlockSpec((rr, 1, tiles * group, 128), lambda c, m, *_: (0, c, 0, 0)),
                pl.BlockSpec((D, wide), flat),
                pl.BlockSpec((D, wide), flat),
            ],
            scratch_shapes=[
                pltpu.VMEM((own, D), F32),
                pltpu.VMEM((own, D), F32),
                pltpu.VMEM((own, wide), F32),
                pltpu.VMEM((own, wide), F32),
                pltpu.VMEM((own, wide), BF),
                pltpu.VMEM((wide, hidden), F32),
                pltpu.VMEM((wide, hidden), F32),
                pltpu.VMEM((wide, D), F32),
                pltpu.VMEM((wide, D), F32),
            ],
        ),
        compiler_params=params(2, 67043328),
        cost_estimate=cost(8 * own * D * nc * hidden * 1.2, D * nc * hidden * 4 + own * D * 30, own * nc * hidden * 2),
        name="mlp",
    )(
        sets, scales, normed, g, middle, gathered, gathered, b1, gathered, gathered, tables, tables, r1, bias2, gain
    )


def assemble_kernel(width, parts, w_ref, o_ref, w_out, o_out):
    _, nc = w_ref.shape[:2]
    columns, downs = [], []
    for c in range(nc):
        block = w_ref[:, c]
        rows = [block[:, :, j * width : (j + 1) * width] for j in range(parts)]
        columns.append(jnp.concatenate(rows, axis=1).reshape(D, width))
        downs.append(o_ref[:, c, :, 0:width].reshape(-1, width))
    w_out[...] = jnp.concatenate(columns, axis=1)
    o_out[...] = jnp.concatenate(downs, axis=1)


def assemble(gathered, at_w, rows_w, at_o, group, width):
    nr, nc, _, hidden = gathered.shape
    parts = hidden // width
    if rows_w % 8 == 0 and at_w % rows_w == 0:
        return pl.pallas_call(
            functools.partial(assemble_kernel, width, parts),
            out_shape=(
                jax.ShapeDtypeStruct((D, D), BF),
                jax.ShapeDtypeStruct((nr * group, D), BF),
            ),
            grid=(1,),
            in_specs=[
                pl.BlockSpec((nr, nc, rows_w, hidden), lambda i: (0, 0, at_w // rows_w, 0)),
                pl.BlockSpec((nr, nc, group, hidden), lambda i: (0, 0, at_o // group, 0)),
            ],
            out_specs=[
                pl.BlockSpec((D, D), lambda i: (0, 0)),
                pl.BlockSpec((nr * group, D), lambda i: (0, 0)),
            ],
            compiler_params=params(1),
            name="assemble",
        )(gathered, gathered)
    w = gathered[:, :, at_w : at_w + rows_w].reshape(nr, nc, rows_w, parts, width)
    o = gathered[:, :, at_o : at_o + group, :width]
    return (
        w.transpose(0, 3, 2, 1, 4).reshape(D, D),
        o.transpose(0, 2, 1, 3).reshape(nr * group, D),
    )


def pick(flag, first, second):
    return jnp.where(flag, first, second)


def table_of(values):
    return jnp.stack([jnp.asarray(v, jnp.int32) for v in values])


class Exchange:
    def __init__(self, nc, own, clips, clip_len, tm):
        self.nc, self.own, self.clips, self.clip_len, self.tm = nc, own, clips, clip_len, tm
        self.local = nc == 4 and clips == 3 and own == 3 * tm and clip_len == 4 * tm
        col = lax.axis_index("cols")
        self.nm = nm = own // tm
        if not self.local:
            self.order = jnp.arange(nc, dtype=jnp.int32)
            self.side = jnp.ones((1,), jnp.int32)
            self.plans = [jnp.zeros((2,), jnp.int32)]
            self.indices = [jnp.arange(clips, dtype=jnp.int32)]
            entry = jnp.arange(nc * nm, dtype=jnp.int32)
            self.code = jnp.stack([entry * 0, entry // nm, entry % nm], axis=1).reshape(-1)
            return
        y, k = col // 2, col % 2
        self.y, self.k = y, k
        self.holder = y != k
        self.order = (jnp.arange(4, dtype=jnp.int32) + 2 * (1 - k)) % 4
        self.side = k[None]
        b = jnp.arange(4, dtype=jnp.int32)
        g = b + 2 * y
        clip_plan = jnp.concatenate([pick(g // 3 == k, 0, 1), g % 3])
        g = pick(y == 0, 4 + b, b - 2)
        near = b // 2 == y
        source = pick(near, pick(g // 3 == k, 0, 1), pick(self.holder, 3, 2))
        shared_plan = jnp.concatenate([source, pick(near, g % 3, b % 2)])
        self.plans = [clip_plan.astype(jnp.int32), shared_plan.astype(jnp.int32)]
        self.indices = [jnp.array([0, 1, 0, 1], jnp.int32), table_of([y, y, 0, 0])]
        entry = jnp.arange(12, dtype=jnp.int32)
        c, m = entry // 3, entry % 3
        g = 3 * k + m
        inside = (g >= 2 * y) & (g < 2 * y + 4)
        same, idx = c // 2 == k, c % 2
        source = pick(
            inside,
            pick(same, 0, 2),
            pick(idx == y, pick(same, 1, 3), pick(same, 4, 5)),
        )
        block = pick(
            inside,
            g - 2 * y,
            pick(y == 0, g - 4, pick(idx == y, g + 2, g)),
        )
        self.code = (
            jnp.stack([source, pick(inside, idx, 0), block], axis=1).astype(jnp.int32).reshape(-1)
        )

    def lens(self, lengths):
        if not self.local:
            return (lengths,)
        mine = pick(self.y == 0, lengths[0], lengths[2])
        return (jnp.stack([mine, mine]), lengths[1:2])

    def to_heads(self, away, mine):
        f = mine.shape[-1]
        if not self.local:
            moved = lax.all_to_all(jnp.concatenate([away, mine]), "cols", 0, 0, tiled=True)
            return [[moved.reshape(self.clips, self.clip_len, f)]]
        y, k, half = self.y, self.k, self.clip_len // 2
        start = pick(k == 1, self.own - half, 0)
        got = lax.ppermute(away, "cols", [(i, i ^ 1) for i in range(4)])
        one = lax.dynamic_slice(mine, (1 - y, start, 0), (1, half, f))
        two = lax.dynamic_slice(away, (1 - y, start, 0), (1, half, f))
        got_one = lax.ppermute(one, "cols", [(1, 3), (2, 0)])
        got_two = lax.ppermute(two, "cols", [(1, 2), (2, 1)])
        return [[mine, got], [mine, got, got_one, got_two]]

    def from_heads(self, parts):
        if not self.local:
            (v,) = parts
            v = v.reshape(self.nc, self.own, v.shape[-1])
            return [lax.all_to_all(v, "cols", 0, 0, tiled=True)]
        clip, shared = parts
        half = self.clip_len // 2
        far = lax.dynamic_slice(shared, (0, (1 - self.y) * half, 0), (1, half, clip.shape[-1]))
        swap = [(i, i ^ 1) for i in range(4)]
        got_one = lax.ppermute(far, "cols", [(3, 1), (0, 2)])
        got_two = lax.ppermute(far, "cols", [(2, 1), (1, 2)])
        got_shared = lax.ppermute(shared, "cols", swap)
        return [clip, shared, lax.ppermute(clip, "cols", swap), got_shared, got_one, got_two]


def up_to(n, k):
    return -(-n // k) * k


def rows_padded(v, rows, lanes):
    return jnp.pad(v.astype(BF), ((0, rows - v.shape[0]), (0, lanes - v.shape[1])))


def halves(v):
    high = v.astype(BF)
    return high, (v - high.astype(F32)).astype(BF)


def scatter_sum(pieces):
    whole = jnp.concatenate(pieces, axis=2)
    n = whole.shape[2]
    whole = jnp.pad(whole, ((0, 0), (0, 0), (0, up_to(n, 8) - n), (0, 0)))
    return whole.reshape(-1, 128)


def join(v, nc):
    col = lax.axis_index("cols")
    zeros = (0,) * v.ndim
    held = lax.dynamic_update_slice(jnp.zeros((nc,) + v.shape, v.dtype), v[None], (col,) + zeros)
    step = 1
    while step < nc:
        base = col // step * step
        sent = lax.dynamic_slice(held, (base,) + zeros, (step,) + v.shape)
        got = lax.ppermute(sent, "cols", [(i, i ^ step) for i in range(nc)])
        held = lax.dynamic_update_slice(held, got, (base ^ step,) + zeros)
        step *= 2
    return held


def body(
    tokens,
    cotangent,
    clip_lengths,
    clip_sets,
    clip_scales,
    norm1_gain,
    norm1_shift,
    w_query,
    query_bias,
    w_key,
    w_value,
    value_bias,
    w_out,
    out_bias,
    norm2_gain,
    norm2_shift,
    w_fc1,
    fc1_bias,
    w_fc2,
    fc2_bias,
    query_down,
    query_up,
    key_down,
    key_up,
    value_down,
    value_up,
    out_down,
    out_up,
    fc1_down,
    fc1_up,
    fc2_down,
    fc2_up,
):
    nr = lax.axis_size("rows")
    nc = lax.axis_size("cols")
    col = lax.axis_index("cols")
    clips = clip_lengths.shape[0]
    own = tokens.shape[0]
    clip_len = own * nc // clips
    tm = math.gcd(own, clip_len)
    width = query_bias.shape[0]
    hidden = fc1_bias.shape[0]
    hh = width // HEAD_DIM
    dr = w_query.shape[0]
    per = RANK // nr
    group = SETS * per
    wide = group * nr
    dc = dr // nc
    exchange = Exchange(nc, own, clips, clip_len, tm)

    block_clip = (col * own + jnp.arange(own // tm, dtype=jnp.int32) * tm) // clip_len
    sets = jnp.take(clip_sets, block_clip)
    scales = jnp.take(clip_scales, block_clip)

    downs = jnp.stack([query_down, key_down, value_down, fc1_down])
    downs = lax.dynamic_slice(downs, (0, 0, col * dc, 0), (4, SETS, dc, RANK))
    downs = downs.reshape(4, SETS, dc, nr, per).transpose(2, 0, 3, 1, 4).reshape(dc, 4 * wide)
    ups = jnp.stack([out_up, fc2_up])
    ups = lax.dynamic_slice(ups, (0, 0, 0, col * dc), (2, SETS, RANK, dc))
    ups = ups.reshape(2, SETS, nr, per, dc).transpose(4, 0, 2, 1, 3).reshape(dc, 2 * wide)
    tables = jnp.concatenate([downs, ups], axis=1)

    lanes = 3 * width
    qh, ql = halves(query_bias)
    vh, vl = halves(value_bias)
    none = jnp.zeros_like(qh)
    ids = jnp.pad(clip_sets.astype(BF), (0, lanes - clips))
    natural = lanes >= 6 * wide
    small = rows_padded(tables, dc, lanes) if natural else tables.reshape(-1, lanes)
    small_rows = small.shape[0]
    at_bias = dr + group
    at_table = up_to(at_bias + 3, 16)
    packed = jnp.concatenate(
        [
            jnp.concatenate([w_query, w_key, w_value], axis=1),
            jnp.concatenate([v.reshape(group, width) for v in (query_up, key_up, value_up)], axis=1),
            rows_padded(
                jnp.stack([jnp.concatenate([qh, none, vh]), jnp.concatenate([ql, none, vl]), ids]),
                at_table - at_bias,
                lanes,
            ),
            rows_padded(small, up_to(small_rows, 16), lanes),
        ],
        axis=0,
    )
    g1 = lax.all_gather(packed, BOTH, axis=0).reshape(nr, nc, -1, lanes)
    tables = g1[:, :, at_table : at_table + small_rows]
    if natural:
        tables = tables[..., : 6 * wide]
    tables = tables.reshape(D, 6 * wide)
    every_set = g1[:, 0, at_bias + 2, :clips].astype(jnp.int32)
    bias_qkv = jnp.sum(g1[0, :, at_bias : at_bias + 2].astype(F32), axis=1, keepdims=True)

    parts = hidden // width
    rows_w = dr // parts
    at_w = 2 * dr
    at_f = up_to(at_w + rows_w, 16)
    at_o = at_f + 2 * group
    at_b = at_o + group
    wo = w_out.T.reshape(parts, rows_w, width).transpose(1, 0, 2).reshape(rows_w, hidden)
    turn = lambda v: jnp.swapaxes(v, 1, 2).reshape(group, -1)
    packed = jnp.concatenate(
        [
            w_fc1,
            w_fc2.T,
            rows_padded(wo, at_f - at_w, hidden),
            fc1_up.reshape(group, hidden),
            turn(fc2_down),
            rows_padded(turn(out_down), group, hidden),
            rows_padded(jnp.stack(halves(fc1_bias)), 16, hidden),
        ],
        axis=0,
    )
    packed, g1 = lax.optimization_barrier((packed, g1))
    g2 = lax.all_gather(packed, BOTH, axis=0).reshape(nr, nc, -1, hidden)
    wo_t, odown = assemble(g2, at_w, rows_w, at_o, group, width)
    b1 = jnp.sum(g2[0, :, at_b : at_b + 2].astype(F32), axis=1, keepdims=True)

    gain1, shift1 = norm1_gain[None], norm1_shift[None]
    gain2, shift2 = norm2_gain[None], norm2_shift[None]

    normed, ranks, away, mine = project(
        tokens, gain1, shift1, g1, bias_qkv, tables, sets, scales, exchange.order, tm, per
    )
    lens = exchange.lens(clip_lengths)
    results = []
    for sources, plan, index, n in zip(
        exchange.to_heads(away, mine), exchange.plans, exchange.indices, lens
    ):
        if results:
            n, _ = lax.optimization_barrier((n, results[-1][1]))
        results.append(attend(sources, plan, index, n, clip_len, hh))
    pieces = exchange.from_heads([r[0] for r in results])
    att, middle, normed_mlp, ro, r1 = out_project(
        pieces, exchange.code, tokens, wo_t, out_bias[None], odown, tables, gain2, shift2, sets, scales, tm, nc, per, nr
    )
    output, grad_middle, grad_branch, gup1, gdown2, gup2, gdown1 = mlp(
        normed_mlp, cotangent, middle, g2, b1, tables, r1, fc2_bias[None], gain2, sets, scales, tm, per, at_f
    )
    away, mine, goup, godown = out_back(
        grad_branch, wo_t, tables, odown, att, ro, sets, scales, exchange.side, tm, nc, per, nr
    )

    by_model = lambda v: v.reshape(nr, nc, dc, wide)
    late = scatter_sum([gup1, gdown2, godown, by_model(gdown1), by_model(goup), by_model(gup2)])
    late, away, mine = lax.optimization_barrier((late, away, mine))
    late = lax.psum_scatter(late, BOTH, scatter_dimension=0, tiled=True)

    def untile(v, n):
        t = v.shape[0] // group
        return v.reshape(t, group, 128).transpose(1, 0, 2).reshape(group, t * 128)[:, :n].reshape(SETS, per, n)

    def model_tables(v):
        k = v.shape[0] // dc
        every = join(v, nc).reshape(nc, k, dc, wide).swapaxes(0, 1)
        return every.reshape(k, dr, nr, SETS, per)

    as_down = lambda v: v.transpose(2, 0, 1, 3).reshape(SETS, dr, RANK)
    as_up = lambda v: v.transpose(2, 1, 3, 0).reshape(SETS, RANK, dr)
    flip = lambda v: jnp.swapaxes(v, 1, 2)
    calls = list(
        zip(exchange.to_heads(away, mine), exchange.plans, exchange.indices, results, lens)
    )
    backs = []
    for sources, plan, index, (o, lse, x), n in reversed(calls):
        if backs:
            n, _ = lax.optimization_barrier((n, backs[-1]))
        backs.append(attend_back(sources, plan, index, x, o, lse, n, hh))
    pieces = exchange.from_heads(backs[::-1])
    dy, grank, gup, gdown = adapt_back(
        pieces, exchange.code, g1, normed, ranks, sets, scales, block_clip, clips, tm, per
    )
    tiles = gup.shape[1] // (3 * clips)
    folded = gdown.shape[0]
    ups = gup.reshape(nc, clips * 3 * tiles, nr, per, 128).transpose(2, 0, 1, 3, 4)
    ups = ups.reshape(nr, nc, -1, 128)
    downs = [gdown[i].reshape(nr, nc, dc, 128) for i in range(folded)]
    last = scatter_sum([ups] + downs).reshape(nr * nc, -1, 128)
    last, dy = lax.optimization_barrier((last, dy))
    got = lax.all_to_all(last, BOTH, 0, 0, tiled=True)
    grad_tokens = project_back(dy, g1, grank, tables, tokens, grad_middle, gain1, tm)
    late, grad_tokens = lax.optimization_barrier((late, grad_tokens))
    summed = late.astype(F32)
    a = gup1.shape[2]
    b = godown.shape[2]
    grad_fc1_up = untile(summed[:a], hidden)
    grad_fc2_down = flip(untile(summed[a : 2 * a], hidden))
    grad_out_down = flip(untile(summed[2 * a : 2 * a + b], width))
    model = model_tables(summed[2 * a + b : 2 * a + b + 3 * dc])
    grad_fc1_down, grad_out_up, grad_fc2_up = as_down(model[0]), as_up(model[1]), as_up(model[2])

    got = jnp.sum(got.reshape(nr, nc, -1, 128).astype(F32), axis=1)
    onehot = (every_set[:, :, None] == jnp.arange(SETS, dtype=jnp.int32)).astype(F32)
    n = ups.shape[2]
    per_clip = got[:, :n].reshape(nr, clips, -1, 128)
    per_set = jnp.sum(onehot[:, :, :, None, None] * per_clip[:, :, None], axis=(0, 1))
    per_set = per_set.reshape(SETS, 3, tiles, per, 128).transpose(1, 0, 3, 2, 4)
    up = per_set.reshape(3, SETS, per, tiles * 128)[..., :width]
    side = got[:, n : n + folded * dc].reshape(nr, folded, dc, 128).transpose(0, 2, 1, 3)
    side = side.reshape(nr, dc, folded * 128)[..., : clips * 3 * RANK]
    side = side.reshape(nr, dc, clips, 3 * RANK).transpose(0, 2, 1, 3)
    side = jnp.sum(onehot[:, :, :, None, None] * side[:, :, None], axis=(0, 1))
    side = side.transpose(1, 0, 2).reshape(dc, SETS * 3 * RANK)
    side = lax.all_gather(side, "cols", axis=0, tiled=True).reshape(dr, SETS, 3, RANK)
    down = side.transpose(2, 1, 0, 3)
    return (
        output,
        grad_tokens,
        down[0],
        up[0],
        down[1],
        up[1],
        down[2],
        up[2],
        grad_out_down,
        grad_out_up,
        grad_fc1_down,
        grad_fc1_up,
        grad_fc2_down,
        grad_fc2_up,
    )


def solution(mesh):
    both = P(("rows", "cols"), None)
    grid = P("rows", "cols")
    turned = P("cols", "rows")
    down = P(None, "rows", None)
    up = P(None, "rows", "cols")
    far_down = P(None, "cols", "rows")
    far_up = P(None, None, "rows")
    return jax.shard_map(
        body,
        mesh=mesh,
        in_specs=(
            both,
            both,
            P("rows"),
            P("rows"),
            P("rows"),
            P(),
            P(),
            grid,
            P("cols"),
            grid,
            grid,
            P("cols"),
            turned,
            P(),
            P(),
            P(),
            grid,
            P("cols"),
            turned,
            P(),
            down,
            up,
            down,
            up,
            down,
            up,
            far_down,
            far_up,
            down,
            up,
            far_down,
            far_up,
        ),
        out_specs=(
            both,
            both,
            down,
            up,
            down,
            up,
            down,
            up,
            far_down,
            far_up,
            down,
            up,
            far_down,
            far_up,
        ),
        check_vma=False,
    )
```

```python
import functools
import math

import jax
import jax.numpy as jnp
from jax import lax
from jax.experimental import pallas as pl
from jax.experimental.pallas import tpu as pltpu
from jax.sharding import PartitionSpec as P


D = 1280
SETS = 8
RANK = 16
HEAD_DIM = 80
EPSILON = 1e-05
LOG2E = 1.4426950408889634
LOW = -1e30
F32 = jnp.float32
BF = jnp.bfloat16
BOTH = ("rows", "cols")


def dot(a, b):
    return lax.dot_general(a, b, (((1,), (0,)), ((), ())), preferred_element_type=F32)


def dot_t(a, b):
    return lax.dot_general(a, b, (((1,), (1,)), ((), ())), preferred_element_type=F32)


def token_sum(a, b):
    return dot(a.T.astype(BF), b)


def norm_parts(x):
    mean = jnp.mean(x, axis=-1, keepdims=True)
    centred = x - mean
    inverse = lax.rsqrt(jnp.mean(centred * centred, axis=-1, keepdims=True) + EPSILON)
    return centred * inverse, inverse


def params(n, limit=60 << 20):
    return pltpu.CompilerParams(
        dimension_semantics=("arbitrary",) * n, vmem_limit_bytes=limit
    )


def cost(flops, nbytes, trans=0):
    return pl.CostEstimate(flops=int(flops), bytes_accessed=int(nbytes), transcendentals=int(trans))


def set_mask(shape, which, group, per):
    column = lax.broadcasted_iota(jnp.int32, shape, len(shape) - 1)
    return (column % group) // per == which


def choose(code, refs, dst, at):
    for j, ref in enumerate(refs):

        @pl.when(code == j)
        def _(ref=ref):
            dst[at] = ref[0, :, 0 : dst.shape[-1]]


def gather_clip(refs, plan, dst, bs):
    blocks = plan.shape[0] // 2
    for b in range(blocks):
        rows = slice(b * bs, (b + 1) * bs)
        for j, ref in enumerate(refs):

            @pl.when(plan[b] == j)
            def _(ref=ref, b=b, rows=rows):
                off = pl.multiple_of(plan[blocks + b] * bs, bs)
                dst[0, rows, :] = ref[0, pl.ds(off, bs), 0 : dst.shape[2]]


def attend_kernel(hh, length, qb, kb, ns, lens, plan, index, *refs):
    sources, (o_ref, lse_ref, x_ref, k_scr, vt_scr, acc, m_scr, l_scr) = refs[:ns], refs[ns:]
    p = pl.program_id(0)
    qi = pl.program_id(1)
    w = hh * HEAD_DIM
    c = HEAD_DIM**-0.5 * LOG2E

    @pl.when(qi == 0)
    def _():
        gather_clip(sources, plan, x_ref, 2 * length // plan.shape[0])
        vt_scr[...] = x_ref[0, :, 2 * w : 3 * w].T
        for h in range(hh):
            k_scr[h] = x_ref[0, :, w + h * HEAD_DIM : w + (h + 1) * HEAD_DIM]

    size = lens[p]
    block = x_ref[0, pl.ds(pl.multiple_of(qi * qb, qb), qb), 0:w]
    qs = [block[:, h * HEAD_DIM : (h + 1) * HEAD_DIM] for h in range(hh)]
    m_scr[...] = jnp.full_like(m_scr, LOW)
    l_scr[...] = jnp.zeros_like(l_scr)
    acc[...] = jnp.zeros_like(acc)

    def chunk(i, masked):
        r0 = pl.multiple_of(i * kb, kb)
        for h in range(hh):
            s = dot_t(k_scr[h, pl.ds(r0, kb), :], qs[h])
            if masked:
                keys = lax.broadcasted_iota(jnp.int32, (kb, qb), 0) + i * kb
                s = jnp.where(keys < size, s, LOW)
            old = m_scr[h : h + 1]
            top = jnp.maximum(old, jnp.max(s, axis=0, keepdims=True))
            probs = jnp.exp2((s - top) * c)
            shrink = jnp.exp2((old - top) * c)
            l_scr[h : h + 1] = l_scr[h : h + 1] * shrink + jnp.sum(probs, axis=0, keepdims=True)
            m_scr[h : h + 1] = top
            acc[h] = acc[h] * shrink + dot(
                vt_scr[h * HEAD_DIM : (h + 1) * HEAD_DIM, pl.ds(r0, kb)], probs.astype(BF)
            )

    full = size // kb

    def step(i, carry):
        chunk(i, False)
        return carry

    lax.fori_loop(0, full, step, 0)

    @pl.when(full * kb < size)
    def _():
        chunk(full, True)

    outs = [acc[h] * (1.0 / l_scr[h : h + 1]) for h in range(hh)]
    o_ref[0, :, 0:w] = jnp.concatenate(outs, axis=0).T.astype(BF)
    lse_ref[0] = m_scr[0:hh] * c + jnp.log2(l_scr[0:hh])


def lanes_of(n):
    return -(-n // 128) * 128


def source_specs(sources, problems):
    def spec(j, v):
        return pl.BlockSpec(
            (1,) + v.shape[1:], lambda p, q, l, plan, index: (index[j * problems + p], 0, 0)
        )

    return [spec(j, v) for j, v in enumerate(sources)]


def attend(sources, plan, index, lens, length, hh):
    problems = lens.shape[0]
    w3 = 3 * hh * HEAD_DIM
    w = hh * HEAD_DIM
    qb = math.gcd(length, 512)
    kb = math.gcd(length, 768)
    return pl.pallas_call(
        functools.partial(attend_kernel, hh, length, qb, kb, len(sources)),
        out_shape=(
            jax.ShapeDtypeStruct((problems, length, lanes_of(w)), BF),
            jax.ShapeDtypeStruct((problems, hh, length), F32),
            jax.ShapeDtypeStruct((problems, length, w3), BF),
        ),
        grid_spec=pltpu.PrefetchScalarGridSpec(
            num_scalar_prefetch=3,
            grid=(problems, length // qb),
            in_specs=source_specs(sources, problems),
            out_specs=[
                pl.BlockSpec((1, qb, lanes_of(w)), lambda p, q, *_: (p, q, 0)),
                pl.BlockSpec((1, hh, qb), lambda p, q, *_: (p, 0, q)),
                pl.BlockSpec((1, length, w3), lambda p, q, *_: (p, 0, 0)),
            ],
            scratch_shapes=[
                pltpu.VMEM((hh, length, HEAD_DIM), BF),
                pltpu.VMEM((w, length), BF),
                pltpu.VMEM((hh, HEAD_DIM, qb), F32),
                pltpu.VMEM((max(8, hh), qb), F32),
                pltpu.VMEM((max(8, hh), qb), F32),
            ],
        ),
        compiler_params=params(2),
        cost_estimate=cost(
            problems * hh * 4 * length * length * 256,
            problems * length * w3 * 6,
            problems * hh * length * length,
        ),
        name="attend",
    )(lens, plan, index, *sources)


def attend_back_kernel(hh, length, qb, kb, ns, lens, plan, index, *refs):
    sources = refs[:ns]
    x_ref, o_ref, lse_ref, dx_ref, do_scr, k_scr, v_scr, kt_scr, dk, dv, dqt = refs[ns:]
    p = pl.program_id(0)
    qi = pl.program_id(1)
    w = hh * HEAD_DIM
    scale = HEAD_DIM**-0.5
    c = scale * LOG2E

    @pl.when(qi == 0)
    def _():
        gather_clip(sources, plan, do_scr, 2 * length // plan.shape[0])
        kt_scr[...] = x_ref[0, :, w : 2 * w].T
        for h in range(hh):
            k_scr[h] = x_ref[0, :, w + h * HEAD_DIM : w + (h + 1) * HEAD_DIM]
            v_scr[h] = x_ref[0, :, 2 * w + h * HEAD_DIM : 2 * w + (h + 1) * HEAD_DIM]
        dk[...] = jnp.zeros_like(dk)
        dv[...] = jnp.zeros_like(dv)

    size = lens[p]
    rows = pl.ds(pl.multiple_of(qi * qb, qb), qb)
    block = x_ref[0, rows, 0:w]
    qs = [block[:, h * HEAD_DIM : (h + 1) * HEAD_DIM] for h in range(hh)]
    do = do_scr[0, rows, :]
    dos = [do[:, h * HEAD_DIM : (h + 1) * HEAD_DIM] for h in range(hh)]
    prod = (do.astype(F32) * o_ref[0, :, 0:w].astype(F32)).T
    inner = [
        jnp.sum(prod[h * HEAD_DIM : (h + 1) * HEAD_DIM], axis=0, keepdims=True) for h in range(hh)
    ]
    dqt[...] = jnp.zeros_like(dqt)

    def chunk(i, masked):
        keys_at = pl.ds(pl.multiple_of(i * kb, kb), kb)
        for h in range(hh):
            s = dot_t(k_scr[h, keys_at, :], qs[h])
            probs = jnp.exp2(s * c - lse_ref[0, h : h + 1])
            if masked:
                keys = lax.broadcasted_iota(jnp.int32, (kb, qb), 0) + i * kb
                probs = jnp.where(keys < size, probs, 0.0)
            dp = dot_t(v_scr[h, keys_at, :], dos[h])
            ds = (probs * (dp - inner[h])).astype(BF)
            dv[h, keys_at, :] += dot(probs.astype(BF), dos[h])
            dk[h, keys_at, :] += dot(ds, qs[h])
            dqt[h] += dot(kt_scr[h * HEAD_DIM : (h + 1) * HEAD_DIM, keys_at], ds)

    full = size // kb

    def step(i, carry):
        chunk(i, False)
        return carry

    lax.fori_loop(0, full, step, 0)

    @pl.when(full * kb < size)
    def _():
        chunk(full, True)

    dq = jnp.concatenate([dqt[h] for h in range(hh)], axis=0).T * scale
    dx_ref[0, rows, 0:w] = dq.astype(BF)

    @pl.when(qi == pl.num_programs(1) - 1)
    def _():
        for h in range(hh):
            dx_ref[0, :, w + h * HEAD_DIM : w + (h + 1) * HEAD_DIM] = (dk[h] * scale).astype(BF)
            dx_ref[0, :, 2 * w + h * HEAD_DIM : 2 * w + (h + 1) * HEAD_DIM] = dv[h].astype(BF)


def attend_back(sources, plan, index, x, o, lse, lens, hh):
    problems, length, w3 = x.shape
    w = hh * HEAD_DIM
    qb = math.gcd(length, 512)
    kb = math.gcd(length, 512)
    return pl.pallas_call(
        functools.partial(attend_back_kernel, hh, length, qb, kb, len(sources)),
        out_shape=jax.ShapeDtypeStruct((problems, length, lanes_of(w3)), BF),
        grid_spec=pltpu.PrefetchScalarGridSpec(
            num_scalar_prefetch=3,
            grid=(problems, length // qb),
            in_specs=source_specs(sources, problems)
            + [
                pl.BlockSpec((1, length, w3), lambda p, q, *_: (p, 0, 0)),
                pl.BlockSpec((1, qb, lanes_of(w)), lambda p, q, *_: (p, q, 0)),
                pl.BlockSpec((1, hh, qb), lambda p, q, *_: (p, 0, q)),
            ],
            out_specs=pl.BlockSpec((1, length, lanes_of(w3)), lambda p, q, *_: (p, 0, 0)),
            scratch_shapes=[
                pltpu.VMEM((1, length, w), BF),
                pltpu.VMEM((hh, length, HEAD_DIM), BF),
                pltpu.VMEM((hh, length, HEAD_DIM), BF),
                pltpu.VMEM((w, length), BF),
                pltpu.VMEM((hh, length, HEAD_DIM), F32),
                pltpu.VMEM((hh, length, HEAD_DIM), F32),
                pltpu.VMEM((hh, HEAD_DIM, qb), F32),
            ],
        ),
        compiler_params=params(2),
        cost_estimate=cost(
            problems * hh * 10 * length * length * 256, x.size * 6, problems * hh * length * length
        ),
        name="attend_back",
    )(lens, plan, index, *sources, x, o, lse)


def project_kernel(
    tm, width, group, per, sets, scales, order, x_ref, gain, shift, w_ref, bias, down, up, *outs
):
    normed_ref, ranks_ref, away_ref, mine_ref, n_scr, r_scr = outs
    c = pl.program_id(0)
    m = pl.program_id(1)
    rows = pl.ds(pl.multiple_of(m * tm, tm), tm)
    wide = group * w_ref.shape[0]

    @pl.when(c == 0)
    def _():
        unit, _ = norm_parts(x_ref[...].astype(F32))
        normed = (unit * gain[...] + shift[...]).astype(BF)
        n_scr[rows, :] = normed
        normed_ref[...] = normed
        rank = dot(normed, down[...]) * scales[m]
        keep = set_mask(rank.shape, sets[m], group, per)
        rank = jnp.where(keep, rank, 0.0).astype(BF)
        r_scr[rows, :] = rank
        ranks_ref[...] = rank

    y = dot(n_scr[rows, :], w_ref[:, 0].reshape(D, 3 * width)) + bias[0]
    table = up[:, 0].reshape(wide, 3 * width)
    rank = r_scr[rows, :]
    extra = [
        dot(rank[:, j * wide : (j + 1) * wide], table[:, j * width : (j + 1) * width]) for j in range(3)
    ]
    y = (y + jnp.concatenate(extra, axis=1)).astype(BF)
    half = pl.num_programs(0) // 2

    @pl.when(c < half)
    def _():
        away_ref[0, :, 0 : 3 * width] = y

    @pl.when(c >= half)
    def _():
        mine_ref[0, :, 0 : 3 * width] = y


def project(tokens, gain, shift, gathered, bias, tables, sets, scales, order, tm, per):
    own = tokens.shape[0]
    rr, nc, _, w3 = gathered.shape
    width = w3 // 3
    group = SETS * per
    wide = group * rr
    nm = own // tm
    half = nc // 2
    first = lambda c, m, *_: (jnp.where(c == 0, m, nm - 1), 0)
    flat = lambda c, m, *_: (0, 0)
    return pl.pallas_call(
        functools.partial(project_kernel, tm, width, group, per),
        out_shape=(
            jax.ShapeDtypeStruct((own, D), BF),
            jax.ShapeDtypeStruct((own, 3 * wide), BF),
            jax.ShapeDtypeStruct((half, own, lanes_of(w3)), BF),
            jax.ShapeDtypeStruct((half, own, lanes_of(w3)), BF),
        ),
        grid_spec=pltpu.PrefetchScalarGridSpec(
            num_scalar_prefetch=3,
            grid=(nc, nm),
            in_specs=[
                pl.BlockSpec((tm, D), first),
                pl.BlockSpec((1, D), flat),
                pl.BlockSpec((1, D), flat),
                pl.BlockSpec((rr, 1, D // rr, w3), lambda c, m, s, a, o: (0, o[c], 0, 0)),
                pl.BlockSpec((1, 1, w3), lambda c, m, s, a, o: (o[c], 0, 0)),
                pl.BlockSpec((D, 3 * wide), flat),
                pl.BlockSpec(
                    (rr, 1, group, w3), lambda c, m, s, a, o: (0, o[c], D // rr // group, 0)
                ),
            ],
            out_specs=[
                pl.BlockSpec((tm, D), first),
                pl.BlockSpec((tm, 3 * wide), first),
                pl.BlockSpec(
                    (1, tm, lanes_of(w3)),
                    lambda c, m, *_: (jnp.minimum(c, half - 1), jnp.where(c < half, m, nm - 1), 0),
                ),
                pl.BlockSpec(
                    (1, tm, lanes_of(w3)),
                    lambda c, m, *_: (jnp.maximum(c - half, 0), jnp.where(c < half, 0, m), 0),
                ),
            ],
            scratch_shapes=[pltpu.VMEM((own, D), BF), pltpu.VMEM((own, 3 * wide), BF)],
        ),
        compiler_params=params(2),
        cost_estimate=cost(2 * own * D * nc * w3 * 1.3, D * nc * w3 * 2 + own * (2 * D + nc * w3) * 2),
        name="project",
    )(sets, scales, order, tokens, gain, shift, gathered, bias, tables, gathered)


def piece_specs(sources, tm, at):
    def spec(j, v):
        def where_from(*ids):
            code = ids[-1]
            i = at(*ids[:-1])
            hit = code[3 * i] == j
            return (jnp.where(hit, code[3 * i + 1], 0), jnp.where(hit, code[3 * i + 2], 0), 0)

        return pl.BlockSpec((1, tm, v.shape[-1]), where_from)

    return [spec(j, v) for j, v in enumerate(sources)]


def lane_tiles(v, group):
    n = v.shape[1]
    pad = -n % 128
    if pad:
        v = jnp.concatenate([v, jnp.zeros((v.shape[0], pad), v.dtype)], axis=1)
    return [
        v[:, t * 128 : (t + 1) * 128].reshape(-1, group, 128) for t in range((n + pad) // 128)
    ]


def put_tiles(ref, first, v, group):
    for t, tile in enumerate(lane_tiles(v, group)):
        at = (first + t) * group
        ref[:, 0, at : at + group, :] = tile.astype(BF)


def fold_sets(turned, group, per):
    wide = turned.shape[0]
    row = lax.broadcasted_iota(jnp.int32, (RANK, wide), 0)
    column = lax.broadcasted_iota(jnp.int32, (RANK, wide), 1)
    match = (column // group == row // per) & (column % per == row % per)
    return dot(jnp.where(match, 1.0, 0.0).astype(BF), turned).astype(BF)


def adapt_back_kernel(tm, width, group, per, ns, nm, sets, scales, slots, code, *refs):
    sources = refs[:ns]
    up, normed_ref, ranks_ref, dy_ref, grank_ref, gup_ref, gdown_ref, racc, gup, gdown = refs[ns:]
    slot = slots[pl.program_id(1)]
    c = pl.program_id(0)
    m = pl.program_id(1)
    last = c == pl.num_programs(0) - 1
    rows = pl.ds(pl.multiple_of(m * tm, tm), tm)
    wide = group * up.shape[0]
    choose(code[3 * (c * nm + m)], sources, dy_ref, 0)
    dy = dy_ref[0]
    table = up[:, 0].reshape(wide, 3 * width)
    pieces = [dy[:, j * width : (j + 1) * width] for j in range(3)]
    rpart = jnp.concatenate(
        [dot_t(pieces[j], table[:, j * width : (j + 1) * width]) for j in range(3)], axis=1
    )

    @pl.when(c == 0)
    def _():
        racc[rows, :] = rpart

    @pl.when(c > 0)
    def _():
        racc[rows, :] += rpart

    turned = ranks_ref[...].T

    @pl.when(m == 0)
    def _():
        gup[...] = jnp.zeros_like(gup)

    for j in range(3):
        gup[slot, j] += dot(fold_sets(turned[j * wide : (j + 1) * wide], group, per), pieces[j])

    @pl.when(m == nm - 1)
    def _():
        tiles = -(-width // 128)
        clips = gup.shape[0]
        for i in range(clips):
            for j in range(3):
                for t, tile in enumerate(lane_tiles(gup[i, j], RANK)):
                    gup_ref[0, (i * 3 + j) * tiles + t] = tile[0].astype(BF)

    @pl.when(last)
    def _():
        grank = racc[rows, :] * scales[m]
        grank = jnp.where(set_mask(grank.shape, sets[m], group, per), grank, 0.0)
        grank_ref[...] = grank.astype(BF)
        turned = grank.T.astype(BF)

        @pl.when(m == 0)
        def _():
            gdown[...] = jnp.zeros_like(gdown)

        for j in range(3):
            part = dot(fold_sets(turned[j * wide : (j + 1) * wide], group, per), normed_ref[...])
            gdown[slot, j * RANK : (j + 1) * RANK] += part

        @pl.when(m == nm - 1)
        def _():
            whole = gdown[...].reshape(-1, D)
            pad = gdown_ref.shape[0] * 128 - whole.shape[0]
            whole = jnp.concatenate([whole, jnp.zeros((pad, D), F32)], axis=0)
            for i in range(gdown_ref.shape[0]):
                gdown_ref[i] = whole[i * 128 : (i + 1) * 128].T.astype(BF)


def adapt_back(sources, code, gathered, normed, ranks, sets, scales, slots, clips, tm, per):
    own = normed.shape[0]
    rr, nc, _, w3 = gathered.shape
    width = w3 // 3
    group = SETS * per
    wide = group * rr
    nm = own // tm
    tiles = 3 * -(-width // 128)
    folded = -(-clips * 3 * RANK // 128)
    final = lambda c, m, *_: (jnp.where(c == nc - 1, m, 0), 0)
    return pl.pallas_call(
        functools.partial(adapt_back_kernel, tm, width, group, per, len(sources), nm),
        out_shape=(
            jax.ShapeDtypeStruct((nc, own, w3), BF),
            jax.ShapeDtypeStruct((own, 3 * wide), BF),
            jax.ShapeDtypeStruct((nc, clips * tiles, RANK, 128), BF),
            jax.ShapeDtypeStruct((folded, D, 128), BF),
        ),
        grid_spec=pltpu.PrefetchScalarGridSpec(
            num_scalar_prefetch=4,
            grid=(nc, nm),
            in_specs=piece_specs(sources, tm, lambda c, m, s, a, i: c * nm + m)
            + [
                pl.BlockSpec((rr, 1, group, w3), lambda c, m, *_: (0, c, D // rr // group, 0)),
                pl.BlockSpec((tm, D), final),
                pl.BlockSpec((tm, 3 * wide), lambda c, m, *_: (m, 0)),
            ],
            out_specs=[
                pl.BlockSpec((1, tm, w3), lambda c, m, *_: (c, m, 0)),
                pl.BlockSpec((tm, 3 * wide), final),
                pl.BlockSpec((1, clips * tiles, RANK, 128), lambda c, m, *_: (c, 0, 0, 0)),
                pl.BlockSpec((folded, D, 128), lambda c, m, *_: (0, 0, 0)),
            ],
            scratch_shapes=[
                pltpu.VMEM((own, 3 * wide), F32),
                pltpu.VMEM((clips, 3, RANK, width), F32),
                pltpu.VMEM((clips, 3 * RANK, D), F32),
            ],
        ),
        compiler_params=params(2),
        cost_estimate=cost(own * D * nc * w3 * 0.6, own * nc * w3 * 4),
        name="adapt_back",
    )(sets, scales, slots, code, *sources, gathered, normed, ranks)


def project_back_kernel(tm, width, dy_ref, w_ref, grank_ref, down, x_ref, gm_ref, gain, gt_ref, acc):
    c = pl.program_id(0)
    m = pl.program_id(1)
    rows = pl.ds(pl.multiple_of(m * tm, tm), tm)
    part = dot_t(dy_ref[0], w_ref[:, 0].reshape(D, 3 * width))

    @pl.when(c == 0)
    def _():
        acc[rows, :] = part + dot_t(grank_ref[...], down[...])

    @pl.when(c > 0)
    def _():
        acc[rows, :] += part

    @pl.when(c == pl.num_programs(0) - 1)
    def _():
        unit, inverse = norm_parts(x_ref[...].astype(F32))
        e = acc[rows, :] * gain[...]
        mean = jnp.mean(e, axis=-1, keepdims=True)
        second = jnp.mean(e * unit, axis=-1, keepdims=True)
        gt_ref[...] = (gm_ref[...] + (e - mean - unit * second) * inverse).astype(BF)


def project_back(dy, gathered, grank, tables, tokens, grad_middle, gain, tm):
    own = tokens.shape[0]
    rr, nc, _, w3 = gathered.shape
    width = w3 // 3
    wide3 = grank.shape[1]
    nm = own // tm
    final = lambda c, m: (jnp.where(c == nc - 1, m, 0), 0)
    return pl.pallas_call(
        functools.partial(project_back_kernel, tm, width),
        out_shape=jax.ShapeDtypeStruct((own, D), BF),
        grid=(nc, nm),
        in_specs=[
            pl.BlockSpec((1, tm, w3), lambda c, m: (c, m, 0)),
            pl.BlockSpec((rr, 1, D // rr, w3), lambda c, m: (0, c, 0, 0)),
            pl.BlockSpec((tm, wide3), lambda c, m: (jnp.where(c == 0, m, nm - 1), 0)),
            pl.BlockSpec((D, wide3), lambda c, m: (0, 0)),
            pl.BlockSpec((tm, D), final),
            pl.BlockSpec((tm, D), final),
            pl.BlockSpec((1, D), lambda c, m: (0, 0)),
        ],
        out_specs=pl.BlockSpec((tm, D), final),
        scratch_shapes=[pltpu.VMEM((own, D), F32)],
        compiler_params=params(2),
        cost_estimate=cost(2 * own * D * nc * w3 * 1.1, D * nc * w3 * 2 + own * (4 * D + nc * w3) * 2),
        name="project_back",
    )(dy, gathered, grank, tables, tokens, grad_middle, gain)


def collect_kernel(nc, nm, ns, code, *refs):
    sources = refs[:ns]
    att_ref, a_scr = refs[ns:]
    m = pl.program_id(0)
    c = pl.program_id(1)
    choose(code[3 * (c * nm + m)], sources, a_scr, c)

    @pl.when(c == nc - 1)
    def _():
        att_ref[...] = jnp.concatenate([a_scr[i] for i in range(nc)], axis=1)


def collect(sources, code, own, tm, nc):
    nm = own // tm
    return pl.pallas_call(
        functools.partial(collect_kernel, nc, nm, len(sources)),
        out_shape=jax.ShapeDtypeStruct((own, D), BF),
        grid_spec=pltpu.PrefetchScalarGridSpec(
            num_scalar_prefetch=1,
            grid=(nm, nc),
            in_specs=piece_specs(sources, tm, lambda m, c: c * nm + m),
            out_specs=pl.BlockSpec((tm, D), lambda m, c, *_: (m, 0)),
            scratch_shapes=[pltpu.VMEM((nc, tm, D // nc), BF)],
        ),
        compiler_params=params(2),
        cost_estimate=cost(own * D, own * D * 10),
        name="collect",
    )(code, *sources)


def out_kernel(group, per, sets, scales, *refs):
    att_ref, x_ref, w_ref, bias, odown, oup, gain, shift, fdown = refs[:9]
    middle_ref, normed_ref, ro_ref, r1_ref = refs[9:]
    m = pl.program_id(0)
    att = att_ref[...]
    ro = dot_t(att, odown[...]) * scales[m]
    keep = set_mask(ro.shape, sets[m], group, per)
    ro = jnp.where(keep, ro, 0.0).astype(BF)
    ro_ref[...] = ro
    middle = x_ref[...].astype(F32) + dot_t(att, w_ref[...]) + dot_t(ro, oup[...]) + bias[...]
    middle_ref[...] = middle
    unit, _ = norm_parts(middle)
    normed = (unit * gain[...] + shift[...]).astype(BF)
    normed_ref[...] = normed
    r1_ref[...] = jnp.where(keep, dot(normed, fdown[...]) * scales[m], 0.0).astype(BF)


def out_project(att, tokens, wo_t, bias, odown, tables, gain, shift, sets, scales, tm, per):
    own = tokens.shape[0]
    wide = odown.shape[0]
    row = lambda m, *_: (m, 0)
    flat = lambda m, *_: (0, 0)
    return pl.pallas_call(
        functools.partial(out_kernel, SETS * per, per),
        out_shape=(
            jax.ShapeDtypeStruct((own, D), F32),
            jax.ShapeDtypeStruct((own, D), BF),
            jax.ShapeDtypeStruct((own, wide), BF),
            jax.ShapeDtypeStruct((own, wide), BF),
        ),
        grid_spec=pltpu.PrefetchScalarGridSpec(
            num_scalar_prefetch=2,
            grid=(own // tm,),
            in_specs=[
                pl.BlockSpec((tm, D), row),
                pl.BlockSpec((tm, D), row),
                pl.BlockSpec((D, D), flat),
                pl.BlockSpec((1, D), flat),
                pl.BlockSpec((wide, D), flat),
                pl.BlockSpec((D, wide), lambda m, *_: (0, 4)),
                pl.BlockSpec((1, D), flat),
                pl.BlockSpec((1, D), flat),
                pl.BlockSpec((D, wide), lambda m, *_: (0, 3)),
            ],
            out_specs=[
                pl.BlockSpec((tm, D), row),
                pl.BlockSpec((tm, D), row),
                pl.BlockSpec((tm, wide), row),
                pl.BlockSpec((tm, wide), row),
            ],
        ),
        compiler_params=params(1),
        cost_estimate=cost(2 * own * D * D * 1.5, D * D * 2 + own * D * 12),
        name="out_project",
    )(sets, scales, att, tokens, wo_t, bias, odown, tables, gain, shift, tables)


def out_back_kernel(nc, width, group, per, sets, scales, side, gb_ref, w_ref, oup, odown, att_ref, ro_ref, *outs):
    away_ref, mine_ref, gup_ref, gdown_ref, gup, gdown = outs
    m = pl.program_id(0)

    @pl.when(m == 0)
    def _():
        gup[...] = jnp.zeros_like(gup)
        gdown[...] = jnp.zeros_like(gdown)

    gb = gb_ref[...]
    gro = dot(gb, oup[...]) * scales[m]
    gro = jnp.where(set_mask(gro.shape, sets[m], group, per), gro, 0.0)
    ga = (dot(gb, w_ref[...]) + dot(gro.astype(BF), odown[...])).astype(BF)
    half = nc // 2
    for i in range(nc):
        piece = ga[:, i * width : (i + 1) * width]

        @pl.when(side[0] == i // half)
        def _(i=i, piece=piece):
            mine_ref[i % half, :, 0:width] = piece

        @pl.when(side[0] != i // half)
        def _(i=i, piece=piece):
            away_ref[i % half, :, 0:width] = piece

    gup[...] += dot(ro_ref[...].T, gb)
    gdown[...] += token_sum(gro, att_ref[...])

    @pl.when(m == pl.num_programs(0) - 1)
    def _():
        gup_ref[...] = gup[...].T.astype(BF)
        whole = gdown[...]
        for i in range(nc):
            for t, tile in enumerate(lane_tiles(whole[:, i * width : (i + 1) * width], group)):
                gdown_ref[:, i, t * group : (t + 1) * group, :] = tile.astype(BF)


def out_back(gb, wo_t, tables, odown, att, ro, sets, scales, side, tm, nc, per, rr):
    own = gb.shape[0]
    width = D // nc
    group = SETS * per
    wide = group * rr
    half = nc // 2
    tiles = -(-width // 128)
    row = lambda m, *_: (m, 0)
    flat = lambda m, *_: (0, 0)
    return pl.pallas_call(
        functools.partial(out_back_kernel, nc, width, group, per),
        out_shape=(
            jax.ShapeDtypeStruct((half, own, lanes_of(width)), BF),
            jax.ShapeDtypeStruct((half, own, lanes_of(width)), BF),
            jax.ShapeDtypeStruct((D, wide), BF),
            jax.ShapeDtypeStruct((rr, nc, tiles * group, 128), BF),
        ),
        grid_spec=pltpu.PrefetchScalarGridSpec(
            num_scalar_prefetch=3,
            grid=(own // tm,),
            in_specs=[
                pl.BlockSpec((tm, D), row),
                pl.BlockSpec((D, D), flat),
                pl.BlockSpec((D, wide), lambda m, *_: (0, 4)),
                pl.BlockSpec((wide, D), flat),
                pl.BlockSpec((tm, D), row),
                pl.BlockSpec((tm, wide), row),
            ],
            out_specs=[
                pl.BlockSpec((half, tm, lanes_of(width)), lambda m, *_: (0, m, 0)),
                pl.BlockSpec((half, tm, lanes_of(width)), lambda m, *_: (0, m, 0)),
                pl.BlockSpec((D, wide), flat),
                pl.BlockSpec((rr, nc, tiles * group, 128), lambda m, *_: (0, 0, 0, 0)),
            ],
            scratch_shapes=[pltpu.VMEM((wide, D), F32), pltpu.VMEM((wide, D), F32)],
        ),
        compiler_params=params(1),
        cost_estimate=cost(2 * own * D * D * 1.5, D * D * 2 + own * D * 6),
        name="out_back",
    )(sets, scales, side, gb, wo_t, tables, odown, att, ro)


def mlp_kernel(tm, nm, group, per, sets, scales, *refs):
    n_ref, g_ref, mid_ref, w1_ref, w2_ref, b1, up1_ref, down2_ref, up2, down1, r1_ref, bias2, gain = refs[:13]
    out_ref, gm_ref, gb_ref, gup1_ref, gdown2_ref, gup2_ref, gdown1_ref = refs[13:20]
    acc, gacc, r2acc, gr1acc, gr2, gup1, gdown2, gup2, gdown1 = refs[20:]
    c = pl.program_id(0)
    m = pl.program_id(1)
    rows = pl.ds(pl.multiple_of(m * tm, tm), tm)
    a = scales[m]
    g = g_ref[...]
    normed = n_ref[...]
    hidden = w1_ref.shape[-1]
    wide = r1_ref.shape[1]
    keep = set_mask((tm, wide), sets[m], group, per)

    @pl.when(c == 0)
    def _():
        gr2[rows, :] = jnp.where(keep, dot(g, up2[...]) * a, 0.0).astype(BF)
        acc[rows, :] = jnp.zeros((tm, D), F32)
        gacc[rows, :] = jnp.zeros((tm, D), F32)
        r2acc[rows, :] = jnp.zeros((tm, wide), F32)
        gr1acc[rows, :] = jnp.zeros((tm, wide), F32)

    @pl.when(m == 0)
    def _():
        gup1[...] = jnp.zeros_like(gup1)
        gdown2[...] = jnp.zeros_like(gdown2)

    @pl.when((m == 0) & (c == 0))
    def _():
        gup2[...] = jnp.zeros_like(gup2)
        gdown1[...] = jnp.zeros_like(gdown1)

    w1 = w1_ref[:, 0].reshape(D, hidden)
    w2 = w2_ref[:, 0].reshape(D, hidden)
    up1 = up1_ref[:, 0].reshape(wide, hidden)
    down2 = down2_ref[:, 0].reshape(wide, hidden)
    r1 = r1_ref[...]
    grank2 = gr2[rows, :]
    pre = dot(normed, w1) + dot(r1, up1) + b1[0]
    upper = 0.5 + 0.5 * lax.erf(pre * (0.5**0.5))
    density = jnp.exp(pre * pre * -0.5) * ((2.0 * math.pi) ** -0.5)
    act = (pre * upper).astype(BF)
    slope = upper + pre * density
    gact = dot(g, w2) + dot(grank2, down2)
    gpre = (gact * slope).astype(BF)
    acc[rows, :] += dot_t(act, w2)
    r2acc[rows, :] += dot_t(act, down2)
    gacc[rows, :] += dot_t(gpre, w1)
    gr1acc[rows, :] += dot_t(gpre, up1)
    gdown2[...] += dot(grank2.T, act)
    gup1[...] += dot(r1.T, gpre)

    @pl.when(m == nm - 1)
    def _():
        put_tiles(gup1_ref, 0, gup1[...], group)
        put_tiles(gdown2_ref, 0, gdown2[...], group)

    @pl.when(c == pl.num_programs(0) - 1)
    def _():
        r2 = jnp.where(keep, r2acc[rows, :] * a, 0.0).astype(BF)
        middle = mid_ref[...]
        out_ref[...] = (middle + acc[rows, :] + dot_t(r2, up2[...]) + bias2[...]).astype(BF)
        gup2[...] += dot(r2.T, g)
        gr1 = jnp.where(keep, gr1acc[rows, :] * a, 0.0).astype(BF)
        e = (gacc[rows, :] + dot_t(gr1, down1[...])) * gain[...]
        gdown1[...] += dot(gr1.T, normed)
        unit, inverse = norm_parts(middle)
        mean = jnp.mean(e, axis=-1, keepdims=True)
        second = jnp.mean(e * unit, axis=-1, keepdims=True)
        gm = g.astype(F32) + (e - mean - unit * second) * inverse
        gm_ref[...] = gm
        gb_ref[...] = gm.astype(BF)

        @pl.when(m == nm - 1)
        def _():
            gup2_ref[...] = gup2[...].T.astype(BF)
            gdown1_ref[...] = gdown1[...].T.astype(BF)


def mlp(normed, g, middle, gathered, b1, tables, r1, bias2, gain, sets, scales, tm, per, at):
    own = g.shape[0]
    rr, nc, _, hidden = gathered.shape
    group = SETS * per
    wide = group * rr
    nm = own // tm
    tiles = -(-hidden // 128)
    row = lambda c, m, *_: (m, 0)
    final = lambda c, m, *_: (jnp.where(c == nc - 1, m, 0), 0)
    flat = lambda c, m, *_: (0, 0)
    wblock = (rr, 1, D // rr, hidden)
    return pl.pallas_call(
        functools.partial(mlp_kernel, tm, nm, group, per),
        out_shape=(
            jax.ShapeDtypeStruct((own, D), BF),
            jax.ShapeDtypeStruct((own, D), F32),
            jax.ShapeDtypeStruct((own, D), BF),
            jax.ShapeDtypeStruct((rr, nc, tiles * group, 128), BF),
            jax.ShapeDtypeStruct((rr, nc, tiles * group, 128), BF),
            jax.ShapeDtypeStruct((D, wide), BF),
            jax.ShapeDtypeStruct((D, wide), BF),
        ),
        grid_spec=pltpu.PrefetchScalarGridSpec(
            num_scalar_prefetch=2,
            grid=(nc, nm),
            in_specs=[
                pl.BlockSpec((tm, D), row),
                pl.BlockSpec((tm, D), row),
                pl.BlockSpec((tm, D), final, pipeline_mode=pl.Buffered(1)),
                pl.BlockSpec(wblock, lambda c, m, *_: (0, c, 0, 0)),
                pl.BlockSpec(wblock, lambda c, m, *_: (0, c, 1, 0)),
                pl.BlockSpec((1, 1, hidden), lambda c, m, *_: (c, 0, 0)),
                pl.BlockSpec((rr, 1, group, hidden), lambda c, m, *_: (0, c, at // group, 0)),
                pl.BlockSpec((rr, 1, group, hidden), lambda c, m, *_: (0, c, at // group + 1, 0)),
                pl.BlockSpec((D, wide), lambda c, m, *_: (0, 5), pipeline_mode=pl.Buffered(1)),
                pl.BlockSpec((D, wide), lambda c, m, *_: (0, 3), pipeline_mode=pl.Buffered(1)),
                pl.BlockSpec((tm, wide), row),
                pl.BlockSpec((1, D), flat),
                pl.BlockSpec((1, D), flat),
            ],
            out_specs=[
                pl.BlockSpec((tm, D), final),
                pl.BlockSpec((tm, D), final),
                pl.BlockSpec((tm, D), final),
                pl.BlockSpec((rr, 1, tiles * group, 128), lambda c, m, *_: (0, c, 0, 0)),
                pl.BlockSpec((rr, 1, tiles * group, 128), lambda c, m, *_: (0, c, 0, 0)),
                pl.BlockSpec((D, wide), flat),
                pl.BlockSpec((D, wide), flat),
            ],
            scratch_shapes=[
                pltpu.VMEM((own, D), F32),
                pltpu.VMEM((own, D), F32),
                pltpu.VMEM((own, wide), F32),
                pltpu.VMEM((own, wide), F32),
                pltpu.VMEM((own, wide), BF),
                pltpu.VMEM((wide, hidden), F32),
                pltpu.VMEM((wide, hidden), F32),
                pltpu.VMEM((wide, D), F32),
                pltpu.VMEM((wide, D), F32),
            ],
        ),
        compiler_params=params(2, 67043328),
        cost_estimate=cost(8 * own * D * nc * hidden * 1.2, D * nc * hidden * 4 + own * D * 30, own * nc * hidden * 2),
        name="mlp",
    )(
        sets, scales, normed, g, middle, gathered, gathered, b1, gathered, gathered, tables, tables, r1, bias2, gain
    )


def assemble_kernel(width, parts, w_ref, o_ref, w_out, o_out):
    _, nc = w_ref.shape[:2]
    columns, downs = [], []
    for c in range(nc):
        block = w_ref[:, c]
        rows = [block[:, :, j * width : (j + 1) * width] for j in range(parts)]
        columns.append(jnp.concatenate(rows, axis=1).reshape(D, width))
        downs.append(o_ref[:, c, :, 0:width].reshape(-1, width))
    w_out[...] = jnp.concatenate(columns, axis=1)
    o_out[...] = jnp.concatenate(downs, axis=1)


def assemble(gathered, at_w, rows_w, at_o, group, width):
    nr, nc, _, hidden = gathered.shape
    parts = hidden // width
    if rows_w % 8 == 0 and at_w % rows_w == 0:
        return pl.pallas_call(
            functools.partial(assemble_kernel, width, parts),
            out_shape=(
                jax.ShapeDtypeStruct((D, D), BF),
                jax.ShapeDtypeStruct((nr * group, D), BF),
            ),
            grid=(1,),
            in_specs=[
                pl.BlockSpec((nr, nc, rows_w, hidden), lambda i: (0, 0, at_w // rows_w, 0)),
                pl.BlockSpec((nr, nc, group, hidden), lambda i: (0, 0, at_o // group, 0)),
            ],
            out_specs=[
                pl.BlockSpec((D, D), lambda i: (0, 0)),
                pl.BlockSpec((nr * group, D), lambda i: (0, 0)),
            ],
            compiler_params=params(1),
            name="assemble",
        )(gathered, gathered)
    w = gathered[:, :, at_w : at_w + rows_w].reshape(nr, nc, rows_w, parts, width)
    o = gathered[:, :, at_o : at_o + group, :width]
    return (
        w.transpose(0, 3, 2, 1, 4).reshape(D, D),
        o.transpose(0, 2, 1, 3).reshape(nr * group, D),
    )


def pick(flag, first, second):
    return jnp.where(flag, first, second)


def table_of(values):
    return jnp.stack([jnp.asarray(v, jnp.int32) for v in values])


class Exchange:
    def __init__(self, nc, own, clips, clip_len, tm):
        self.nc, self.own, self.clips, self.clip_len, self.tm = nc, own, clips, clip_len, tm
        self.local = nc == 4 and clips == 3 and own == 3 * tm and clip_len == 4 * tm
        col = lax.axis_index("cols")
        self.nm = nm = own // tm
        if not self.local:
            self.order = jnp.arange(nc, dtype=jnp.int32)
            self.side = jnp.ones((1,), jnp.int32)
            self.plans = [jnp.zeros((2,), jnp.int32)]
            self.indices = [jnp.arange(clips, dtype=jnp.int32)]
            entry = jnp.arange(nc * nm, dtype=jnp.int32)
            self.code = jnp.stack([entry * 0, entry // nm, entry % nm], axis=1).reshape(-1)
            return
        y, k = col // 2, col % 2
        self.y, self.k = y, k
        self.holder = y != k
        self.order = (jnp.arange(4, dtype=jnp.int32) + 2 * (1 - k)) % 4
        self.side = k[None]
        b = jnp.arange(4, dtype=jnp.int32)
        g = b + 2 * y
        clip_plan = jnp.concatenate([pick(g // 3 == k, 0, 1), g % 3])
        g = pick(y == 0, 4 + b, b - 2)
        near = b // 2 == y
        source = pick(near, pick(g // 3 == k, 0, 1), pick(self.holder, 3, 2))
        shared_plan = jnp.concatenate([source, pick(near, g % 3, b % 2)])
        self.plans = [clip_plan.astype(jnp.int32), shared_plan.astype(jnp.int32)]
        self.indices = [jnp.array([0, 1, 0, 1], jnp.int32), table_of([y, y, 0, 0])]
        entry = jnp.arange(12, dtype=jnp.int32)
        c, m = entry // 3, entry % 3
        g = 3 * k + m
        inside = (g >= 2 * y) & (g < 2 * y + 4)
        same, idx = c // 2 == k, c % 2
        source = pick(
            inside,
            pick(same, 0, 2),
            pick(idx == y, pick(same, 1, 3), pick(same, 4, 5)),
        )
        block = pick(
            inside,
            g - 2 * y,
            pick(y == 0, g - 4, pick(idx == y, g + 2, g)),
        )
        self.code = (
            jnp.stack([source, pick(inside, idx, 0), block], axis=1).astype(jnp.int32).reshape(-1)
        )

    def lens(self, lengths):
        if not self.local:
            return (lengths,)
        mine = pick(self.y == 0, lengths[0], lengths[2])
        return (jnp.stack([mine, mine]), lengths[1:2])

    def to_heads(self, away, mine):
        f = mine.shape[-1]
        if not self.local:
            moved = lax.all_to_all(jnp.concatenate([away, mine]), "cols", 0, 0, tiled=True)
            return [[moved.reshape(self.clips, self.clip_len, f)]]
        y, k, half = self.y, self.k, self.clip_len // 2
        start = pick(k == 1, self.own - half, 0)
        got = lax.ppermute(away, "cols", [(i, i ^ 1) for i in range(4)])
        one = lax.dynamic_slice(mine, (1 - y, start, 0), (1, half, f))
        two = lax.dynamic_slice(away, (1 - y, start, 0), (1, half, f))
        got_one = lax.ppermute(one, "cols", [(1, 3), (2, 0)])
        got_two = lax.ppermute(two, "cols", [(1, 2), (2, 1)])
        return [[mine, got], [mine, got, got_one, got_two]]

    def from_heads(self, parts):
        if not self.local:
            (v,) = parts
            v = v.reshape(self.nc, self.own, v.shape[-1])
            return [lax.all_to_all(v, "cols", 0, 0, tiled=True)]
        clip, shared = parts
        half = self.clip_len // 2
        far = lax.dynamic_slice(shared, (0, (1 - self.y) * half, 0), (1, half, clip.shape[-1]))
        swap = [(i, i ^ 1) for i in range(4)]
        got_one = lax.ppermute(far, "cols", [(3, 1), (0, 2)])
        got_two = lax.ppermute(far, "cols", [(2, 1), (1, 2)])
        got_shared = lax.ppermute(shared, "cols", swap)
        return [clip, shared, lax.ppermute(clip, "cols", swap), got_shared, got_one, got_two]


def up_to(n, k):
    return -(-n // k) * k


def rows_padded(v, rows, lanes):
    return jnp.pad(v.astype(BF), ((0, rows - v.shape[0]), (0, lanes - v.shape[1])))


def halves(v):
    high = v.astype(BF)
    return high, (v - high.astype(F32)).astype(BF)


def scatter_sum(pieces):
    whole = jnp.concatenate(pieces, axis=2)
    n = whole.shape[2]
    whole = jnp.pad(whole, ((0, 0), (0, 0), (0, up_to(n, 8) - n), (0, 0)))
    return whole.reshape(-1, 128)


def join(v, nc):
    col = lax.axis_index("cols")
    zeros = (0,) * v.ndim
    held = lax.dynamic_update_slice(jnp.zeros((nc,) + v.shape, v.dtype), v[None], (col,) + zeros)
    step = 1
    while step < nc:
        base = col // step * step
        sent = lax.dynamic_slice(held, (base,) + zeros, (step,) + v.shape)
        got = lax.ppermute(sent, "cols", [(i, i ^ step) for i in range(nc)])
        held = lax.dynamic_update_slice(held, got, (base ^ step,) + zeros)
        step *= 2
    return held


def body(
    tokens,
    cotangent,
    clip_lengths,
    clip_sets,
    clip_scales,
    norm1_gain,
    norm1_shift,
    w_query,
    query_bias,
    w_key,
    w_value,
    value_bias,
    w_out,
    out_bias,
    norm2_gain,
    norm2_shift,
    w_fc1,
    fc1_bias,
    w_fc2,
    fc2_bias,
    query_down,
    query_up,
    key_down,
    key_up,
    value_down,
    value_up,
    out_down,
    out_up,
    fc1_down,
    fc1_up,
    fc2_down,
    fc2_up,
):
    nr = lax.axis_size("rows")
    nc = lax.axis_size("cols")
    col = lax.axis_index("cols")
    clips = clip_lengths.shape[0]
    own = tokens.shape[0]
    clip_len = own * nc // clips
    tm = math.gcd(own, clip_len)
    width = query_bias.shape[0]
    hidden = fc1_bias.shape[0]
    hh = width // HEAD_DIM
    dr = w_query.shape[0]
    per = RANK // nr
    group = SETS * per
    wide = group * nr
    dc = dr // nc
    exchange = Exchange(nc, own, clips, clip_len, tm)

    block_clip = (col * own + jnp.arange(own // tm, dtype=jnp.int32) * tm) // clip_len
    sets = jnp.take(clip_sets, block_clip)
    scales = jnp.take(clip_scales, block_clip)

    downs = jnp.stack([query_down, key_down, value_down, fc1_down])
    downs = lax.dynamic_slice(downs, (0, 0, col * dc, 0), (4, SETS, dc, RANK))
    downs = downs.reshape(4, SETS, dc, nr, per).transpose(2, 0, 3, 1, 4).reshape(dc, 4 * wide)
    ups = jnp.stack([out_up, fc2_up])
    ups = lax.dynamic_slice(ups, (0, 0, 0, col * dc), (2, SETS, RANK, dc))
    ups = ups.reshape(2, SETS, nr, per, dc).transpose(4, 0, 2, 1, 3).reshape(dc, 2 * wide)
    tables = jnp.concatenate([downs, ups], axis=1)

    lanes = 3 * width
    qh, ql = halves(query_bias)
    vh, vl = halves(value_bias)
    none = jnp.zeros_like(qh)
    ids = jnp.pad(clip_sets.astype(BF), (0, lanes - clips))
    natural = lanes >= 6 * wide
    small = rows_padded(tables, dc, lanes) if natural else tables.reshape(-1, lanes)
    small_rows = small.shape[0]
    at_bias = dr + group
    at_table = up_to(at_bias + 3, 16)
    packed = jnp.concatenate(
        [
            jnp.concatenate([w_query, w_key, w_value], axis=1),
            jnp.concatenate([v.reshape(group, width) for v in (query_up, key_up, value_up)], axis=1),
            rows_padded(
                jnp.stack([jnp.concatenate([qh, none, vh]), jnp.concatenate([ql, none, vl]), ids]),
                at_table - at_bias,
                lanes,
            ),
            rows_padded(small, up_to(small_rows, 16), lanes),
        ],
        axis=0,
    )
    g1 = lax.all_gather(packed, BOTH, axis=0).reshape(nr, nc, -1, lanes)
    tables = g1[:, :, at_table : at_table + small_rows]
    if natural:
        tables = tables[..., : 6 * wide]
    tables = tables.reshape(D, 6 * wide)
    every_set = g1[:, 0, at_bias + 2, :clips].astype(jnp.int32)
    bias_qkv = jnp.sum(g1[0, :, at_bias : at_bias + 2].astype(F32), axis=1, keepdims=True)

    parts = hidden // width
    rows_w = dr // parts
    at_w = 2 * dr
    at_f = up_to(at_w + rows_w, 16)
    at_o = at_f + 2 * group
    at_b = at_o + group
    wo = w_out.T.reshape(parts, rows_w, width).transpose(1, 0, 2).reshape(rows_w, hidden)
    turn = lambda v: jnp.swapaxes(v, 1, 2).reshape(group, -1)
    packed = jnp.concatenate(
        [
            w_fc1,
            w_fc2.T,
            rows_padded(wo, at_f - at_w, hidden),
            fc1_up.reshape(group, hidden),
            turn(fc2_down),
            rows_padded(turn(out_down), group, hidden),
            rows_padded(jnp.stack(halves(fc1_bias)), 16, hidden),
        ],
        axis=0,
    )
    packed, g1 = lax.optimization_barrier((packed, g1))
    g2 = lax.all_gather(packed, BOTH, axis=0).reshape(nr, nc, -1, hidden)
    wo_t, odown = assemble(g2, at_w, rows_w, at_o, group, width)
    b1 = jnp.sum(g2[0, :, at_b : at_b + 2].astype(F32), axis=1, keepdims=True)

    gain1, shift1 = norm1_gain[None], norm1_shift[None]
    gain2, shift2 = norm2_gain[None], norm2_shift[None]

    normed, ranks, away, mine = project(
        tokens, gain1, shift1, g1, bias_qkv, tables, sets, scales, exchange.order, tm, per
    )
    lens = exchange.lens(clip_lengths)
    results = []
    for sources, plan, index, n in zip(
        exchange.to_heads(away, mine), exchange.plans, exchange.indices, lens
    ):
        if results:
            n, _ = lax.optimization_barrier((n, results[-1][1]))
        results.append(attend(sources, plan, index, n, clip_len, hh))
    pieces = exchange.from_heads([r[0] for r in results])
    att = collect(pieces, exchange.code, own, tm, nc)
    middle, normed_mlp, ro, r1 = out_project(
        att, tokens, wo_t, out_bias[None], odown, tables, gain2, shift2, sets, scales, tm, per
    )
    output, grad_middle, grad_branch, gup1, gdown2, gup2, gdown1 = mlp(
        normed_mlp, cotangent, middle, g2, b1, tables, r1, fc2_bias[None], gain2, sets, scales, tm, per, at_f
    )
    away, mine, goup, godown = out_back(
        grad_branch, wo_t, tables, odown, att, ro, sets, scales, exchange.side, tm, nc, per, nr
    )

    by_model = lambda v: v.reshape(nr, nc, dc, wide)
    late = scatter_sum([gup1, gdown2, godown, by_model(gdown1), by_model(goup), by_model(gup2)])
    late, away, mine = lax.optimization_barrier((late, away, mine))
    late = lax.psum_scatter(late, BOTH, scatter_dimension=0, tiled=True)

    def untile(v, n):
        t = v.shape[0] // group
        return v.reshape(t, group, 128).transpose(1, 0, 2).reshape(group, t * 128)[:, :n].reshape(SETS, per, n)

    def model_tables(v):
        k = v.shape[0] // dc
        every = join(v, nc).reshape(nc, k, dc, wide).swapaxes(0, 1)
        return every.reshape(k, dr, nr, SETS, per)

    as_down = lambda v: v.transpose(2, 0, 1, 3).reshape(SETS, dr, RANK)
    as_up = lambda v: v.transpose(2, 1, 3, 0).reshape(SETS, RANK, dr)
    flip = lambda v: jnp.swapaxes(v, 1, 2)
    calls = list(
        zip(exchange.to_heads(away, mine), exchange.plans, exchange.indices, results, lens)
    )
    backs = []
    for sources, plan, index, (o, lse, x), n in reversed(calls):
        if backs:
            n, _ = lax.optimization_barrier((n, backs[-1]))
        backs.append(attend_back(sources, plan, index, x, o, lse, n, hh))
    pieces = exchange.from_heads(backs[::-1])
    dy, grank, gup, gdown = adapt_back(
        pieces, exchange.code, g1, normed, ranks, sets, scales, block_clip, clips, tm, per
    )
    tiles = gup.shape[1] // (3 * clips)
    folded = gdown.shape[0]
    ups = gup.reshape(nc, clips * 3 * tiles, nr, per, 128).transpose(2, 0, 1, 3, 4)
    ups = ups.reshape(nr, nc, -1, 128)
    downs = [gdown[i].reshape(nr, nc, dc, 128) for i in range(folded)]
    last = scatter_sum([ups] + downs).reshape(nr * nc, -1, 128)
    last, dy = lax.optimization_barrier((last, dy))
    got = lax.all_to_all(last, BOTH, 0, 0, tiled=True)
    grad_tokens = project_back(dy, g1, grank, tables, tokens, grad_middle, gain1, tm)
    late, grad_tokens = lax.optimization_barrier((late, grad_tokens))
    summed = late.astype(F32)
    a = gup1.shape[2]
    b = godown.shape[2]
    grad_fc1_up = untile(summed[:a], hidden)
    grad_fc2_down = flip(untile(summed[a : 2 * a], hidden))
    grad_out_down = flip(untile(summed[2 * a : 2 * a + b], width))
    model = model_tables(summed[2 * a + b : 2 * a + b + 3 * dc])
    grad_fc1_down, grad_out_up, grad_fc2_up = as_down(model[0]), as_up(model[1]), as_up(model[2])

    got = jnp.sum(got.reshape(nr, nc, -1, 128).astype(F32), axis=1)
    onehot = (every_set[:, :, None] == jnp.arange(SETS, dtype=jnp.int32)).astype(F32)
    n = ups.shape[2]
    per_clip = got[:, :n].reshape(nr, clips, -1, 128)
    per_set = jnp.sum(onehot[:, :, :, None, None] * per_clip[:, :, None], axis=(0, 1))
    per_set = per_set.reshape(SETS, 3, tiles, per, 128).transpose(1, 0, 3, 2, 4)
    up = per_set.reshape(3, SETS, per, tiles * 128)[..., :width]
    side = got[:, n : n + folded * dc].reshape(nr, folded, dc, 128).transpose(0, 2, 1, 3)
    side = side.reshape(nr, dc, folded * 128)[..., : clips * 3 * RANK]
    side = side.reshape(nr, dc, clips, 3 * RANK).transpose(0, 2, 1, 3)
    side = jnp.sum(onehot[:, :, :, None, None] * side[:, :, None], axis=(0, 1))
    side = side.transpose(1, 0, 2).reshape(dc, SETS * 3 * RANK)
    side = lax.all_gather(side, "cols", axis=0, tiled=True).reshape(dr, SETS, 3, RANK)
    down = side.transpose(2, 1, 0, 3)
    return (
        output,
        grad_tokens,
        down[0],
        up[0],
        down[1],
        up[1],
        down[2],
        up[2],
        grad_out_down,
        grad_out_up,
        grad_fc1_down,
        grad_fc1_up,
        grad_fc2_down,
        grad_fc2_up,
    )


def solution(mesh):
    both = P(("rows", "cols"), None)
    grid = P("rows", "cols")
    turned = P("cols", "rows")
    down = P(None, "rows", None)
    up = P(None, "rows", "cols")
    far_down = P(None, "cols", "rows")
    far_up = P(None, None, "rows")
    return jax.shard_map(
        body,
        mesh=mesh,
        in_specs=(
            both,
            both,
            P("rows"),
            P("rows"),
            P("rows"),
            P(),
            P(),
            grid,
            P("cols"),
            grid,
            grid,
            P("cols"),
            turned,
            P(),
            P(),
            P(),
            grid,
            P("cols"),
            turned,
            P(),
            down,
            up,
            down,
            up,
            down,
            up,
            far_down,
            far_up,
            down,
            up,
            far_down,
            far_up,
        ),
        out_specs=(
            both,
            both,
            down,
            up,
            down,
            up,
            down,
            up,
            far_down,
            far_up,
            down,
            up,
            far_down,
            far_up,
        ),
        check_vma=False,
    )
```

```python
import functools
import math

import jax
import jax.numpy as jnp
from jax import lax
from jax.experimental import pallas as pl
from jax.experimental.pallas import tpu as pltpu
from jax.sharding import PartitionSpec as P


D = 1280
SETS = 8
RANK = 16
HEAD_DIM = 80
EPSILON = 1e-05
LOG2E = 1.4426950408889634
LOW = -1e30
F32 = jnp.float32
BF = jnp.bfloat16
BOTH = ("rows", "cols")


def dot(a, b):
    return lax.dot_general(a, b, (((1,), (0,)), ((), ())), preferred_element_type=F32)


def dot_t(a, b):
    return lax.dot_general(a, b, (((1,), (1,)), ((), ())), preferred_element_type=F32)


def token_sum(a, b):
    return dot(a.T.astype(BF), b)


def norm_parts(x):
    mean = jnp.mean(x, axis=-1, keepdims=True)
    centred = x - mean
    inverse = lax.rsqrt(jnp.mean(centred * centred, axis=-1, keepdims=True) + EPSILON)
    return centred * inverse, inverse


def params(n, limit=60 << 20):
    return pltpu.CompilerParams(
        dimension_semantics=("arbitrary",) * n, vmem_limit_bytes=limit
    )


def cost(flops, nbytes, trans=0):
    return pl.CostEstimate(flops=int(flops), bytes_accessed=int(nbytes), transcendentals=int(trans))


def set_mask(shape, which, group, per):
    column = lax.broadcasted_iota(jnp.int32, shape, len(shape) - 1)
    return (column % group) // per == which


def choose(code, refs, dst, at):
    for j, ref in enumerate(refs):

        @pl.when(code == j)
        def _(ref=ref):
            dst[at] = ref[0, :, 0 : dst.shape[-1]]


def gather_clip(refs, plan, dst, bs):
    blocks = plan.shape[0] // 2
    for b in range(blocks):
        rows = slice(b * bs, (b + 1) * bs)
        for j, ref in enumerate(refs):

            @pl.when(plan[b] == j)
            def _(ref=ref, b=b, rows=rows):
                off = pl.multiple_of(plan[blocks + b] * bs, bs)
                dst[0, rows, :] = ref[0, pl.ds(off, bs), 0 : dst.shape[2]]


def attend_kernel(hh, length, qb, kb, ns, lens, plan, index, *refs):
    sources, (o_ref, lse_ref, x_ref, k_scr, vt_scr, acc, m_scr, l_scr) = refs[:ns], refs[ns:]
    p = pl.program_id(0)
    qi = pl.program_id(1)
    w = hh * HEAD_DIM
    c = HEAD_DIM**-0.5 * LOG2E

    @pl.when(qi == 0)
    def _():
        gather_clip(sources, plan, x_ref, 2 * length // plan.shape[0])
        vt_scr[...] = x_ref[0, :, 2 * w : 3 * w].T
        for h in range(hh):
            k_scr[h] = x_ref[0, :, w + h * HEAD_DIM : w + (h + 1) * HEAD_DIM]

    size = lens[p]
    block = x_ref[0, pl.ds(pl.multiple_of(qi * qb, qb), qb), 0:w]
    qs = [block[:, h * HEAD_DIM : (h + 1) * HEAD_DIM] for h in range(hh)]
    m_scr[...] = jnp.full_like(m_scr, LOW)
    l_scr[...] = jnp.zeros_like(l_scr)
    acc[...] = jnp.zeros_like(acc)

    def chunk(i, masked):
        r0 = pl.multiple_of(i * kb, kb)
        for h in range(hh):
            s = dot_t(k_scr[h, pl.ds(r0, kb), :], qs[h])
            if masked:
                keys = lax.broadcasted_iota(jnp.int32, (kb, qb), 0) + i * kb
                s = jnp.where(keys < size, s, LOW)
            old = m_scr[h : h + 1]
            top = jnp.maximum(old, jnp.max(s, axis=0, keepdims=True))
            probs = jnp.exp2((s - top) * c)
            shrink = jnp.exp2((old - top) * c)
            l_scr[h : h + 1] = l_scr[h : h + 1] * shrink + jnp.sum(probs, axis=0, keepdims=True)
            m_scr[h : h + 1] = top
            acc[h] = acc[h] * shrink + dot(
                vt_scr[h * HEAD_DIM : (h + 1) * HEAD_DIM, pl.ds(r0, kb)], probs.astype(BF)
            )

    full = size // kb

    def step(i, carry):
        chunk(i, False)
        return carry

    lax.fori_loop(0, full, step, 0)

    @pl.when(full * kb < size)
    def _():
        chunk(full, True)

    outs = [acc[h] * (1.0 / l_scr[h : h + 1]) for h in range(hh)]
    o_ref[0, :, 0:w] = jnp.concatenate(outs, axis=0).T.astype(BF)
    lse_ref[0] = m_scr[0:hh] * c + jnp.log2(l_scr[0:hh])


def lanes_of(n):
    return -(-n // 128) * 128


def source_specs(sources, problems):
    def spec(j, v):
        return pl.BlockSpec(
            (1,) + v.shape[1:], lambda p, q, l, plan, index: (index[j * problems + p], 0, 0)
        )

    return [spec(j, v) for j, v in enumerate(sources)]


def attend(sources, plan, index, lens, length, hh):
    problems = lens.shape[0]
    w3 = 3 * hh * HEAD_DIM
    w = hh * HEAD_DIM
    qb = math.gcd(length, 512)
    kb = math.gcd(length, 768)
    return pl.pallas_call(
        functools.partial(attend_kernel, hh, length, qb, kb, len(sources)),
        out_shape=(
            jax.ShapeDtypeStruct((problems, length, lanes_of(w)), BF),
            jax.ShapeDtypeStruct((problems, hh, length), F32),
            jax.ShapeDtypeStruct((problems, length, w3), BF),
        ),
        grid_spec=pltpu.PrefetchScalarGridSpec(
            num_scalar_prefetch=3,
            grid=(problems, length // qb),
            in_specs=source_specs(sources, problems),
            out_specs=[
                pl.BlockSpec((1, qb, lanes_of(w)), lambda p, q, *_: (p, q, 0)),
                pl.BlockSpec((1, hh, qb), lambda p, q, *_: (p, 0, q)),
                pl.BlockSpec((1, length, w3), lambda p, q, *_: (p, 0, 0)),
            ],
            scratch_shapes=[
                pltpu.VMEM((hh, length, HEAD_DIM), BF),
                pltpu.VMEM((w, length), BF),
                pltpu.VMEM((hh, HEAD_DIM, qb), F32),
                pltpu.VMEM((max(8, hh), qb), F32),
                pltpu.VMEM((max(8, hh), qb), F32),
            ],
        ),
        compiler_params=params(2),
        cost_estimate=cost(
            problems * hh * 4 * length * length * 256,
            problems * length * w3 * 6,
            problems * hh * length * length,
        ),
        name="attend",
    )(lens, plan, index, *sources)


def attend_back_kernel(hh, length, qb, kb, ns, lens, plan, index, *refs):
    sources = refs[:ns]
    x_ref, o_ref, lse_ref, dx_ref, do_scr, k_scr, v_scr, kt_scr, dk, dv, dqt = refs[ns:]
    p = pl.program_id(0)
    qi = pl.program_id(1)
    w = hh * HEAD_DIM
    scale = HEAD_DIM**-0.5
    c = scale * LOG2E

    @pl.when(qi == 0)
    def _():
        gather_clip(sources, plan, do_scr, 2 * length // plan.shape[0])
        kt_scr[...] = x_ref[0, :, w : 2 * w].T
        for h in range(hh):
            k_scr[h] = x_ref[0, :, w + h * HEAD_DIM : w + (h + 1) * HEAD_DIM]
            v_scr[h] = x_ref[0, :, 2 * w + h * HEAD_DIM : 2 * w + (h + 1) * HEAD_DIM]
        dk[...] = jnp.zeros_like(dk)
        dv[...] = jnp.zeros_like(dv)

    size = lens[p]
    rows = pl.ds(pl.multiple_of(qi * qb, qb), qb)
    block = x_ref[0, rows, 0:w]
    qs = [block[:, h * HEAD_DIM : (h + 1) * HEAD_DIM] for h in range(hh)]
    do = do_scr[0, rows, :]
    dos = [do[:, h * HEAD_DIM : (h + 1) * HEAD_DIM] for h in range(hh)]
    prod = (do.astype(F32) * o_ref[0, :, 0:w].astype(F32)).T
    inner = [
        jnp.sum(prod[h * HEAD_DIM : (h + 1) * HEAD_DIM], axis=0, keepdims=True) for h in range(hh)
    ]
    dqt[...] = jnp.zeros_like(dqt)

    def chunk(i, masked):
        keys_at = pl.ds(pl.multiple_of(i * kb, kb), kb)
        for h in range(hh):
            s = dot_t(k_scr[h, keys_at, :], qs[h])
            probs = jnp.exp2(s * c - lse_ref[0, h : h + 1])
            if masked:
                keys = lax.broadcasted_iota(jnp.int32, (kb, qb), 0) + i * kb
                probs = jnp.where(keys < size, probs, 0.0)
            dp = dot_t(v_scr[h, keys_at, :], dos[h])
            ds = (probs * (dp - inner[h])).astype(BF)
            dv[h, keys_at, :] += dot(probs.astype(BF), dos[h])
            dk[h, keys_at, :] += dot(ds, qs[h])
            dqt[h] += dot(kt_scr[h * HEAD_DIM : (h + 1) * HEAD_DIM, keys_at], ds)

    full = size // kb

    def step(i, carry):
        chunk(i, False)
        return carry

    lax.fori_loop(0, full, step, 0)

    @pl.when(full * kb < size)
    def _():
        chunk(full, True)

    dq = jnp.concatenate([dqt[h] for h in range(hh)], axis=0).T * scale
    dx_ref[0, rows, 0:w] = dq.astype(BF)

    @pl.when(qi == pl.num_programs(1) - 1)
    def _():
        for h in range(hh):
            dx_ref[0, :, w + h * HEAD_DIM : w + (h + 1) * HEAD_DIM] = (dk[h] * scale).astype(BF)
            dx_ref[0, :, 2 * w + h * HEAD_DIM : 2 * w + (h + 1) * HEAD_DIM] = dv[h].astype(BF)


def attend_back(sources, plan, index, x, o, lse, lens, hh):
    problems, length, w3 = x.shape
    w = hh * HEAD_DIM
    qb = math.gcd(length, 512)
    kb = math.gcd(length, 512)
    return pl.pallas_call(
        functools.partial(attend_back_kernel, hh, length, qb, kb, len(sources)),
        out_shape=jax.ShapeDtypeStruct((problems, length, lanes_of(w3)), BF),
        grid_spec=pltpu.PrefetchScalarGridSpec(
            num_scalar_prefetch=3,
            grid=(problems, length // qb),
            in_specs=source_specs(sources, problems)
            + [
                pl.BlockSpec((1, length, w3), lambda p, q, *_: (p, 0, 0)),
                pl.BlockSpec((1, qb, lanes_of(w)), lambda p, q, *_: (p, q, 0)),
                pl.BlockSpec((1, hh, qb), lambda p, q, *_: (p, 0, q)),
            ],
            out_specs=pl.BlockSpec((1, length, lanes_of(w3)), lambda p, q, *_: (p, 0, 0)),
            scratch_shapes=[
                pltpu.VMEM((1, length, w), BF),
                pltpu.VMEM((hh, length, HEAD_DIM), BF),
                pltpu.VMEM((hh, length, HEAD_DIM), BF),
                pltpu.VMEM((w, length), BF),
                pltpu.VMEM((hh, length, HEAD_DIM), F32),
                pltpu.VMEM((hh, length, HEAD_DIM), F32),
                pltpu.VMEM((hh, HEAD_DIM, qb), F32),
            ],
        ),
        compiler_params=params(2),
        cost_estimate=cost(
            problems * hh * 10 * length * length * 256, x.size * 6, problems * hh * length * length
        ),
        name="attend_back",
    )(lens, plan, index, *sources, x, o, lse)


def project_kernel(
    tm, width, group, per, sets, scales, order, x_ref, gain, shift, w_ref, bias, down, up, *outs
):
    normed_ref, ranks_ref, away_ref, mine_ref, n_scr, r_scr = outs
    c = pl.program_id(0)
    m = pl.program_id(1)
    rows = pl.ds(pl.multiple_of(m * tm, tm), tm)
    wide = group * w_ref.shape[0]

    @pl.when(c == 0)
    def _():
        unit, _ = norm_parts(x_ref[...].astype(F32))
        normed = (unit * gain[...] + shift[...]).astype(BF)
        n_scr[rows, :] = normed
        normed_ref[...] = normed
        rank = dot(normed, down[...]) * scales[m]
        keep = set_mask(rank.shape, sets[m], group, per)
        rank = jnp.where(keep, rank, 0.0).astype(BF)
        r_scr[rows, :] = rank
        ranks_ref[...] = rank

    y = dot(n_scr[rows, :], w_ref[:, 0].reshape(D, 4 * width)[:, 0 : 3 * width]) + bias[0]
    table = up[:, 0].reshape(wide, 4 * width)
    rank = r_scr[rows, :]
    extra = [
        dot(rank[:, j * wide : (j + 1) * wide], table[:, j * width : (j + 1) * width]) for j in range(3)
    ]
    y = (y + jnp.concatenate(extra, axis=1)).astype(BF)
    half = pl.num_programs(0) // 2

    @pl.when(c < half)
    def _():
        away_ref[0, :, 0 : 3 * width] = y

    @pl.when(c >= half)
    def _():
        mine_ref[0, :, 0 : 3 * width] = y


def project(tokens, gain, shift, gathered, bias, tables, sets, scales, order, tm, per):
    own = tokens.shape[0]
    rr, nc, _, w4 = gathered.shape
    width = w4 // 4
    w3 = 3 * width
    group = SETS * per
    wide = group * rr
    nm = own // tm
    half = nc // 2
    first = lambda c, m, *_: (jnp.where(c == 0, m, nm - 1), 0)
    flat = lambda c, m, *_: (0, 0)
    return pl.pallas_call(
        functools.partial(project_kernel, tm, width, group, per),
        out_shape=(
            jax.ShapeDtypeStruct((own, D), BF),
            jax.ShapeDtypeStruct((own, 3 * wide), BF),
            jax.ShapeDtypeStruct((half, own, lanes_of(w3)), BF),
            jax.ShapeDtypeStruct((half, own, lanes_of(w3)), BF),
        ),
        grid_spec=pltpu.PrefetchScalarGridSpec(
            num_scalar_prefetch=3,
            grid=(nc, nm),
            in_specs=[
                pl.BlockSpec((tm, D), first),
                pl.BlockSpec((1, D), flat),
                pl.BlockSpec((1, D), flat),
                pl.BlockSpec((rr, 1, D // rr, w4), lambda c, m, s, a, o: (0, o[c], 0, 0)),
                pl.BlockSpec((1, 1, w3), lambda c, m, s, a, o: (o[c], 0, 0)),
                pl.BlockSpec((D, 3 * wide), flat),
                pl.BlockSpec(
                    (rr, 1, group, w4), lambda c, m, s, a, o: (0, o[c], D // rr // group, 0)
                ),
            ],
            out_specs=[
                pl.BlockSpec((tm, D), first),
                pl.BlockSpec((tm, 3 * wide), first),
                pl.BlockSpec(
                    (1, tm, lanes_of(w3)),
                    lambda c, m, *_: (jnp.minimum(c, half - 1), jnp.where(c < half, m, nm - 1), 0),
                ),
                pl.BlockSpec(
                    (1, tm, lanes_of(w3)),
                    lambda c, m, *_: (jnp.maximum(c - half, 0), jnp.where(c < half, 0, m), 0),
                ),
            ],
            scratch_shapes=[pltpu.VMEM((own, D), BF), pltpu.VMEM((own, 3 * wide), BF)],
        ),
        compiler_params=params(2),
        cost_estimate=cost(2 * own * D * nc * w3 * 1.3, D * nc * w3 * 2 + own * (2 * D + nc * w3) * 2),
        name="project",
    )(sets, scales, order, tokens, gain, shift, gathered, bias, tables, gathered)


def piece_specs(sources, tm, at):
    def spec(j, v):
        def where_from(*ids):
            code = ids[-1]
            i = at(*ids[:-1])
            hit = code[3 * i] == j
            return (jnp.where(hit, code[3 * i + 1], 0), jnp.where(hit, code[3 * i + 2], 0), 0)

        return pl.BlockSpec((1, tm, v.shape[-1]), where_from)

    return [spec(j, v) for j, v in enumerate(sources)]


def lane_tiles(v, group):
    n = v.shape[1]
    pad = -n % 128
    if pad:
        v = jnp.concatenate([v, jnp.zeros((v.shape[0], pad), v.dtype)], axis=1)
    return [
        v[:, t * 128 : (t + 1) * 128].reshape(-1, group, 128) for t in range((n + pad) // 128)
    ]


def put_tiles(ref, first, v, group):
    for t, tile in enumerate(lane_tiles(v, group)):
        at = (first + t) * group
        ref[:, 0, at : at + group, :] = tile.astype(BF)


def fold_sets(turned, group, per):
    wide = turned.shape[0]
    row = lax.broadcasted_iota(jnp.int32, (RANK, wide), 0)
    column = lax.broadcasted_iota(jnp.int32, (RANK, wide), 1)
    match = (column // group == row // per) & (column % per == row % per)
    return dot(jnp.where(match, 1.0, 0.0).astype(BF), turned).astype(BF)


def adapt_back_kernel(tm, width, group, per, ns, nm, sets, scales, slots, code, *refs):
    sources = refs[:ns]
    up, normed_ref, ranks_ref, dy_ref, grank_ref, gup_ref, gdown_ref, racc, gup, gdown = refs[ns:]
    slot = slots[pl.program_id(1)]
    c = pl.program_id(0)
    m = pl.program_id(1)
    last = c == pl.num_programs(0) - 1
    rows = pl.ds(pl.multiple_of(m * tm, tm), tm)
    wide = group * up.shape[0]
    choose(code[3 * (c * nm + m)], sources, dy_ref, 0)
    dy = dy_ref[0]
    table = up[:, 0].reshape(wide, 4 * width)
    pieces = [dy[:, j * width : (j + 1) * width] for j in range(3)]
    rpart = jnp.concatenate(
        [dot_t(pieces[j], table[:, j * width : (j + 1) * width]) for j in range(3)], axis=1
    )

    @pl.when(c == 0)
    def _():
        racc[rows, :] = rpart

    @pl.when(c > 0)
    def _():
        racc[rows, :] += rpart

    turned = ranks_ref[...].T

    @pl.when(m == 0)
    def _():
        gup[...] = jnp.zeros_like(gup)

    for j in range(3):
        gup[slot, j] += dot(fold_sets(turned[j * wide : (j + 1) * wide], group, per), pieces[j])

    @pl.when(m == nm - 1)
    def _():
        tiles = -(-width // 128)
        clips = gup.shape[0]
        for i in range(clips):
            for j in range(3):
                for t, tile in enumerate(lane_tiles(gup[i, j], RANK)):
                    gup_ref[0, (i * 3 + j) * tiles + t] = tile[0].astype(BF)

    @pl.when(last)
    def _():
        grank = racc[rows, :] * scales[m]
        grank = jnp.where(set_mask(grank.shape, sets[m], group, per), grank, 0.0)
        grank_ref[...] = grank.astype(BF)
        turned = grank.T.astype(BF)

        @pl.when(m == 0)
        def _():
            gdown[...] = jnp.zeros_like(gdown)

        for j in range(3):
            part = dot(fold_sets(turned[j * wide : (j + 1) * wide], group, per), normed_ref[...])
            gdown[slot, j * RANK : (j + 1) * RANK] += part

        @pl.when(m == nm - 1)
        def _():
            whole = gdown[...].reshape(-1, D)
            pad = gdown_ref.shape[0] * 128 - whole.shape[0]
            whole = jnp.concatenate([whole, jnp.zeros((pad, D), F32)], axis=0)
            for i in range(gdown_ref.shape[0]):
                gdown_ref[i] = whole[i * 128 : (i + 1) * 128].T.astype(BF)


def adapt_back(sources, code, gathered, normed, ranks, sets, scales, slots, clips, tm, per):
    own = normed.shape[0]
    rr, nc, _, w4 = gathered.shape
    width = w4 // 4
    w3 = 3 * width
    group = SETS * per
    wide = group * rr
    nm = own // tm
    tiles = 3 * -(-width // 128)
    folded = -(-clips * 3 * RANK // 128)
    final = lambda c, m, *_: (jnp.where(c == nc - 1, m, 0), 0)
    return pl.pallas_call(
        functools.partial(adapt_back_kernel, tm, width, group, per, len(sources), nm),
        out_shape=(
            jax.ShapeDtypeStruct((nc, own, w3), BF),
            jax.ShapeDtypeStruct((own, 3 * wide), BF),
            jax.ShapeDtypeStruct((nc, clips * tiles, RANK, 128), BF),
            jax.ShapeDtypeStruct((folded, D, 128), BF),
        ),
        grid_spec=pltpu.PrefetchScalarGridSpec(
            num_scalar_prefetch=4,
            grid=(nc, nm),
            in_specs=piece_specs(sources, tm, lambda c, m, s, a, i: c * nm + m)
            + [
                pl.BlockSpec((rr, 1, group, w4), lambda c, m, *_: (0, c, D // rr // group, 0)),
                pl.BlockSpec((tm, D), final),
                pl.BlockSpec((tm, 3 * wide), lambda c, m, *_: (m, 0)),
            ],
            out_specs=[
                pl.BlockSpec((1, tm, w3), lambda c, m, *_: (c, m, 0)),
                pl.BlockSpec((tm, 3 * wide), final),
                pl.BlockSpec((1, clips * tiles, RANK, 128), lambda c, m, *_: (c, 0, 0, 0)),
                pl.BlockSpec((folded, D, 128), lambda c, m, *_: (0, 0, 0)),
            ],
            scratch_shapes=[
                pltpu.VMEM((own, 3 * wide), F32),
                pltpu.VMEM((clips, 3, RANK, width), F32),
                pltpu.VMEM((clips, 3 * RANK, D), F32),
            ],
        ),
        compiler_params=params(2),
        cost_estimate=cost(own * D * nc * w3 * 0.6, own * nc * w3 * 4),
        name="adapt_back",
    )(sets, scales, slots, code, *sources, gathered, normed, ranks)


def project_back_kernel(tm, width, dy_ref, w_ref, grank_ref, down, x_ref, gm_ref, gain, gt_ref, acc):
    c = pl.program_id(0)
    m = pl.program_id(1)
    rows = pl.ds(pl.multiple_of(m * tm, tm), tm)
    part = dot_t(dy_ref[0], w_ref[:, 0].reshape(D, 4 * width)[:, 0 : 3 * width])

    @pl.when(c == 0)
    def _():
        acc[rows, :] = part + dot_t(grank_ref[...], down[...])

    @pl.when(c > 0)
    def _():
        acc[rows, :] += part

    @pl.when(c == pl.num_programs(0) - 1)
    def _():
        unit, inverse = norm_parts(x_ref[...].astype(F32))
        e = acc[rows, :] * gain[...]
        mean = jnp.mean(e, axis=-1, keepdims=True)
        second = jnp.mean(e * unit, axis=-1, keepdims=True)
        gt_ref[...] = (gm_ref[...] + (e - mean - unit * second) * inverse).astype(BF)


def project_back(dy, gathered, grank, tables, tokens, grad_middle, gain, tm):
    own = tokens.shape[0]
    rr, nc, _, w4 = gathered.shape
    width = w4 // 4
    w3 = 3 * width
    wide3 = grank.shape[1]
    nm = own // tm
    final = lambda c, m: (jnp.where(c == nc - 1, m, 0), 0)
    return pl.pallas_call(
        functools.partial(project_back_kernel, tm, width),
        out_shape=jax.ShapeDtypeStruct((own, D), BF),
        grid=(nc, nm),
        in_specs=[
            pl.BlockSpec((1, tm, w3), lambda c, m: (c, m, 0)),
            pl.BlockSpec((rr, 1, D // rr, w4), lambda c, m: (0, c, 0, 0)),
            pl.BlockSpec((tm, wide3), lambda c, m: (jnp.where(c == 0, m, nm - 1), 0)),
            pl.BlockSpec((D, wide3), lambda c, m: (0, 0)),
            pl.BlockSpec((tm, D), final),
            pl.BlockSpec((tm, D), final),
            pl.BlockSpec((1, D), lambda c, m: (0, 0)),
        ],
        out_specs=pl.BlockSpec((tm, D), final),
        scratch_shapes=[pltpu.VMEM((own, D), F32)],
        compiler_params=params(2),
        cost_estimate=cost(2 * own * D * nc * w3 * 1.1, D * nc * w3 * 2 + own * (4 * D + nc * w3) * 2),
        name="project_back",
    )(dy, gathered, grank, tables, tokens, grad_middle, gain)


def collect_kernel(nc, nm, ns, code, *refs):
    sources = refs[:ns]
    att_ref, a_scr = refs[ns:]
    m = pl.program_id(0)
    c = pl.program_id(1)
    choose(code[3 * (c * nm + m)], sources, a_scr, c)

    @pl.when(c == nc - 1)
    def _():
        att_ref[...] = jnp.concatenate([a_scr[i] for i in range(nc)], axis=1)


def collect(sources, code, own, tm, nc):
    nm = own // tm
    return pl.pallas_call(
        functools.partial(collect_kernel, nc, nm, len(sources)),
        out_shape=jax.ShapeDtypeStruct((own, D), BF),
        grid_spec=pltpu.PrefetchScalarGridSpec(
            num_scalar_prefetch=1,
            grid=(nm, nc),
            in_specs=piece_specs(sources, tm, lambda m, c: c * nm + m),
            out_specs=pl.BlockSpec((tm, D), lambda m, c, *_: (m, 0)),
            scratch_shapes=[pltpu.VMEM((nc, tm, D // nc), BF)],
        ),
        compiler_params=params(2),
        cost_estimate=cost(own * D, own * D * 10),
        name="collect",
    )(code, *sources)


def out_kernel(group, per, sets, scales, *refs):
    att_ref, x_ref, w_ref, bias, odown, oup, gain, shift, fdown = refs[:9]
    middle_ref, normed_ref, ro_ref, r1_ref = refs[9:]
    m = pl.program_id(0)
    att = att_ref[...]
    ro = dot_t(att, odown[...]) * scales[m]
    keep = set_mask(ro.shape, sets[m], group, per)
    ro = jnp.where(keep, ro, 0.0).astype(BF)
    ro_ref[...] = ro
    middle = x_ref[...].astype(F32) + dot_t(att, w_ref[...]) + dot_t(ro, oup[...]) + bias[...]
    middle_ref[...] = middle
    unit, _ = norm_parts(middle)
    normed = (unit * gain[...] + shift[...]).astype(BF)
    normed_ref[...] = normed
    r1_ref[...] = jnp.where(keep, dot(normed, fdown[...]) * scales[m], 0.0).astype(BF)


def out_project(att, tokens, wo_t, bias, odown, tables, gain, shift, sets, scales, tm, per):
    own = tokens.shape[0]
    wide = odown.shape[0]
    row = lambda m, *_: (m, 0)
    flat = lambda m, *_: (0, 0)
    return pl.pallas_call(
        functools.partial(out_kernel, SETS * per, per),
        out_shape=(
            jax.ShapeDtypeStruct((own, D), F32),
            jax.ShapeDtypeStruct((own, D), BF),
            jax.ShapeDtypeStruct((own, wide), BF),
            jax.ShapeDtypeStruct((own, wide), BF),
        ),
        grid_spec=pltpu.PrefetchScalarGridSpec(
            num_scalar_prefetch=2,
            grid=(own // tm,),
            in_specs=[
                pl.BlockSpec((tm, D), row),
                pl.BlockSpec((tm, D), row),
                pl.BlockSpec((D, D), flat),
                pl.BlockSpec((1, D), flat),
                pl.BlockSpec((wide, D), flat),
                pl.BlockSpec((D, wide), lambda m, *_: (0, 4)),
                pl.BlockSpec((1, D), flat),
                pl.BlockSpec((1, D), flat),
                pl.BlockSpec((D, wide), lambda m, *_: (0, 3)),
            ],
            out_specs=[
                pl.BlockSpec((tm, D), row),
                pl.BlockSpec((tm, D), row),
                pl.BlockSpec((tm, wide), row),
                pl.BlockSpec((tm, wide), row),
            ],
        ),
        compiler_params=params(1),
        cost_estimate=cost(2 * own * D * D * 1.5, D * D * 2 + own * D * 12),
        name="out_project",
    )(sets, scales, att, tokens, wo_t, bias, odown, tables, gain, shift, tables)


def out_back_kernel(nc, width, group, per, sets, scales, side, gb_ref, w_ref, oup, odown, att_ref, ro_ref, *outs):
    away_ref, mine_ref, gup_ref, gdown_ref, gup, gdown = outs
    m = pl.program_id(0)

    @pl.when(m == 0)
    def _():
        gup[...] = jnp.zeros_like(gup)
        gdown[...] = jnp.zeros_like(gdown)

    gb = gb_ref[...]
    gro = dot(gb, oup[...]) * scales[m]
    gro = jnp.where(set_mask(gro.shape, sets[m], group, per), gro, 0.0)
    ga = (dot(gb, w_ref[...]) + dot(gro.astype(BF), odown[...])).astype(BF)
    half = nc // 2
    for i in range(nc):
        piece = ga[:, i * width : (i + 1) * width]

        @pl.when(side[0] == i // half)
        def _(i=i, piece=piece):
            mine_ref[i % half, :, 0:width] = piece

        @pl.when(side[0] != i // half)
        def _(i=i, piece=piece):
            away_ref[i % half, :, 0:width] = piece

    gup[...] += dot(ro_ref[...].T, gb)
    gdown[...] += token_sum(gro, att_ref[...])

    @pl.when(m == pl.num_programs(0) - 1)
    def _():
        gup_ref[...] = gup[...].T.astype(BF)
        whole = gdown[...]
        for i in range(nc):
            for t, tile in enumerate(lane_tiles(whole[:, i * width : (i + 1) * width], group)):
                gdown_ref[:, i, t * group : (t + 1) * group, :] = tile.astype(BF)


def out_back(gb, wo_t, tables, odown, att, ro, sets, scales, side, tm, nc, per, rr):
    own = gb.shape[0]
    width = D // nc
    group = SETS * per
    wide = group * rr
    half = nc // 2
    tiles = -(-width // 128)
    row = lambda m, *_: (m, 0)
    flat = lambda m, *_: (0, 0)
    return pl.pallas_call(
        functools.partial(out_back_kernel, nc, width, group, per),
        out_shape=(
            jax.ShapeDtypeStruct((half, own, lanes_of(width)), BF),
            jax.ShapeDtypeStruct((half, own, lanes_of(width)), BF),
            jax.ShapeDtypeStruct((D, wide), BF),
            jax.ShapeDtypeStruct((rr, nc, tiles * group, 128), BF),
        ),
        grid_spec=pltpu.PrefetchScalarGridSpec(
            num_scalar_prefetch=3,
            grid=(own // tm,),
            in_specs=[
                pl.BlockSpec((tm, D), row),
                pl.BlockSpec((D, D), flat),
                pl.BlockSpec((D, wide), lambda m, *_: (0, 4)),
                pl.BlockSpec((wide, D), flat),
                pl.BlockSpec((tm, D), row),
                pl.BlockSpec((tm, wide), row),
            ],
            out_specs=[
                pl.BlockSpec((half, tm, lanes_of(width)), lambda m, *_: (0, m, 0)),
                pl.BlockSpec((half, tm, lanes_of(width)), lambda m, *_: (0, m, 0)),
                pl.BlockSpec((D, wide), flat),
                pl.BlockSpec((rr, nc, tiles * group, 128), lambda m, *_: (0, 0, 0, 0)),
            ],
            scratch_shapes=[pltpu.VMEM((wide, D), F32), pltpu.VMEM((wide, D), F32)],
        ),
        compiler_params=params(1),
        cost_estimate=cost(2 * own * D * D * 1.5, D * D * 2 + own * D * 6),
        name="out_back",
    )(sets, scales, side, gb, wo_t, tables, odown, att, ro)


def mlp_kernel(tm, nm, group, per, sets, scales, *refs):
    n_ref, g_ref, mid_ref, w1_ref, w2_ref, b1, up1_ref, down2_ref, up2, down1, r1_ref, bias2, gain = refs[:13]
    out_ref, gm_ref, gb_ref, gup1_ref, gdown2_ref, gup2_ref, gdown1_ref = refs[13:20]
    acc, gacc, r2acc, gr1acc, gr2, gup1, gdown2, gup2, gdown1 = refs[20:]
    c = pl.program_id(0)
    m = pl.program_id(1)
    rows = pl.ds(pl.multiple_of(m * tm, tm), tm)
    a = scales[m]
    g = g_ref[...]
    normed = n_ref[...]
    hidden = w1_ref.shape[-1]
    wide = r1_ref.shape[1]
    keep = set_mask((tm, wide), sets[m], group, per)

    @pl.when(c == 0)
    def _():
        gr2[rows, :] = jnp.where(keep, dot(g, up2[...]) * a, 0.0).astype(BF)
        acc[rows, :] = jnp.zeros((tm, D), F32)
        gacc[rows, :] = jnp.zeros((tm, D), F32)
        r2acc[rows, :] = jnp.zeros((tm, wide), F32)
        gr1acc[rows, :] = jnp.zeros((tm, wide), F32)

    @pl.when(m == 0)
    def _():
        gup1[...] = jnp.zeros_like(gup1)
        gdown2[...] = jnp.zeros_like(gdown2)

    @pl.when((m == 0) & (c == 0))
    def _():
        gup2[...] = jnp.zeros_like(gup2)
        gdown1[...] = jnp.zeros_like(gdown1)

    w1 = w1_ref[:, 0].reshape(D, hidden)
    w2 = w2_ref[:, 0].reshape(D, hidden)
    up1 = up1_ref[:, 0].reshape(wide, hidden)
    down2 = down2_ref[:, 0].reshape(wide, hidden)
    r1 = r1_ref[...]
    grank2 = gr2[rows, :]
    pre = dot(normed, w1) + dot(r1, up1) + b1[0]
    upper = 0.5 + 0.5 * lax.erf(pre * (0.5**0.5))
    density = jnp.exp(pre * pre * -0.5) * ((2.0 * math.pi) ** -0.5)
    act = (pre * upper).astype(BF)
    slope = upper + pre * density
    gact = dot(g, w2) + dot(grank2, down2)
    gpre = (gact * slope).astype(BF)
    acc[rows, :] += dot_t(act, w2)
    r2acc[rows, :] += dot_t(act, down2)
    gacc[rows, :] += dot_t(gpre, w1)
    gr1acc[rows, :] += dot_t(gpre, up1)
    gdown2[...] += dot(grank2.T, act)
    gup1[...] += dot(r1.T, gpre)

    @pl.when(m == nm - 1)
    def _():
        put_tiles(gup1_ref, 0, gup1[...], group)
        put_tiles(gdown2_ref, 0, gdown2[...], group)

    @pl.when(c == pl.num_programs(0) - 1)
    def _():
        r2 = jnp.where(keep, r2acc[rows, :] * a, 0.0).astype(BF)
        middle = mid_ref[...]
        out_ref[...] = (middle + acc[rows, :] + dot_t(r2, up2[...]) + bias2[...]).astype(BF)
        gup2[...] += dot(r2.T, g)
        gr1 = jnp.where(keep, gr1acc[rows, :] * a, 0.0).astype(BF)
        e = (gacc[rows, :] + dot_t(gr1, down1[...])) * gain[...]
        gdown1[...] += dot(gr1.T, normed)
        unit, inverse = norm_parts(middle)
        mean = jnp.mean(e, axis=-1, keepdims=True)
        second = jnp.mean(e * unit, axis=-1, keepdims=True)
        gm = g.astype(F32) + (e - mean - unit * second) * inverse
        gm_ref[...] = gm
        gb_ref[...] = gm.astype(BF)

        @pl.when(m == nm - 1)
        def _():
            gup2_ref[...] = gup2[...].T.astype(BF)
            gdown1_ref[...] = gdown1[...].T.astype(BF)


def mlp(normed, g, middle, gathered, b1, tables, r1, bias2, gain, sets, scales, tm, per, at):
    own = g.shape[0]
    rr, nc, _, hidden = gathered.shape
    group = SETS * per
    wide = group * rr
    nm = own // tm
    tiles = -(-hidden // 128)
    row = lambda c, m, *_: (m, 0)
    final = lambda c, m, *_: (jnp.where(c == nc - 1, m, 0), 0)
    flat = lambda c, m, *_: (0, 0)
    wblock = (rr, 1, D // rr, hidden)
    return pl.pallas_call(
        functools.partial(mlp_kernel, tm, nm, group, per),
        out_shape=(
            jax.ShapeDtypeStruct((own, D), BF),
            jax.ShapeDtypeStruct((own, D), F32),
            jax.ShapeDtypeStruct((own, D), BF),
            jax.ShapeDtypeStruct((rr, nc, tiles * group, 128), BF),
            jax.ShapeDtypeStruct((rr, nc, tiles * group, 128), BF),
            jax.ShapeDtypeStruct((D, wide), BF),
            jax.ShapeDtypeStruct((D, wide), BF),
        ),
        grid_spec=pltpu.PrefetchScalarGridSpec(
            num_scalar_prefetch=2,
            grid=(nc, nm),
            in_specs=[
                pl.BlockSpec((tm, D), row),
                pl.BlockSpec((tm, D), row),
                pl.BlockSpec((tm, D), final, pipeline_mode=pl.Buffered(1)),
                pl.BlockSpec(wblock, lambda c, m, *_: (0, c, 0, 0)),
                pl.BlockSpec(wblock, lambda c, m, *_: (0, c, 1, 0)),
                pl.BlockSpec((1, 1, hidden), lambda c, m, *_: (c, 0, 0)),
                pl.BlockSpec((rr, 1, group, hidden), lambda c, m, *_: (0, c, at // group, 0)),
                pl.BlockSpec((rr, 1, group, hidden), lambda c, m, *_: (0, c, at // group + 1, 0)),
                pl.BlockSpec((D, wide), lambda c, m, *_: (0, 5), pipeline_mode=pl.Buffered(1)),
                pl.BlockSpec((D, wide), lambda c, m, *_: (0, 3), pipeline_mode=pl.Buffered(1)),
                pl.BlockSpec((tm, wide), row),
                pl.BlockSpec((1, D), flat),
                pl.BlockSpec((1, D), flat),
            ],
            out_specs=[
                pl.BlockSpec((tm, D), final),
                pl.BlockSpec((tm, D), final),
                pl.BlockSpec((tm, D), final),
                pl.BlockSpec((rr, 1, tiles * group, 128), lambda c, m, *_: (0, c, 0, 0)),
                pl.BlockSpec((rr, 1, tiles * group, 128), lambda c, m, *_: (0, c, 0, 0)),
                pl.BlockSpec((D, wide), flat),
                pl.BlockSpec((D, wide), flat),
            ],
            scratch_shapes=[
                pltpu.VMEM((own, D), F32),
                pltpu.VMEM((own, D), F32),
                pltpu.VMEM((own, wide), F32),
                pltpu.VMEM((own, wide), F32),
                pltpu.VMEM((own, wide), BF),
                pltpu.VMEM((wide, hidden), F32),
                pltpu.VMEM((wide, hidden), F32),
                pltpu.VMEM((wide, D), F32),
                pltpu.VMEM((wide, D), F32),
            ],
        ),
        compiler_params=params(2, 67043328),
        cost_estimate=cost(8 * own * D * nc * hidden * 1.2, D * nc * hidden * 4 + own * D * 30, own * nc * hidden * 2),
        name="mlp",
    )(
        sets, scales, normed, g, middle, gathered, gathered, b1, gathered, gathered, tables, tables, r1, bias2, gain
    )


def assemble_kernel(width, w_ref, o_ref, w_out, o_out):
    nc = w_ref.shape[1]
    columns = [w_ref[:, c].reshape(D, 2 * width)[:, width:] for c in range(nc)]
    downs = [o_ref[:, c].reshape(-1, 2 * width)[:, width:] for c in range(nc)]
    w_out[...] = jnp.concatenate(columns, axis=1)
    o_out[...] = jnp.concatenate(downs, axis=1)


def assemble(gathered, group):
    nr, nc, _, w4 = gathered.shape
    width = w4 // 4
    rows = D // nr
    if 2 * width % 128 == 0:
        return pl.pallas_call(
            functools.partial(assemble_kernel, width),
            out_shape=(
                jax.ShapeDtypeStruct((D, D), BF),
                jax.ShapeDtypeStruct((nr * group, D), BF),
            ),
            grid=(1,),
            in_specs=[
                pl.BlockSpec((nr, nc, rows, 2 * width), lambda i: (0, 0, 0, 1)),
                pl.BlockSpec((nr, nc, group, 2 * width), lambda i: (0, 0, rows // group, 1)),
            ],
            out_specs=[
                pl.BlockSpec((D, D), lambda i: (0, 0)),
                pl.BlockSpec((nr * group, D), lambda i: (0, 0)),
            ],
            compiler_params=params(1),
            name="assemble",
        )(gathered, gathered)
    w = gathered[:, :, :rows, 3 * width :]
    o = gathered[:, :, rows : rows + group, 3 * width :]
    return (
        w.transpose(0, 2, 1, 3).reshape(D, D),
        o.transpose(0, 2, 1, 3).reshape(nr * group, D),
    )


def pick(flag, first, second):
    return jnp.where(flag, first, second)


def table_of(values):
    return jnp.stack([jnp.asarray(v, jnp.int32) for v in values])


class Exchange:
    def __init__(self, nc, own, clips, clip_len, tm):
        self.nc, self.own, self.clips, self.clip_len, self.tm = nc, own, clips, clip_len, tm
        self.local = nc == 4 and clips == 3 and own == 3 * tm and clip_len == 4 * tm
        col = lax.axis_index("cols")
        self.nm = nm = own // tm
        if not self.local:
            self.order = jnp.arange(nc, dtype=jnp.int32)
            self.side = jnp.ones((1,), jnp.int32)
            self.plans = [jnp.zeros((2,), jnp.int32)]
            self.indices = [jnp.arange(clips, dtype=jnp.int32)]
            entry = jnp.arange(nc * nm, dtype=jnp.int32)
            self.code = jnp.stack([entry * 0, entry // nm, entry % nm], axis=1).reshape(-1)
            return
        y, k = col // 2, col % 2
        self.y, self.k = y, k
        self.holder = y != k
        self.order = (jnp.arange(4, dtype=jnp.int32) + 2 * (1 - k)) % 4
        self.side = k[None]
        b = jnp.arange(4, dtype=jnp.int32)
        g = b + 2 * y
        clip_plan = jnp.concatenate([pick(g // 3 == k, 0, 1), g % 3])
        g = pick(y == 0, 4 + b, b - 2)
        near = b // 2 == y
        source = pick(near, pick(g // 3 == k, 0, 1), pick(self.holder, 3, 2))
        shared_plan = jnp.concatenate([source, pick(near, g % 3, b % 2)])
        self.plans = [clip_plan.astype(jnp.int32), shared_plan.astype(jnp.int32)]
        self.indices = [jnp.array([0, 1, 0, 1], jnp.int32), table_of([y, y, 0, 0])]
        entry = jnp.arange(12, dtype=jnp.int32)
        c, m = entry // 3, entry % 3
        g = 3 * k + m
        inside = (g >= 2 * y) & (g < 2 * y + 4)
        same, idx = c // 2 == k, c % 2
        source = pick(
            inside,
            pick(same, 0, 2),
            pick(idx == y, pick(same, 1, 3), pick(same, 4, 5)),
        )
        block = pick(
            inside,
            g - 2 * y,
            pick(y == 0, g - 4, pick(idx == y, g + 2, g)),
        )
        self.code = (
            jnp.stack([source, pick(inside, idx, 0), block], axis=1).astype(jnp.int32).reshape(-1)
        )

    def lens(self, lengths):
        if not self.local:
            return (lengths,)
        mine = pick(self.y == 0, lengths[0], lengths[2])
        return (jnp.stack([mine, mine]), lengths[1:2])

    def to_heads(self, away, mine):
        f = mine.shape[-1]
        if not self.local:
            moved = lax.all_to_all(jnp.concatenate([away, mine]), "cols", 0, 0, tiled=True)
            return [[moved.reshape(self.clips, self.clip_len, f)]]
        y, k, half = self.y, self.k, self.clip_len // 2
        start = pick(k == 1, self.own - half, 0)
        got = lax.ppermute(away, "cols", [(i, i ^ 1) for i in range(4)])
        one = lax.dynamic_slice(mine, (1 - y, start, 0), (1, half, f))
        two = lax.dynamic_slice(away, (1 - y, start, 0), (1, half, f))
        got_one = lax.ppermute(one, "cols", [(1, 3), (2, 0)])
        got_two = lax.ppermute(two, "cols", [(1, 2), (2, 1)])
        return [[mine, got], [mine, got, got_one, got_two]]

    def from_heads(self, parts):
        if not self.local:
            (v,) = parts
            v = v.reshape(self.nc, self.own, v.shape[-1])
            return [lax.all_to_all(v, "cols", 0, 0, tiled=True)]
        clip, shared = parts
        half = self.clip_len // 2
        far = lax.dynamic_slice(shared, (0, (1 - self.y) * half, 0), (1, half, clip.shape[-1]))
        swap = [(i, i ^ 1) for i in range(4)]
        got_one = lax.ppermute(far, "cols", [(3, 1), (0, 2)])
        got_two = lax.ppermute(far, "cols", [(2, 1), (1, 2)])
        got_shared = lax.ppermute(shared, "cols", swap)
        return [clip, shared, lax.ppermute(clip, "cols", swap), got_shared, got_one, got_two]


def up_to(n, k):
    return -(-n // k) * k


def rows_padded(v, rows, lanes):
    return jnp.pad(v.astype(BF), ((0, rows - v.shape[0]), (0, lanes - v.shape[1])))


def halves(v):
    high = v.astype(BF)
    return high, (v - high.astype(F32)).astype(BF)


def scatter_sum(pieces):
    whole = jnp.concatenate(pieces, axis=2)
    n = whole.shape[2]
    whole = jnp.pad(whole, ((0, 0), (0, 0), (0, up_to(n, 8) - n), (0, 0)))
    return whole.reshape(-1, 128)


def join(v, nc):
    col = lax.axis_index("cols")
    zeros = (0,) * v.ndim
    held = lax.dynamic_update_slice(jnp.zeros((nc,) + v.shape, v.dtype), v[None], (col,) + zeros)
    step = 1
    while step < nc:
        base = col // step * step
        sent = lax.dynamic_slice(held, (base,) + zeros, (step,) + v.shape)
        got = lax.ppermute(sent, "cols", [(i, i ^ step) for i in range(nc)])
        held = lax.dynamic_update_slice(held, got, (base ^ step,) + zeros)
        step *= 2
    return held


def body(
    tokens,
    cotangent,
    clip_lengths,
    clip_sets,
    clip_scales,
    norm1_gain,
    norm1_shift,
    w_query,
    query_bias,
    w_key,
    w_value,
    value_bias,
    w_out,
    out_bias,
    norm2_gain,
    norm2_shift,
    w_fc1,
    fc1_bias,
    w_fc2,
    fc2_bias,
    query_down,
    query_up,
    key_down,
    key_up,
    value_down,
    value_up,
    out_down,
    out_up,
    fc1_down,
    fc1_up,
    fc2_down,
    fc2_up,
):
    nr = lax.axis_size("rows")
    nc = lax.axis_size("cols")
    col = lax.axis_index("cols")
    clips = clip_lengths.shape[0]
    own = tokens.shape[0]
    clip_len = own * nc // clips
    tm = math.gcd(own, clip_len)
    width = query_bias.shape[0]
    hidden = fc1_bias.shape[0]
    hh = width // HEAD_DIM
    dr = w_query.shape[0]
    per = RANK // nr
    group = SETS * per
    wide = group * nr
    dc = dr // nc
    exchange = Exchange(nc, own, clips, clip_len, tm)

    block_clip = (col * own + jnp.arange(own // tm, dtype=jnp.int32) * tm) // clip_len
    sets = jnp.take(clip_sets, block_clip)
    scales = jnp.take(clip_scales, block_clip)

    downs = jnp.stack([query_down, key_down, value_down, fc1_down])
    downs = lax.dynamic_slice(downs, (0, 0, col * dc, 0), (4, SETS, dc, RANK))
    downs = downs.reshape(4, SETS, dc, nr, per).transpose(2, 0, 3, 1, 4).reshape(dc, 4 * wide)
    ups = jnp.stack([out_up, fc2_up])
    ups = lax.dynamic_slice(ups, (0, 0, 0, col * dc), (2, SETS, RANK, dc))
    ups = ups.reshape(2, SETS, nr, per, dc).transpose(4, 0, 2, 1, 3).reshape(dc, 2 * wide)
    tables = jnp.concatenate([downs, ups], axis=1)

    lanes = 4 * width
    turn = lambda v: jnp.swapaxes(v, 1, 2).reshape(group, -1)
    extra = jnp.concatenate(
        [*halves(query_bias), *halves(value_bias), *halves(fc1_bias), clip_sets.astype(BF)]
    )
    extra_lanes = up_to(-(-extra.shape[0] // dc), 128)
    extra = jnp.pad(extra, (0, dc * extra_lanes - extra.shape[0])).reshape(dc, extra_lanes)
    small = jnp.concatenate([tables, extra], axis=1)
    small_lanes = small.shape[1]
    natural = lanes >= small_lanes
    small = rows_padded(small, dc, lanes) if natural else small.reshape(-1, lanes)
    small_rows = small.shape[0]
    at_table = dr + group
    packed = jnp.concatenate(
        [
            jnp.concatenate([w_query, w_key, w_value, w_out.T], axis=1),
            jnp.concatenate(
                [v.reshape(group, width) for v in (query_up, key_up, value_up)] + [turn(out_down)], axis=1
            ),
            rows_padded(small, up_to(small_rows, 8), lanes),
        ],
        axis=0,
    )
    g1 = lax.all_gather(packed, BOTH, axis=0).reshape(nr, nc, -1, lanes)
    small = g1[:, :, at_table : at_table + small_rows]
    small = small[..., :small_lanes] if natural else small.reshape(nr, nc, dc, small_lanes)
    tables = small[..., : 6 * wide].reshape(D, 6 * wide)
    extra = small[..., 6 * wide :].reshape(nr, nc, -1)
    sums = extra[0].astype(F32)
    both = lambda at, n: sums[:, at : at + n] + sums[:, at + n : at + 2 * n]
    zeros = jnp.zeros((nc, width), F32)
    bias_qkv = jnp.concatenate([both(0, width), zeros, both(2 * width, width)], axis=1)[:, None]
    b1 = both(4 * width, hidden)[:, None]
    every_set = extra[:, 0, 4 * width + 2 * hidden :][:, :clips].astype(jnp.int32)
    wo_t, odown = assemble(g1, group)

    packed = jnp.concatenate(
        [w_fc1, w_fc2.T, fc1_up.reshape(group, hidden), turn(fc2_down)], axis=0
    )
    packed, g1 = lax.optimization_barrier((packed, g1))
    g2 = lax.all_gather(packed, BOTH, axis=0).reshape(nr, nc, -1, hidden)
    at_f = 2 * dr

    gain1, shift1 = norm1_gain[None], norm1_shift[None]
    gain2, shift2 = norm2_gain[None], norm2_shift[None]

    normed, ranks, away, mine = project(
        tokens, gain1, shift1, g1, bias_qkv, tables, sets, scales, exchange.order, tm, per
    )
    lens = exchange.lens(clip_lengths)
    results = []
    for sources, plan, index, n in zip(
        exchange.to_heads(away, mine), exchange.plans, exchange.indices, lens
    ):
        if results:
            n, _ = lax.optimization_barrier((n, results[-1][1]))
        results.append(attend(sources, plan, index, n, clip_len, hh))
    pieces = exchange.from_heads([r[0] for r in results])
    att = collect(pieces, exchange.code, own, tm, nc)
    middle, normed_mlp, ro, r1 = out_project(
        att, tokens, wo_t, out_bias[None], odown, tables, gain2, shift2, sets, scales, tm, per
    )
    output, grad_middle, grad_branch, gup1, gdown2, gup2, gdown1 = mlp(
        normed_mlp, cotangent, middle, g2, b1, tables, r1, fc2_bias[None], gain2, sets, scales, tm, per, at_f
    )
    away, mine, goup, godown = out_back(
        grad_branch, wo_t, tables, odown, att, ro, sets, scales, exchange.side, tm, nc, per, nr
    )

    by_model = lambda v: v.reshape(nr, nc, dc, wide)
    late = scatter_sum([gup1, gdown2, godown, by_model(gdown1), by_model(goup), by_model(gup2)])
    late = lax.psum_scatter(late, BOTH, scatter_dimension=0, tiled=True)

    def untile(v, n):
        t = v.shape[0] // group
        return v.reshape(t, group, 128).transpose(1, 0, 2).reshape(group, t * 128)[:, :n].reshape(SETS, per, n)

    def model_tables(v):
        k = v.shape[0] // dc
        every = join(v, nc).reshape(nc, k, dc, wide).swapaxes(0, 1)
        return every.reshape(k, dr, nr, SETS, per)

    as_down = lambda v: v.transpose(2, 0, 1, 3).reshape(SETS, dr, RANK)
    as_up = lambda v: v.transpose(2, 1, 3, 0).reshape(SETS, RANK, dr)
    flip = lambda v: jnp.swapaxes(v, 1, 2)
    calls = list(
        zip(exchange.to_heads(away, mine), exchange.plans, exchange.indices, results, lens)
    )
    backs = []
    for sources, plan, index, (o, lse, x), n in reversed(calls):
        if backs:
            n, _ = lax.optimization_barrier((n, backs[-1]))
        backs.append(attend_back(sources, plan, index, x, o, lse, n, hh))
    pieces = exchange.from_heads(backs[::-1])
    dy, grank, gup, gdown = adapt_back(
        pieces, exchange.code, g1, normed, ranks, sets, scales, block_clip, clips, tm, per
    )
    tiles = gup.shape[1] // (3 * clips)
    folded = gdown.shape[0]
    ups = gup.reshape(nc, clips * 3 * tiles, nr, per, 128).transpose(2, 0, 1, 3, 4)
    ups = ups.reshape(nr, nc, -1, 128)
    downs = [gdown[i].reshape(nr, nc, dc, 128) for i in range(folded)]
    last = scatter_sum([ups] + downs).reshape(nr * nc, -1, 128)
    last, dy = lax.optimization_barrier((last, dy))
    got = lax.all_to_all(last, BOTH, 0, 0, tiled=True)
    grad_tokens = project_back(dy, g1, grank, tables, tokens, grad_middle, gain1, tm)
    late, grad_tokens = lax.optimization_barrier((late, grad_tokens))
    summed = late.astype(F32)
    a = gup1.shape[2]
    b = godown.shape[2]
    grad_fc1_up = untile(summed[:a], hidden)
    grad_fc2_down = flip(untile(summed[a : 2 * a], hidden))
    grad_out_down = flip(untile(summed[2 * a : 2 * a + b], width))
    model = model_tables(summed[2 * a + b : 2 * a + b + 3 * dc])
    grad_fc1_down, grad_out_up, grad_fc2_up = as_down(model[0]), as_up(model[1]), as_up(model[2])

    got = jnp.sum(got.reshape(nr, nc, -1, 128).astype(F32), axis=1)
    onehot = (every_set[:, :, None] == jnp.arange(SETS, dtype=jnp.int32)).astype(F32)
    n = ups.shape[2]
    per_clip = got[:, :n].reshape(nr, clips, -1, 128)
    per_set = jnp.sum(onehot[:, :, :, None, None] * per_clip[:, :, None], axis=(0, 1))
    per_set = per_set.reshape(SETS, 3, tiles, per, 128).transpose(1, 0, 3, 2, 4)
    up = per_set.reshape(3, SETS, per, tiles * 128)[..., :width]
    side = got[:, n : n + folded * dc].reshape(nr, folded, dc, 128).transpose(0, 2, 1, 3)
    side = side.reshape(nr, dc, folded * 128)[..., : clips * 3 * RANK]
    side = side.reshape(nr, dc, clips, 3 * RANK).transpose(0, 2, 1, 3)
    side = jnp.sum(onehot[:, :, :, None, None] * side[:, :, None], axis=(0, 1))
    side = side.transpose(1, 0, 2).reshape(dc, SETS * 3 * RANK)
    side = lax.all_gather(side, "cols", axis=0, tiled=True).reshape(dr, SETS, 3, RANK)
    down = side.transpose(2, 1, 0, 3)
    return (
        output,
        grad_tokens,
        down[0],
        up[0],
        down[1],
        up[1],
        down[2],
        up[2],
        grad_out_down,
        grad_out_up,
        grad_fc1_down,
        grad_fc1_up,
        grad_fc2_down,
        grad_fc2_up,
    )


def solution(mesh):
    both = P(("rows", "cols"), None)
    grid = P("rows", "cols")
    turned = P("cols", "rows")
    down = P(None, "rows", None)
    up = P(None, "rows", "cols")
    far_down = P(None, "cols", "rows")
    far_up = P(None, None, "rows")
    return jax.shard_map(
        body,
        mesh=mesh,
        in_specs=(
            both,
            both,
            P("rows"),
            P("rows"),
            P("rows"),
            P(),
            P(),
            grid,
            P("cols"),
            grid,
            grid,
            P("cols"),
            turned,
            P(),
            P(),
            P(),
            grid,
            P("cols"),
            turned,
            P(),
            down,
            up,
            down,
            up,
            down,
            up,
            far_down,
            far_up,
            down,
            up,
            far_down,
            far_up,
        ),
        out_specs=(
            both,
            both,
            down,
            up,
            down,
            up,
            down,
            up,
            far_down,
            far_up,
            down,
            up,
            far_down,
            far_up,
        ),
        check_vma=False,
    )
```

```python
import functools
import math

import jax
import jax.numpy as jnp
from jax import lax
from jax.experimental import pallas as pl
from jax.experimental.pallas import tpu as pltpu
from jax.sharding import PartitionSpec as P


D = 1280
SETS = 8
RANK = 16
HEAD_DIM = 80
EPSILON = 1e-05
LOG2E = 1.4426950408889634
LOW = -1e30
F32 = jnp.float32
BF = jnp.bfloat16
BOTH = ("rows", "cols")


def dot(a, b):
    return lax.dot_general(a, b, (((1,), (0,)), ((), ())), preferred_element_type=F32)


def dot_t(a, b):
    return lax.dot_general(a, b, (((1,), (1,)), ((), ())), preferred_element_type=F32)


def token_sum(a, b):
    return dot(a.T.astype(BF), b)


def norm_parts(x):
    mean = jnp.mean(x, axis=-1, keepdims=True)
    centred = x - mean
    inverse = lax.rsqrt(jnp.mean(centred * centred, axis=-1, keepdims=True) + EPSILON)
    return centred * inverse, inverse


def params(n, limit=60 << 20):
    return pltpu.CompilerParams(
        dimension_semantics=("arbitrary",) * n, vmem_limit_bytes=limit
    )


def cost(flops, nbytes, trans=0):
    return pl.CostEstimate(flops=int(flops), bytes_accessed=int(nbytes), transcendentals=int(trans))


def set_mask(shape, which, group, per):
    column = lax.broadcasted_iota(jnp.int32, shape, len(shape) - 1)
    return (column % group) // per == which


def choose(code, refs, dst, at):
    for j, ref in enumerate(refs):

        @pl.when(code == j)
        def _(ref=ref):
            dst[at] = ref[0, :, 0 : dst.shape[-1]]


def gather_clip(refs, plan, dst, bs):
    blocks = plan.shape[0] // 2
    for b in range(blocks):
        rows = slice(b * bs, (b + 1) * bs)
        for j, ref in enumerate(refs):

            @pl.when(plan[b] == j)
            def _(ref=ref, b=b, rows=rows):
                off = pl.multiple_of(plan[blocks + b] * bs, bs)
                dst[0, rows, :] = ref[0, pl.ds(off, bs), 0 : dst.shape[2]]


def attend_kernel(hh, length, qb, kb, ns, lens, plan, index, *refs):
    sources, (o_ref, lse_ref, x_ref, k_scr, vt_scr, acc, m_scr, l_scr) = refs[:ns], refs[ns:]
    p = pl.program_id(0)
    qi = pl.program_id(1)
    w = hh * HEAD_DIM
    c = HEAD_DIM**-0.5 * LOG2E

    @pl.when(qi == 0)
    def _():
        gather_clip(sources, plan, x_ref, 2 * length // plan.shape[0])
        vt_scr[...] = x_ref[0, :, 2 * w : 3 * w].T
        for h in range(hh):
            k_scr[h] = x_ref[0, :, w + h * HEAD_DIM : w + (h + 1) * HEAD_DIM]

    size = lens[p]
    block = x_ref[0, pl.ds(pl.multiple_of(qi * qb, qb), qb), 0:w]
    qs = [block[:, h * HEAD_DIM : (h + 1) * HEAD_DIM] for h in range(hh)]
    m_scr[...] = jnp.full_like(m_scr, LOW)
    l_scr[...] = jnp.zeros_like(l_scr)
    acc[...] = jnp.zeros_like(acc)

    def chunk(i, masked):
        r0 = pl.multiple_of(i * kb, kb)
        for h in range(hh):
            s = dot_t(k_scr[h, pl.ds(r0, kb), :], qs[h])
            if masked:
                keys = lax.broadcasted_iota(jnp.int32, (kb, qb), 0) + i * kb
                s = jnp.where(keys < size, s, LOW)
            old = m_scr[h : h + 1]
            top = jnp.maximum(old, jnp.max(s, axis=0, keepdims=True))
            probs = jnp.exp2((s - top) * c)
            shrink = jnp.exp2((old - top) * c)
            l_scr[h : h + 1] = l_scr[h : h + 1] * shrink + jnp.sum(probs, axis=0, keepdims=True)
            m_scr[h : h + 1] = top
            acc[h] = acc[h] * shrink + dot(
                vt_scr[h * HEAD_DIM : (h + 1) * HEAD_DIM, pl.ds(r0, kb)], probs.astype(BF)
            )

    full = size // kb

    def step(i, carry):
        chunk(i, False)
        return carry

    lax.fori_loop(0, full, step, 0)

    @pl.when(full * kb < size)
    def _():
        chunk(full, True)

    outs = [acc[h] * (1.0 / l_scr[h : h + 1]) for h in range(hh)]
    o_ref[0, :, 0:w] = jnp.concatenate(outs, axis=0).T.astype(BF)
    lse_ref[0] = m_scr[0:hh] * c + jnp.log2(l_scr[0:hh])


def lanes_of(n):
    return -(-n // 128) * 128


def source_specs(sources, problems):
    def spec(j, v):
        return pl.BlockSpec(
            (1,) + v.shape[1:], lambda p, q, l, plan, index: (index[j * problems + p], 0, 0)
        )

    return [spec(j, v) for j, v in enumerate(sources)]


def attend(sources, plan, index, lens, length, hh):
    problems = lens.shape[0]
    w3 = 3 * hh * HEAD_DIM
    w = hh * HEAD_DIM
    qb = math.gcd(length, 512)
    kb = math.gcd(length, 768)
    return pl.pallas_call(
        functools.partial(attend_kernel, hh, length, qb, kb, len(sources)),
        out_shape=(
            jax.ShapeDtypeStruct((problems, length, lanes_of(w)), BF),
            jax.ShapeDtypeStruct((problems, hh, length), F32),
            jax.ShapeDtypeStruct((problems, length, w3), BF),
        ),
        grid_spec=pltpu.PrefetchScalarGridSpec(
            num_scalar_prefetch=3,
            grid=(problems, length // qb),
            in_specs=source_specs(sources, problems),
            out_specs=[
                pl.BlockSpec((1, qb, lanes_of(w)), lambda p, q, *_: (p, q, 0)),
                pl.BlockSpec((1, hh, qb), lambda p, q, *_: (p, 0, q)),
                pl.BlockSpec((1, length, w3), lambda p, q, *_: (p, 0, 0)),
            ],
            scratch_shapes=[
                pltpu.VMEM((hh, length, HEAD_DIM), BF),
                pltpu.VMEM((w, length), BF),
                pltpu.VMEM((hh, HEAD_DIM, qb), F32),
                pltpu.VMEM((max(8, hh), qb), F32),
                pltpu.VMEM((max(8, hh), qb), F32),
            ],
        ),
        compiler_params=params(2),
        cost_estimate=cost(
            problems * hh * 4 * length * length * 256,
            problems * length * w3 * 6,
            problems * hh * length * length,
        ),
        name="attend",
    )(lens, plan, index, *sources)


def attend_back_kernel(hh, length, qb, kb, ns, lens, plan, index, *refs):
    sources = refs[:ns]
    x_ref, o_ref, lse_ref, dx_ref, do_scr, k_scr, v_scr, kt_scr, dk, dv, dqt = refs[ns:]
    p = pl.program_id(0)
    qi = pl.program_id(1)
    w = hh * HEAD_DIM
    scale = HEAD_DIM**-0.5
    c = scale * LOG2E

    @pl.when(qi == 0)
    def _():
        gather_clip(sources, plan, do_scr, 2 * length // plan.shape[0])
        kt_scr[...] = x_ref[0, :, w : 2 * w].T
        for h in range(hh):
            k_scr[h] = x_ref[0, :, w + h * HEAD_DIM : w + (h + 1) * HEAD_DIM]
            v_scr[h] = x_ref[0, :, 2 * w + h * HEAD_DIM : 2 * w + (h + 1) * HEAD_DIM]
        dk[...] = jnp.zeros_like(dk)
        dv[...] = jnp.zeros_like(dv)

    size = lens[p]
    rows = pl.ds(pl.multiple_of(qi * qb, qb), qb)
    block = x_ref[0, rows, 0:w]
    qs = [block[:, h * HEAD_DIM : (h + 1) * HEAD_DIM] for h in range(hh)]
    do = do_scr[0, rows, :]
    dos = [do[:, h * HEAD_DIM : (h + 1) * HEAD_DIM] for h in range(hh)]
    prod = (do.astype(F32) * o_ref[0, :, 0:w].astype(F32)).T
    inner = [
        jnp.sum(prod[h * HEAD_DIM : (h + 1) * HEAD_DIM], axis=0, keepdims=True) for h in range(hh)
    ]
    dqt[...] = jnp.zeros_like(dqt)

    def chunk(i, masked):
        keys_at = pl.ds(pl.multiple_of(i * kb, kb), kb)
        for h in range(hh):
            s = dot_t(k_scr[h, keys_at, :], qs[h])
            probs = jnp.exp2(s * c - lse_ref[0, h : h + 1])
            if masked:
                keys = lax.broadcasted_iota(jnp.int32, (kb, qb), 0) + i * kb
                probs = jnp.where(keys < size, probs, 0.0)
            dp = dot_t(v_scr[h, keys_at, :], dos[h])
            ds = (probs * (dp - inner[h])).astype(BF)
            dv[h, keys_at, :] += dot(probs.astype(BF), dos[h])
            dk[h, keys_at, :] += dot(ds, qs[h])
            dqt[h] += dot(kt_scr[h * HEAD_DIM : (h + 1) * HEAD_DIM, keys_at], ds)

    full = size // kb

    def step(i, carry):
        chunk(i, False)
        return carry

    lax.fori_loop(0, full, step, 0)

    @pl.when(full * kb < size)
    def _():
        chunk(full, True)

    dq = jnp.concatenate([dqt[h] for h in range(hh)], axis=0).T * scale
    dx_ref[0, rows, 0:w] = dq.astype(BF)

    @pl.when(qi == pl.num_programs(1) - 1)
    def _():
        for h in range(hh):
            dx_ref[0, :, w + h * HEAD_DIM : w + (h + 1) * HEAD_DIM] = (dk[h] * scale).astype(BF)
            dx_ref[0, :, 2 * w + h * HEAD_DIM : 2 * w + (h + 1) * HEAD_DIM] = dv[h].astype(BF)


def attend_back(sources, plan, index, x, o, lse, lens, hh):
    problems, length, w3 = x.shape
    w = hh * HEAD_DIM
    qb = math.gcd(length, 512)
    kb = math.gcd(length, 512)
    return pl.pallas_call(
        functools.partial(attend_back_kernel, hh, length, qb, kb, len(sources)),
        out_shape=jax.ShapeDtypeStruct((problems, length, lanes_of(w3)), BF),
        grid_spec=pltpu.PrefetchScalarGridSpec(
            num_scalar_prefetch=3,
            grid=(problems, length // qb),
            in_specs=source_specs(sources, problems)
            + [
                pl.BlockSpec((1, length, w3), lambda p, q, *_: (p, 0, 0)),
                pl.BlockSpec((1, qb, lanes_of(w)), lambda p, q, *_: (p, q, 0)),
                pl.BlockSpec((1, hh, qb), lambda p, q, *_: (p, 0, q)),
            ],
            out_specs=pl.BlockSpec((1, length, lanes_of(w3)), lambda p, q, *_: (p, 0, 0)),
            scratch_shapes=[
                pltpu.VMEM((1, length, w), BF),
                pltpu.VMEM((hh, length, HEAD_DIM), BF),
                pltpu.VMEM((hh, length, HEAD_DIM), BF),
                pltpu.VMEM((w, length), BF),
                pltpu.VMEM((hh, length, HEAD_DIM), F32),
                pltpu.VMEM((hh, length, HEAD_DIM), F32),
                pltpu.VMEM((hh, HEAD_DIM, qb), F32),
            ],
        ),
        compiler_params=params(2),
        cost_estimate=cost(
            problems * hh * 10 * length * length * 256, x.size * 6, problems * hh * length * length
        ),
        name="attend_back",
    )(lens, plan, index, *sources, x, o, lse)


def project_kernel(
    tm, width, group, per, sets, scales, order, x_ref, gain, shift, w_ref, bias, down, up, *outs
):
    normed_ref, ranks_ref, away_ref, mine_ref, n_scr, r_scr = outs
    c = pl.program_id(0)
    m = pl.program_id(1)
    rows = pl.ds(pl.multiple_of(m * tm, tm), tm)
    wide = group * w_ref.shape[0]

    @pl.when(c == 0)
    def _():
        unit, _ = norm_parts(x_ref[...].astype(F32))
        normed = (unit * gain[...] + shift[...]).astype(BF)
        n_scr[rows, :] = normed
        normed_ref[...] = normed
        rank = dot(normed, down[...]) * scales[m]
        keep = set_mask(rank.shape, sets[m], group, per)
        rank = jnp.where(keep, rank, 0.0).astype(BF)
        r_scr[rows, :] = rank
        ranks_ref[...] = rank

    y = dot(n_scr[rows, :], w_ref[:, 0].reshape(D, 4 * width)[:, 0 : 3 * width]) + bias[0]
    table = up[:, 0].reshape(wide, 4 * width)
    rank = r_scr[rows, :]
    extra = [
        dot(rank[:, j * wide : (j + 1) * wide], table[:, j * width : (j + 1) * width]) for j in range(3)
    ]
    y = (y + jnp.concatenate(extra, axis=1)).astype(BF)
    half = pl.num_programs(0) // 2

    @pl.when(c < half)
    def _():
        away_ref[0, :, 0 : 3 * width] = y

    @pl.when(c >= half)
    def _():
        mine_ref[0, :, 0 : 3 * width] = y


def project(tokens, gain, shift, gathered, bias, tables, sets, scales, order, tm, per):
    own = tokens.shape[0]
    rr, nc, _, w4 = gathered.shape
    width = w4 // 4
    w3 = 3 * width
    group = SETS * per
    wide = group * rr
    nm = own // tm
    half = nc // 2
    first = lambda c, m, *_: (jnp.where(c == 0, m, nm - 1), 0)
    flat = lambda c, m, *_: (0, 0)
    return pl.pallas_call(
        functools.partial(project_kernel, tm, width, group, per),
        out_shape=(
            jax.ShapeDtypeStruct((own, D), BF),
            jax.ShapeDtypeStruct((own, 3 * wide), BF),
            jax.ShapeDtypeStruct((half, own, lanes_of(w3)), BF),
            jax.ShapeDtypeStruct((half, own, lanes_of(w3)), BF),
        ),
        grid_spec=pltpu.PrefetchScalarGridSpec(
            num_scalar_prefetch=3,
            grid=(nc, nm),
            in_specs=[
                pl.BlockSpec((tm, D), first),
                pl.BlockSpec((1, D), flat),
                pl.BlockSpec((1, D), flat),
                pl.BlockSpec((rr, 1, D // rr, w4), lambda c, m, s, a, o: (0, o[c], 0, 0)),
                pl.BlockSpec((1, 1, w3), lambda c, m, s, a, o: (o[c], 0, 0)),
                pl.BlockSpec((D, 3 * wide), flat),
                pl.BlockSpec(
                    (rr, 1, group, w4), lambda c, m, s, a, o: (0, o[c], D // rr // group, 0)
                ),
            ],
            out_specs=[
                pl.BlockSpec((tm, D), first),
                pl.BlockSpec((tm, 3 * wide), first),
                pl.BlockSpec(
                    (1, tm, lanes_of(w3)),
                    lambda c, m, *_: (jnp.minimum(c, half - 1), jnp.where(c < half, m, nm - 1), 0),
                ),
                pl.BlockSpec(
                    (1, tm, lanes_of(w3)),
                    lambda c, m, *_: (jnp.maximum(c - half, 0), jnp.where(c < half, 0, m), 0),
                ),
            ],
            scratch_shapes=[pltpu.VMEM((own, D), BF), pltpu.VMEM((own, 3 * wide), BF)],
        ),
        compiler_params=params(2),
        cost_estimate=cost(2 * own * D * nc * w3 * 1.3, D * nc * w3 * 2 + own * (2 * D + nc * w3) * 2),
        name="project",
    )(sets, scales, order, tokens, gain, shift, gathered, bias, tables, gathered)


def piece_specs(sources, tm, at):
    def spec(j, v):
        def where_from(*ids):
            code = ids[-1]
            i = at(*ids[:-1])
            hit = code[3 * i] == j
            return (jnp.where(hit, code[3 * i + 1], 0), jnp.where(hit, code[3 * i + 2], 0), 0)

        return pl.BlockSpec((1, tm, v.shape[-1]), where_from)

    return [spec(j, v) for j, v in enumerate(sources)]


def lane_tiles(v, group):
    n = v.shape[1]
    pad = -n % 128
    if pad:
        v = jnp.concatenate([v, jnp.zeros((v.shape[0], pad), v.dtype)], axis=1)
    return [
        v[:, t * 128 : (t + 1) * 128].reshape(-1, group, 128) for t in range((n + pad) // 128)
    ]


def put_tiles(ref, first, v, group):
    for t, tile in enumerate(lane_tiles(v, group)):
        at = (first + t) * group
        ref[:, 0, at : at + group, :] = tile.astype(BF)


def fold_sets(turned, group, per):
    wide = turned.shape[0]
    row = lax.broadcasted_iota(jnp.int32, (RANK, wide), 0)
    column = lax.broadcasted_iota(jnp.int32, (RANK, wide), 1)
    match = (column // group == row // per) & (column % per == row % per)
    return dot(jnp.where(match, 1.0, 0.0).astype(BF), turned).astype(BF)


def adapt_back_kernel(tm, width, group, per, ns, nm, sets, scales, slots, code, *refs):
    sources = refs[:ns]
    up, normed_ref, ranks_ref, dy_ref, grank_ref, gup_ref, gdown_ref, racc, gup, gdown = refs[ns:]
    slot = slots[pl.program_id(1)]
    c = pl.program_id(0)
    m = pl.program_id(1)
    last = c == pl.num_programs(0) - 1
    rows = pl.ds(pl.multiple_of(m * tm, tm), tm)
    wide = group * up.shape[0]
    choose(code[3 * (c * nm + m)], sources, dy_ref, 0)
    dy = dy_ref[0]
    table = up[:, 0].reshape(wide, 4 * width)
    pieces = [dy[:, j * width : (j + 1) * width] for j in range(3)]
    rpart = jnp.concatenate(
        [dot_t(pieces[j], table[:, j * width : (j + 1) * width]) for j in range(3)], axis=1
    )

    @pl.when(c == 0)
    def _():
        racc[rows, :] = rpart

    @pl.when(c > 0)
    def _():
        racc[rows, :] += rpart

    turned = ranks_ref[...].T

    @pl.when(m == 0)
    def _():
        gup[...] = jnp.zeros_like(gup)

    for j in range(3):
        gup[slot, j] += dot(fold_sets(turned[j * wide : (j + 1) * wide], group, per), pieces[j])

    @pl.when(m == nm - 1)
    def _():
        tiles = -(-width // 128)
        clips = gup.shape[0]
        for i in range(clips):
            for j in range(3):
                for t, tile in enumerate(lane_tiles(gup[i, j], RANK)):
                    gup_ref[0, (i * 3 + j) * tiles + t] = tile[0].astype(BF)

    @pl.when(last)
    def _():
        grank = racc[rows, :] * scales[m]
        grank = jnp.where(set_mask(grank.shape, sets[m], group, per), grank, 0.0)
        grank_ref[...] = grank.astype(BF)
        turned = grank.T.astype(BF)

        @pl.when(m == 0)
        def _():
            gdown[...] = jnp.zeros_like(gdown)

        for j in range(3):
            part = dot(fold_sets(turned[j * wide : (j + 1) * wide], group, per), normed_ref[...])
            gdown[slot, j * RANK : (j + 1) * RANK] += part

        @pl.when(m == nm - 1)
        def _():
            whole = gdown[...].reshape(-1, D)
            pad = gdown_ref.shape[0] * 128 - whole.shape[0]
            whole = jnp.concatenate([whole, jnp.zeros((pad, D), F32)], axis=0)
            for i in range(gdown_ref.shape[0]):
                gdown_ref[i] = whole[i * 128 : (i + 1) * 128].T.astype(BF)


def adapt_back(sources, code, gathered, normed, ranks, sets, scales, slots, clips, tm, per):
    own = normed.shape[0]
    rr, nc, _, w4 = gathered.shape
    width = w4 // 4
    w3 = 3 * width
    group = SETS * per
    wide = group * rr
    nm = own // tm
    tiles = 3 * -(-width // 128)
    folded = -(-clips * 3 * RANK // 128)
    final = lambda c, m, *_: (jnp.where(c == nc - 1, m, 0), 0)
    return pl.pallas_call(
        functools.partial(adapt_back_kernel, tm, width, group, per, len(sources), nm),
        out_shape=(
            jax.ShapeDtypeStruct((nc, own, w3), BF),
            jax.ShapeDtypeStruct((own, 3 * wide), BF),
            jax.ShapeDtypeStruct((nc, clips * tiles, RANK, 128), BF),
            jax.ShapeDtypeStruct((folded, D, 128), BF),
        ),
        grid_spec=pltpu.PrefetchScalarGridSpec(
            num_scalar_prefetch=4,
            grid=(nc, nm),
            in_specs=piece_specs(sources, tm, lambda c, m, s, a, i: c * nm + m)
            + [
                pl.BlockSpec((rr, 1, group, w4), lambda c, m, *_: (0, c, D // rr // group, 0)),
                pl.BlockSpec((tm, D), final),
                pl.BlockSpec((tm, 3 * wide), lambda c, m, *_: (m, 0)),
            ],
            out_specs=[
                pl.BlockSpec((1, tm, w3), lambda c, m, *_: (c, m, 0)),
                pl.BlockSpec((tm, 3 * wide), final),
                pl.BlockSpec((1, clips * tiles, RANK, 128), lambda c, m, *_: (c, 0, 0, 0)),
                pl.BlockSpec((folded, D, 128), lambda c, m, *_: (0, 0, 0)),
            ],
            scratch_shapes=[
                pltpu.VMEM((own, 3 * wide), F32),
                pltpu.VMEM((clips, 3, RANK, width), F32),
                pltpu.VMEM((clips, 3 * RANK, D), F32),
            ],
        ),
        compiler_params=params(2),
        cost_estimate=cost(own * D * nc * w3 * 0.6, own * nc * w3 * 4),
        name="adapt_back",
    )(sets, scales, slots, code, *sources, gathered, normed, ranks)


def project_back_kernel(tm, width, dy_ref, w_ref, grank_ref, down, x_ref, gm_ref, gain, gt_ref, acc):
    c = pl.program_id(0)
    m = pl.program_id(1)
    rows = pl.ds(pl.multiple_of(m * tm, tm), tm)
    part = dot_t(dy_ref[0], w_ref[:, 0].reshape(D, 4 * width)[:, 0 : 3 * width])

    @pl.when(c == 0)
    def _():
        acc[rows, :] = part + dot_t(grank_ref[...], down[...])

    @pl.when(c > 0)
    def _():
        acc[rows, :] += part

    @pl.when(c == pl.num_programs(0) - 1)
    def _():
        unit, inverse = norm_parts(x_ref[...].astype(F32))
        e = acc[rows, :] * gain[...]
        mean = jnp.mean(e, axis=-1, keepdims=True)
        second = jnp.mean(e * unit, axis=-1, keepdims=True)
        gt_ref[...] = (gm_ref[...] + (e - mean - unit * second) * inverse).astype(BF)


def project_back(dy, gathered, grank, tables, tokens, grad_middle, gain, tm):
    own = tokens.shape[0]
    rr, nc, _, w4 = gathered.shape
    width = w4 // 4
    w3 = 3 * width
    wide3 = grank.shape[1]
    nm = own // tm
    final = lambda c, m: (jnp.where(c == nc - 1, m, 0), 0)
    return pl.pallas_call(
        functools.partial(project_back_kernel, tm, width),
        out_shape=jax.ShapeDtypeStruct((own, D), BF),
        grid=(nc, nm),
        in_specs=[
            pl.BlockSpec((1, tm, w3), lambda c, m: (c, m, 0)),
            pl.BlockSpec((rr, 1, D // rr, w4), lambda c, m: (0, c, 0, 0)),
            pl.BlockSpec((tm, wide3), lambda c, m: (jnp.where(c == 0, m, nm - 1), 0)),
            pl.BlockSpec((D, wide3), lambda c, m: (0, 0)),
            pl.BlockSpec((tm, D), final),
            pl.BlockSpec((tm, D), final),
            pl.BlockSpec((1, D), lambda c, m: (0, 0)),
        ],
        out_specs=pl.BlockSpec((tm, D), final),
        scratch_shapes=[pltpu.VMEM((own, D), F32)],
        compiler_params=params(2),
        cost_estimate=cost(2 * own * D * nc * w3 * 1.1, D * nc * w3 * 2 + own * (4 * D + nc * w3) * 2),
        name="project_back",
    )(dy, gathered, grank, tables, tokens, grad_middle, gain)


def collect_kernel(nc, nm, ns, code, *refs):
    sources = refs[:ns]
    att_ref, a_scr = refs[ns:]
    m = pl.program_id(0)
    c = pl.program_id(1)
    choose(code[3 * (c * nm + m)], sources, a_scr, c)

    @pl.when(c == nc - 1)
    def _():
        att_ref[...] = jnp.concatenate([a_scr[i] for i in range(nc)], axis=1)


def collect(sources, code, own, tm, nc):
    nm = own // tm
    return pl.pallas_call(
        functools.partial(collect_kernel, nc, nm, len(sources)),
        out_shape=jax.ShapeDtypeStruct((own, D), BF),
        grid_spec=pltpu.PrefetchScalarGridSpec(
            num_scalar_prefetch=1,
            grid=(nm, nc),
            in_specs=piece_specs(sources, tm, lambda m, c: c * nm + m),
            out_specs=pl.BlockSpec((tm, D), lambda m, c, *_: (m, 0)),
            scratch_shapes=[pltpu.VMEM((nc, tm, D // nc), BF)],
        ),
        compiler_params=params(2),
        cost_estimate=cost(own * D, own * D * 10),
        name="collect",
    )(code, *sources)


def out_kernel(group, per, sets, scales, *refs):
    att_ref, x_ref, w_ref, bias, odown, oup, gain, shift, fdown = refs[:9]
    middle_ref, normed_ref, ro_ref, r1_ref = refs[9:]
    m = pl.program_id(0)
    att = att_ref[...]
    ro = dot_t(att, odown[...]) * scales[m]
    keep = set_mask(ro.shape, sets[m], group, per)
    ro = jnp.where(keep, ro, 0.0).astype(BF)
    ro_ref[...] = ro
    middle = x_ref[...].astype(F32) + dot_t(att, w_ref[...]) + dot_t(ro, oup[...]) + bias[...]
    middle_ref[...] = middle
    unit, _ = norm_parts(middle)
    normed = (unit * gain[...] + shift[...]).astype(BF)
    normed_ref[...] = normed
    r1_ref[...] = jnp.where(keep, dot(normed, fdown[...]) * scales[m], 0.0).astype(BF)


def out_project(att, tokens, wo_t, bias, odown, tables, gain, shift, sets, scales, tm, per):
    own = tokens.shape[0]
    wide = odown.shape[0]
    row = lambda m, *_: (m, 0)
    flat = lambda m, *_: (0, 0)
    return pl.pallas_call(
        functools.partial(out_kernel, SETS * per, per),
        out_shape=(
            jax.ShapeDtypeStruct((own, D), F32),
            jax.ShapeDtypeStruct((own, D), BF),
            jax.ShapeDtypeStruct((own, wide), BF),
            jax.ShapeDtypeStruct((own, wide), BF),
        ),
        grid_spec=pltpu.PrefetchScalarGridSpec(
            num_scalar_prefetch=2,
            grid=(own // tm,),
            in_specs=[
                pl.BlockSpec((tm, D), row),
                pl.BlockSpec((tm, D), row),
                pl.BlockSpec((D, D), flat),
                pl.BlockSpec((1, D), flat),
                pl.BlockSpec((wide, D), flat),
                pl.BlockSpec((D, wide), lambda m, *_: (0, 4)),
                pl.BlockSpec((1, D), flat),
                pl.BlockSpec((1, D), flat),
                pl.BlockSpec((D, wide), lambda m, *_: (0, 3)),
            ],
            out_specs=[
                pl.BlockSpec((tm, D), row),
                pl.BlockSpec((tm, D), row),
                pl.BlockSpec((tm, wide), row),
                pl.BlockSpec((tm, wide), row),
            ],
        ),
        compiler_params=params(1),
        cost_estimate=cost(2 * own * D * D * 1.5, D * D * 2 + own * D * 12),
        name="out_project",
    )(sets, scales, att, tokens, wo_t, bias, odown, tables, gain, shift, tables)


def out_back_kernel(nc, width, group, per, sets, scales, side, gb_ref, w_ref, oup, odown, att_ref, ro_ref, *outs):
    away_ref, mine_ref, gup_ref, gdown_ref, gup, gdown = outs
    m = pl.program_id(0)

    @pl.when(m == 0)
    def _():
        gup[...] = jnp.zeros_like(gup)
        gdown[...] = jnp.zeros_like(gdown)

    gb = gb_ref[...]
    gro = dot(gb, oup[...]) * scales[m]
    gro = jnp.where(set_mask(gro.shape, sets[m], group, per), gro, 0.0)
    ga = (dot(gb, w_ref[...]) + dot(gro.astype(BF), odown[...])).astype(BF)
    half = nc // 2
    for i in range(nc):
        piece = ga[:, i * width : (i + 1) * width]

        @pl.when(side[0] == i // half)
        def _(i=i, piece=piece):
            mine_ref[i % half, :, 0:width] = piece

        @pl.when(side[0] != i // half)
        def _(i=i, piece=piece):
            away_ref[i % half, :, 0:width] = piece

    gup[...] += dot(ro_ref[...].T, gb)
    gdown[...] += token_sum(gro, att_ref[...])

    @pl.when(m == pl.num_programs(0) - 1)
    def _():
        gup_ref[...] = gup[...].T.astype(BF)
        whole = gdown[...]
        for i in range(nc):
            for t, tile in enumerate(lane_tiles(whole[:, i * width : (i + 1) * width], group)):
                gdown_ref[:, i, t * group : (t + 1) * group, :] = tile.astype(BF)


def out_back(gb, wo_t, tables, odown, att, ro, sets, scales, side, tm, nc, per, rr):
    own = gb.shape[0]
    width = D // nc
    group = SETS * per
    wide = group * rr
    half = nc // 2
    tiles = -(-width // 128)
    row = lambda m, *_: (m, 0)
    flat = lambda m, *_: (0, 0)
    return pl.pallas_call(
        functools.partial(out_back_kernel, nc, width, group, per),
        out_shape=(
            jax.ShapeDtypeStruct((half, own, lanes_of(width)), BF),
            jax.ShapeDtypeStruct((half, own, lanes_of(width)), BF),
            jax.ShapeDtypeStruct((D, wide), BF),
            jax.ShapeDtypeStruct((rr, nc, tiles * group, 128), BF),
        ),
        grid_spec=pltpu.PrefetchScalarGridSpec(
            num_scalar_prefetch=3,
            grid=(own // tm,),
            in_specs=[
                pl.BlockSpec((tm, D), row),
                pl.BlockSpec((D, D), flat),
                pl.BlockSpec((D, wide), lambda m, *_: (0, 4)),
                pl.BlockSpec((wide, D), flat),
                pl.BlockSpec((tm, D), row),
                pl.BlockSpec((tm, wide), row),
            ],
            out_specs=[
                pl.BlockSpec((half, tm, lanes_of(width)), lambda m, *_: (0, m, 0)),
                pl.BlockSpec((half, tm, lanes_of(width)), lambda m, *_: (0, m, 0)),
                pl.BlockSpec((D, wide), flat),
                pl.BlockSpec((rr, nc, tiles * group, 128), lambda m, *_: (0, 0, 0, 0)),
            ],
            scratch_shapes=[pltpu.VMEM((wide, D), F32), pltpu.VMEM((wide, D), F32)],
        ),
        compiler_params=params(1),
        cost_estimate=cost(2 * own * D * D * 1.5, D * D * 2 + own * D * 6),
        name="out_back",
    )(sets, scales, side, gb, wo_t, tables, odown, att, ro)


def mlp_kernel(tm, nm, group, per, sets, scales, *refs):
    n_ref, g_ref, mid_ref, w1_ref, w2_ref, b1, up1_ref, down2_ref, up2, down1, r1_ref, bias2, gain = refs[:13]
    out_ref, gm_ref, gb_ref, gup1_ref, gdown2_ref, gup2_ref, gdown1_ref = refs[13:20]
    acc, gacc, r2acc, gr1acc, gr2, gup1, gdown2, gup2, gdown1 = refs[20:]
    c = pl.program_id(0)
    m = pl.program_id(1)
    rows = pl.ds(pl.multiple_of(m * tm, tm), tm)
    a = scales[m]
    g = g_ref[...]
    normed = n_ref[...]
    hidden = w1_ref.shape[-1]
    wide = r1_ref.shape[1]
    keep = set_mask((tm, wide), sets[m], group, per)

    @pl.when(c == 0)
    def _():
        gr2[rows, :] = jnp.where(keep, dot(g, up2[...]) * a, 0.0).astype(BF)
        acc[rows, :] = jnp.zeros((tm, D), F32)
        gacc[rows, :] = jnp.zeros((tm, D), F32)
        r2acc[rows, :] = jnp.zeros((tm, wide), F32)
        gr1acc[rows, :] = jnp.zeros((tm, wide), F32)

    @pl.when(m == 0)
    def _():
        gup1[...] = jnp.zeros_like(gup1)
        gdown2[...] = jnp.zeros_like(gdown2)

    @pl.when((m == 0) & (c == 0))
    def _():
        gup2[...] = jnp.zeros_like(gup2)
        gdown1[...] = jnp.zeros_like(gdown1)

    w1 = w1_ref[:, 0].reshape(D, hidden)
    w2 = w2_ref[:, 0].reshape(D, hidden)
    up1 = up1_ref[:, 0].reshape(wide, hidden)
    down2 = down2_ref[:, 0].reshape(wide, hidden)
    r1 = r1_ref[...]
    grank2 = gr2[rows, :]
    pre = dot(normed, w1) + dot(r1, up1) + b1[0]
    upper = 0.5 + 0.5 * lax.erf(pre * (0.5**0.5))
    density = jnp.exp(pre * pre * -0.5) * ((2.0 * math.pi) ** -0.5)
    act = (pre * upper).astype(BF)
    slope = upper + pre * density
    gact = dot(g, w2) + dot(grank2, down2)
    gpre = (gact * slope).astype(BF)
    acc[rows, :] += dot_t(act, w2)
    r2acc[rows, :] += dot_t(act, down2)
    gacc[rows, :] += dot_t(gpre, w1)
    gr1acc[rows, :] += dot_t(gpre, up1)
    gdown2[...] += dot(grank2.T, act)
    gup1[...] += dot(r1.T, gpre)

    @pl.when(m == nm - 1)
    def _():
        put_tiles(gup1_ref, 0, gup1[...], group)
        put_tiles(gdown2_ref, 0, gdown2[...], group)

    @pl.when(c == pl.num_programs(0) - 1)
    def _():
        r2 = jnp.where(keep, r2acc[rows, :] * a, 0.0).astype(BF)
        middle = mid_ref[...]
        out_ref[...] = (middle + acc[rows, :] + dot_t(r2, up2[...]) + bias2[...]).astype(BF)
        gup2[...] += dot(r2.T, g)
        gr1 = jnp.where(keep, gr1acc[rows, :] * a, 0.0).astype(BF)
        e = (gacc[rows, :] + dot_t(gr1, down1[...])) * gain[...]
        gdown1[...] += dot(gr1.T, normed)
        unit, inverse = norm_parts(middle)
        mean = jnp.mean(e, axis=-1, keepdims=True)
        second = jnp.mean(e * unit, axis=-1, keepdims=True)
        gm = g.astype(F32) + (e - mean - unit * second) * inverse
        gm_ref[...] = gm
        gb_ref[...] = gm.astype(BF)

        @pl.when(m == nm - 1)
        def _():
            gup2_ref[...] = gup2[...].T.astype(BF)
            gdown1_ref[...] = gdown1[...].T.astype(BF)


def mlp(normed, g, middle, gathered, b1, tables, r1, bias2, gain, sets, scales, tm, per, at):
    own = g.shape[0]
    rr, nc, _, hidden = gathered.shape
    group = SETS * per
    wide = group * rr
    nm = own // tm
    tiles = -(-hidden // 128)
    row = lambda c, m, *_: (m, 0)
    final = lambda c, m, *_: (jnp.where(c == nc - 1, m, 0), 0)
    flat = lambda c, m, *_: (0, 0)
    wblock = (rr, 1, D // rr, hidden)
    return pl.pallas_call(
        functools.partial(mlp_kernel, tm, nm, group, per),
        out_shape=(
            jax.ShapeDtypeStruct((own, D), BF),
            jax.ShapeDtypeStruct((own, D), F32),
            jax.ShapeDtypeStruct((own, D), BF),
            jax.ShapeDtypeStruct((rr, nc, tiles * group, 128), BF),
            jax.ShapeDtypeStruct((rr, nc, tiles * group, 128), BF),
            jax.ShapeDtypeStruct((D, wide), BF),
            jax.ShapeDtypeStruct((D, wide), BF),
        ),
        grid_spec=pltpu.PrefetchScalarGridSpec(
            num_scalar_prefetch=2,
            grid=(nc, nm),
            in_specs=[
                pl.BlockSpec((tm, D), row),
                pl.BlockSpec((tm, D), row),
                pl.BlockSpec((tm, D), final, pipeline_mode=pl.Buffered(1)),
                pl.BlockSpec(wblock, lambda c, m, *_: (0, c, 0, 0)),
                pl.BlockSpec(wblock, lambda c, m, *_: (0, c, 1, 0)),
                pl.BlockSpec((1, 1, hidden), lambda c, m, *_: (c, 0, 0)),
                pl.BlockSpec((rr, 1, group, hidden), lambda c, m, *_: (0, c, at // group, 0)),
                pl.BlockSpec((rr, 1, group, hidden), lambda c, m, *_: (0, c, at // group + 1, 0)),
                pl.BlockSpec((D, wide), lambda c, m, *_: (0, 5), pipeline_mode=pl.Buffered(1)),
                pl.BlockSpec((D, wide), lambda c, m, *_: (0, 3), pipeline_mode=pl.Buffered(1)),
                pl.BlockSpec((tm, wide), row),
                pl.BlockSpec((1, D), flat),
                pl.BlockSpec((1, D), flat),
            ],
            out_specs=[
                pl.BlockSpec((tm, D), final),
                pl.BlockSpec((tm, D), final),
                pl.BlockSpec((tm, D), final),
                pl.BlockSpec((rr, 1, tiles * group, 128), lambda c, m, *_: (0, c, 0, 0)),
                pl.BlockSpec((rr, 1, tiles * group, 128), lambda c, m, *_: (0, c, 0, 0)),
                pl.BlockSpec((D, wide), flat),
                pl.BlockSpec((D, wide), flat),
            ],
            scratch_shapes=[
                pltpu.VMEM((own, D), F32),
                pltpu.VMEM((own, D), F32),
                pltpu.VMEM((own, wide), F32),
                pltpu.VMEM((own, wide), F32),
                pltpu.VMEM((own, wide), BF),
                pltpu.VMEM((wide, hidden), F32),
                pltpu.VMEM((wide, hidden), F32),
                pltpu.VMEM((wide, D), F32),
                pltpu.VMEM((wide, D), F32),
            ],
        ),
        compiler_params=params(2, 67043328),
        cost_estimate=cost(8 * own * D * nc * hidden * 1.2, D * nc * hidden * 4 + own * D * 30, own * nc * hidden * 2),
        name="mlp",
    )(
        sets, scales, normed, g, middle, gathered, gathered, b1, gathered, gathered, tables, tables, r1, bias2, gain
    )


def assemble_kernel(width, w_ref, o_ref, w_out, o_out):
    nc = w_ref.shape[1]
    columns = [w_ref[:, c].reshape(D, 2 * width)[:, width:] for c in range(nc)]
    downs = [o_ref[:, c].reshape(-1, 2 * width)[:, width:] for c in range(nc)]
    w_out[...] = jnp.concatenate(columns, axis=1)
    o_out[...] = jnp.concatenate(downs, axis=1)


def assemble(gathered, group):
    nr, nc, _, w4 = gathered.shape
    width = w4 // 4
    rows = D // nr
    if 2 * width % 128 == 0:
        return pl.pallas_call(
            functools.partial(assemble_kernel, width),
            out_shape=(
                jax.ShapeDtypeStruct((D, D), BF),
                jax.ShapeDtypeStruct((nr * group, D), BF),
            ),
            grid=(1,),
            in_specs=[
                pl.BlockSpec((nr, nc, rows, 2 * width), lambda i: (0, 0, 0, 1)),
                pl.BlockSpec((nr, nc, group, 2 * width), lambda i: (0, 0, rows // group, 1)),
            ],
            out_specs=[
                pl.BlockSpec((D, D), lambda i: (0, 0)),
                pl.BlockSpec((nr * group, D), lambda i: (0, 0)),
            ],
            compiler_params=params(1),
            name="assemble",
        )(gathered, gathered)
    w = gathered[:, :, :rows, 3 * width :]
    o = gathered[:, :, rows : rows + group, 3 * width :]
    return (
        w.transpose(0, 2, 1, 3).reshape(D, D),
        o.transpose(0, 2, 1, 3).reshape(nr * group, D),
    )


def pick(flag, first, second):
    return jnp.where(flag, first, second)


def table_of(values):
    return jnp.stack([jnp.asarray(v, jnp.int32) for v in values])


class Exchange:
    def __init__(self, nc, own, clips, clip_len, tm):
        self.nc, self.own, self.clips, self.clip_len, self.tm = nc, own, clips, clip_len, tm
        self.local = nc == 4 and clips == 3 and own == 3 * tm and clip_len == 4 * tm
        col = lax.axis_index("cols")
        self.nm = nm = own // tm
        if not self.local:
            self.order = jnp.arange(nc, dtype=jnp.int32)
            self.side = jnp.ones((1,), jnp.int32)
            self.plans = [jnp.zeros((2,), jnp.int32)]
            self.indices = [jnp.arange(clips, dtype=jnp.int32)]
            entry = jnp.arange(nc * nm, dtype=jnp.int32)
            self.code = jnp.stack([entry * 0, entry // nm, entry % nm], axis=1).reshape(-1)
            return
        y, k = col // 2, col % 2
        self.y, self.k = y, k
        self.holder = y != k
        self.order = (jnp.arange(4, dtype=jnp.int32) + 2 * (1 - k)) % 4
        self.side = k[None]
        b = jnp.arange(4, dtype=jnp.int32)
        g = b + 2 * y
        clip_plan = jnp.concatenate([pick(g // 3 == k, 0, 1), g % 3])
        g = pick(y == 0, 4 + b, b - 2)
        near = b // 2 == y
        source = pick(near, pick(g // 3 == k, 0, 1), pick(self.holder, 3, 2))
        shared_plan = jnp.concatenate([source, pick(near, g % 3, b % 2)])
        self.plans = [clip_plan.astype(jnp.int32), shared_plan.astype(jnp.int32)]
        self.indices = [jnp.array([0, 1, 0, 1], jnp.int32), table_of([y, y, 0, 0])]
        entry = jnp.arange(12, dtype=jnp.int32)
        c, m = entry // 3, entry % 3
        g = 3 * k + m
        inside = (g >= 2 * y) & (g < 2 * y + 4)
        same, idx = c // 2 == k, c % 2
        source = pick(
            inside,
            pick(same, 0, 2),
            pick(idx == y, pick(same, 1, 3), pick(same, 4, 5)),
        )
        block = pick(
            inside,
            g - 2 * y,
            pick(y == 0, g - 4, pick(idx == y, g + 2, g)),
        )
        self.code = (
            jnp.stack([source, pick(inside, idx, 0), block], axis=1).astype(jnp.int32).reshape(-1)
        )

    def lens(self, lengths):
        if not self.local:
            return (lengths,)
        mine = pick(self.y == 0, lengths[0], lengths[2])
        return (jnp.stack([mine, mine]), lengths[1:2])

    def to_heads(self, away, mine):
        f = mine.shape[-1]
        if not self.local:
            moved = lax.all_to_all(jnp.concatenate([away, mine]), "cols", 0, 0, tiled=True)
            return [[moved.reshape(self.clips, self.clip_len, f)]]
        y, k, half = self.y, self.k, self.clip_len // 2
        start = pick(k == 1, self.own - half, 0)
        got = lax.ppermute(away, "cols", [(i, i ^ 1) for i in range(4)])
        one = lax.dynamic_slice(mine, (1 - y, start, 0), (1, half, f))
        two = lax.dynamic_slice(away, (1 - y, start, 0), (1, half, f))
        got_one = lax.ppermute(one, "cols", [(1, 3), (2, 0)])
        got_two = lax.ppermute(two, "cols", [(1, 2), (2, 1)])
        return [[mine, got], [mine, got, got_one, got_two]]

    def from_heads(self, parts):
        if not self.local:
            (v,) = parts
            v = v.reshape(self.nc, self.own, v.shape[-1])
            return [lax.all_to_all(v, "cols", 0, 0, tiled=True)]
        clip, shared = parts
        half = self.clip_len // 2
        far = lax.dynamic_slice(shared, (0, (1 - self.y) * half, 0), (1, half, clip.shape[-1]))
        swap = [(i, i ^ 1) for i in range(4)]
        got_one = lax.ppermute(far, "cols", [(3, 1), (0, 2)])
        got_two = lax.ppermute(far, "cols", [(2, 1), (1, 2)])
        got_shared = lax.ppermute(shared, "cols", swap)
        return [clip, shared, lax.ppermute(clip, "cols", swap), got_shared, got_one, got_two]


def up_to(n, k):
    return -(-n // k) * k


def rows_padded(v, rows, lanes):
    return jnp.pad(v.astype(BF), ((0, rows - v.shape[0]), (0, lanes - v.shape[1])))


def halves(v):
    high = v.astype(BF)
    return high, (v - high.astype(F32)).astype(BF)


def scatter_sum(pieces):
    whole = jnp.concatenate(pieces, axis=2)
    n = whole.shape[2]
    whole = jnp.pad(whole, ((0, 0), (0, 0), (0, up_to(n, 8) - n), (0, 0)))
    return whole.reshape(-1, 128)


def body(
    tokens,
    cotangent,
    clip_lengths,
    clip_sets,
    clip_scales,
    norm1_gain,
    norm1_shift,
    w_query,
    query_bias,
    w_key,
    w_value,
    value_bias,
    w_out,
    out_bias,
    norm2_gain,
    norm2_shift,
    w_fc1,
    fc1_bias,
    w_fc2,
    fc2_bias,
    query_down,
    query_up,
    key_down,
    key_up,
    value_down,
    value_up,
    out_down,
    out_up,
    fc1_down,
    fc1_up,
    fc2_down,
    fc2_up,
):
    nr = lax.axis_size("rows")
    nc = lax.axis_size("cols")
    col = lax.axis_index("cols")
    clips = clip_lengths.shape[0]
    own = tokens.shape[0]
    clip_len = own * nc // clips
    tm = math.gcd(own, clip_len)
    width = query_bias.shape[0]
    hidden = fc1_bias.shape[0]
    hh = width // HEAD_DIM
    dr = w_query.shape[0]
    per = RANK // nr
    group = SETS * per
    wide = group * nr
    dc = dr // nc
    exchange = Exchange(nc, own, clips, clip_len, tm)

    block_clip = (col * own + jnp.arange(own // tm, dtype=jnp.int32) * tm) // clip_len
    sets = jnp.take(clip_sets, block_clip)
    scales = jnp.take(clip_scales, block_clip)

    downs = jnp.stack([query_down, key_down, value_down, fc1_down])
    downs = lax.dynamic_slice(downs, (0, 0, col * dc, 0), (4, SETS, dc, RANK))
    downs = downs.reshape(4, SETS, dc, nr, per).transpose(2, 0, 3, 1, 4).reshape(dc, 4 * wide)
    ups = jnp.stack([out_up, fc2_up])
    ups = lax.dynamic_slice(ups, (0, 0, 0, col * dc), (2, SETS, RANK, dc))
    ups = ups.reshape(2, SETS, nr, per, dc).transpose(4, 0, 2, 1, 3).reshape(dc, 2 * wide)
    tables = jnp.concatenate([downs, ups], axis=1)

    lanes = 4 * width
    turn = lambda v: jnp.swapaxes(v, 1, 2).reshape(group, -1)
    extra = jnp.concatenate(
        [*halves(query_bias), *halves(value_bias), *halves(fc1_bias), clip_sets.astype(BF)]
    )
    extra_lanes = up_to(-(-extra.shape[0] // dc), 128)
    extra = jnp.pad(extra, (0, dc * extra_lanes - extra.shape[0])).reshape(dc, extra_lanes)
    small = jnp.concatenate([tables, extra], axis=1)
    small_lanes = small.shape[1]
    natural = lanes >= small_lanes
    small = rows_padded(small, dc, lanes) if natural else small.reshape(-1, lanes)
    small_rows = small.shape[0]
    at_table = dr + group
    packed = jnp.concatenate(
        [
            jnp.concatenate([w_query, w_key, w_value, w_out.T], axis=1),
            jnp.concatenate(
                [v.reshape(group, width) for v in (query_up, key_up, value_up)] + [turn(out_down)], axis=1
            ),
            rows_padded(small, up_to(small_rows, 8), lanes),
        ],
        axis=0,
    )
    g1 = lax.all_gather(packed, BOTH, axis=0).reshape(nr, nc, -1, lanes)
    small = g1[:, :, at_table : at_table + small_rows]
    small = small[..., :small_lanes] if natural else small.reshape(nr, nc, dc, small_lanes)
    tables = small[..., : 6 * wide].reshape(D, 6 * wide)
    extra = small[..., 6 * wide :].reshape(nr, nc, -1)
    sums = extra[0].astype(F32)
    both = lambda at, n: sums[:, at : at + n] + sums[:, at + n : at + 2 * n]
    zeros = jnp.zeros((nc, width), F32)
    bias_qkv = jnp.concatenate([both(0, width), zeros, both(2 * width, width)], axis=1)[:, None]
    b1 = both(4 * width, hidden)[:, None]
    every_set = extra[:, 0, 4 * width + 2 * hidden :][:, :clips].astype(jnp.int32)
    wo_t, odown = assemble(g1, group)

    packed = jnp.concatenate(
        [w_fc1, w_fc2.T, fc1_up.reshape(group, hidden), turn(fc2_down)], axis=0
    )
    packed, g1 = lax.optimization_barrier((packed, g1))
    g2 = lax.all_gather(packed, BOTH, axis=0).reshape(nr, nc, -1, hidden)
    at_f = 2 * dr

    gain1, shift1 = norm1_gain[None], norm1_shift[None]
    gain2, shift2 = norm2_gain[None], norm2_shift[None]

    normed, ranks, away, mine = project(
        tokens, gain1, shift1, g1, bias_qkv, tables, sets, scales, exchange.order, tm, per
    )
    lens = exchange.lens(clip_lengths)
    results = []
    for sources, plan, index, n in zip(
        exchange.to_heads(away, mine), exchange.plans, exchange.indices, lens
    ):
        if results:
            n, _ = lax.optimization_barrier((n, results[-1][1]))
        results.append(attend(sources, plan, index, n, clip_len, hh))
    pieces = exchange.from_heads([r[0] for r in results])
    att = collect(pieces, exchange.code, own, tm, nc)
    middle, normed_mlp, ro, r1 = out_project(
        att, tokens, wo_t, out_bias[None], odown, tables, gain2, shift2, sets, scales, tm, per
    )
    output, grad_middle, grad_branch, gup1, gdown2, gup2, gdown1 = mlp(
        normed_mlp, cotangent, middle, g2, b1, tables, r1, fc2_bias[None], gain2, sets, scales, tm, per, at_f
    )
    away, mine, goup, godown = out_back(
        grad_branch, wo_t, tables, odown, att, ro, sets, scales, exchange.side, tm, nc, per, nr
    )

    by_model = lambda v: v.reshape(nr, nc, dc, wide)
    late = scatter_sum([gup1, gdown2, godown, by_model(gdown1), by_model(goup), by_model(gup2)])
    late = lax.psum_scatter(late, BOTH, scatter_dimension=0, tiled=True)

    def untile(v, n):
        t = v.shape[0] // group
        return v.reshape(t, group, 128).transpose(1, 0, 2).reshape(group, t * 128)[:, :n].reshape(SETS, per, n)

    as_down = lambda v: v.transpose(2, 0, 1, 3).reshape(SETS, dr, RANK)
    as_up = lambda v: v.transpose(2, 1, 3, 0).reshape(SETS, RANK, dr)
    flip = lambda v: jnp.swapaxes(v, 1, 2)
    calls = list(
        zip(exchange.to_heads(away, mine), exchange.plans, exchange.indices, results, lens)
    )
    backs = []
    for sources, plan, index, (o, lse, x), n in reversed(calls):
        if backs:
            n, _ = lax.optimization_barrier((n, backs[-1]))
        backs.append(attend_back(sources, plan, index, x, o, lse, n, hh))
    pieces = exchange.from_heads(backs[::-1])
    dy, grank, gup, gdown = adapt_back(
        pieces, exchange.code, g1, normed, ranks, sets, scales, block_clip, clips, tm, per
    )
    tiles = gup.shape[1] // (3 * clips)
    folded = gdown.shape[0]
    ups = gup.reshape(nc, clips * 3 * tiles, nr, per, 128).transpose(2, 0, 1, 3, 4)
    ups = ups.reshape(nr, nc, -1, 128)
    downs = [gdown[i].reshape(nr, nc, dc, 128) for i in range(folded)]
    last = scatter_sum([ups] + downs).reshape(nr * nc, -1, 128)
    last, dy = lax.optimization_barrier((last, dy))
    got = lax.all_to_all(last, BOTH, 0, 0, tiled=True)
    grad_tokens = project_back(dy, g1, grank, tables, tokens, grad_middle, gain1, tm)
    late, grad_tokens = lax.optimization_barrier((late, grad_tokens))
    summed = late.astype(F32)
    a = gup1.shape[2]
    b = godown.shape[2]
    grad_fc1_up = untile(summed[:a], hidden)
    grad_fc2_down = flip(untile(summed[a : 2 * a], hidden))
    grad_out_down = flip(untile(summed[2 * a : 2 * a + b], width))
    model = summed[2 * a + b : 2 * a + b + 3 * dc].reshape(3, dc, wide)
    model = model.transpose(1, 0, 2).reshape(dc, 3 * wide)

    got = jnp.sum(got.reshape(nr, nc, -1, 128).astype(F32), axis=1)
    onehot = (every_set[:, :, None] == jnp.arange(SETS, dtype=jnp.int32)).astype(F32)
    n = ups.shape[2]
    per_clip = got[:, :n].reshape(nr, clips, -1, 128)
    per_set = jnp.sum(onehot[:, :, :, None, None] * per_clip[:, :, None], axis=(0, 1))
    per_set = per_set.reshape(SETS, 3, tiles, per, 128).transpose(1, 0, 3, 2, 4)
    up = per_set.reshape(3, SETS, per, tiles * 128)[..., :width]
    side = got[:, n : n + folded * dc].reshape(nr, folded, dc, 128).transpose(0, 2, 1, 3)
    side = side.reshape(nr, dc, folded * 128)[..., : clips * 3 * RANK]
    side = side.reshape(nr, dc, clips, 3 * RANK).transpose(0, 2, 1, 3)
    side = jnp.sum(onehot[:, :, :, None, None] * side[:, :, None], axis=(0, 1))
    side = side.transpose(1, 0, 2).reshape(dc, SETS * 3 * RANK)
    every = lax.all_gather(jnp.concatenate([side, model], axis=1), "cols", axis=0, tiled=True)
    down = every[:, : SETS * 3 * RANK].reshape(dr, SETS, 3, RANK).transpose(2, 1, 0, 3)
    model = every[:, SETS * 3 * RANK :].reshape(dr, 3, nr, SETS, per).swapaxes(0, 1)
    grad_fc1_down, grad_out_up, grad_fc2_up = as_down(model[0]), as_up(model[1]), as_up(model[2])
    return (
        output,
        grad_tokens,
        down[0],
        up[0],
        down[1],
        up[1],
        down[2],
        up[2],
        grad_out_down,
        grad_out_up,
        grad_fc1_down,
        grad_fc1_up,
        grad_fc2_down,
        grad_fc2_up,
    )


def solution(mesh):
    both = P(("rows", "cols"), None)
    grid = P("rows", "cols")
    turned = P("cols", "rows")
    down = P(None, "rows", None)
    up = P(None, "rows", "cols")
    far_down = P(None, "cols", "rows")
    far_up = P(None, None, "rows")
    return jax.shard_map(
        body,
        mesh=mesh,
        in_specs=(
            both,
            both,
            P("rows"),
            P("rows"),
            P("rows"),
            P(),
            P(),
            grid,
            P("cols"),
            grid,
            grid,
            P("cols"),
            turned,
            P(),
            P(),
            P(),
            grid,
            P("cols"),
            turned,
            P(),
            down,
            up,
            down,
            up,
            down,
            up,
            far_down,
            far_up,
            down,
            up,
            far_down,
            far_up,
        ),
        out_specs=(
            both,
            both,
            down,
            up,
            down,
            up,
            down,
            up,
            far_down,
            far_up,
            down,
            up,
            far_down,
            far_up,
        ),
        check_vma=False,
    )
```
